32 devices in a mesh: dp: 2 (over x), cols: 4 (over z), rows: 4 (over y, core).
Axes of the slice: x: 2, y: 2, z: 4, core: 2. Of those that a mesh axis runs over, the one named last changes fastest.
Arguments:
- frames: bfloat16 [24, 2, 192, 128, 16], P(None, 'dp', 'rows', 'cols'), parts along dimension 1
- w_in: bfloat16 [3, 3, 16, 512], replicated
- w_rec: bfloat16 [3, 3, 128, 512], replicated
- gate_bias: float32 [512], replicated
- h_init: bfloat16 [2, 192, 128, 128], P('dp', 'rows', 'cols'), parts along dimension 0
- c_init: float32 [2, 192, 128, 128], P('dp', 'rows', 'cols'), parts along dimension 0
Outputs:
- output 1: bfloat16 [24, 2, 192, 128, 128], P(None, 'dp', 'rows', 'cols'), parts along dimension 1
- output 2: float32 [2, 192, 128, 128], P('dp', 'rows', 'cols'), parts along dimension 0
There are 2 independent parts. The reference program is written for one: setup_inputs(seed, part) draws one part's arguments, and reference() takes and returns one part's arrays. A program takes and returns all parts, laid end to end along the dimension named above; an argument that names none is the same for every part.
All inputs are finite; a program needn't handle non-finite values.
Results may differ from the reference program's by a relative error of at most 0.00438231.
Values are sent between devices in bfloat16 or wider.
A program may use at most 1 GiB of HBM per device.

```python
import jax
import jax.numpy as jnp
from jax import lax

STEPS = 24
BATCH = 1
GRID_H = 192
GRID_W = 128
C_IN = 16
C_HID = 128

CONV_DIMS = ("NHWC", "HWIO", "NHWC")


def setup_inputs(seed: int = 0, part: int = 0) -> dict:
    part_key = jax.random.fold_in(jax.random.key(seed), part)
    k_frames, k_hid, k_cell = jax.random.split(part_key, 3)
    k_win, k_wrec, k_bias = jax.random.split(jax.random.key(seed + 1), 3)
    frames = jax.random.normal(k_frames, (STEPS, BATCH, GRID_H, GRID_W, C_IN), jnp.float32)
    w_in = jax.random.normal(k_win, (3, 3, C_IN, 4 * C_HID), jnp.float32) * (9 * C_IN) ** -0.5
    w_rec = jax.random.normal(k_wrec, (3, 3, C_HID, 4 * C_HID), jnp.float32) * (2.0 * (9 * C_HID) ** -0.5)
    forget_shift = jnp.concatenate([jnp.zeros((C_HID,), jnp.float32), jnp.ones((C_HID,), jnp.float32), jnp.zeros((2 * C_HID,), jnp.float32)])
    gate_bias = 0.5 * jax.random.normal(k_bias, (4 * C_HID,), jnp.float32) + forget_shift
    h_init = 0.5 * jax.random.normal(k_hid, (BATCH, GRID_H, GRID_W, C_HID), jnp.float32)
    c_init = jax.random.normal(k_cell, (BATCH, GRID_H, GRID_W, C_HID), jnp.float32)
    return {
        "frames": frames.astype(jnp.bfloat16),
        "w_in": w_in.astype(jnp.bfloat16),
        "w_rec": w_rec.astype(jnp.bfloat16),
        "gate_bias": gate_bias,
        "h_init": h_init.astype(jnp.bfloat16),
        "c_init": c_init,
    }


def conv_same(operand, kernel):
    return lax.conv_general_dilated(operand.astype(jnp.float32), kernel, (1, 1), "SAME", dimension_numbers=CONV_DIMS)


def reference(frames, w_in, w_rec, gate_bias, h_init, c_init):
    w_in32 = w_in.astype(jnp.float32)
    w_rec32 = w_rec.astype(jnp.float32)

    def time_step(carry_in, frame_t):
        h_prev, c_prev = carry_in
        gate_pre = conv_same(frame_t, w_in32) + conv_same(h_prev, w_rec32) + gate_bias
        gate_i, gate_f, gate_o, gate_g = jnp.split(gate_pre, 4, axis=-1)
        c_next = jax.nn.sigmoid(gate_f) * c_prev + jax.nn.sigmoid(gate_i) * jnp.tanh(gate_g)
        h_next = (jax.nn.sigmoid(gate_o) * jnp.tanh(c_next)).astype(jnp.bfloat16)
        return (h_next, c_next), h_next

    (h_last, c_last), hidden_seq = lax.scan(time_step, (h_init, c_init), frames)
    return hidden_seq, c_last
```

```python
import functools

import jax
import jax.numpy as jnp
from jax import lax
from jax.experimental import pallas as pl
from jax.experimental.pallas import tpu as pltpu
from jax.sharding import PartitionSpec as P

MESH = pl.DeviceIdType.MESH
BF16 = jnp.bfloat16
F32 = jnp.float32

PITCH = 36
DIRECTIONS = ((-1, 0), (1, 0), (0, -1), (0, 1), (-1, -1), (-1, 1), (1, -1), (1, 1))


def opposite(d):
    return DIRECTIONS.index((-DIRECTIONS[d][0], -DIRECTIONS[d][1]))


def cell(r, c):
    return (r + 2) * PITCH + c + 2


def kernel(steps, rows, cols, n_rows, n_cols, frames_ref, w_ref, h0_ref, c0_ref, seq_ref, cout_ref,
           x_buf, p_buf, w_buf, c_main, c_side, out_buf, row_send, col_send, corner_send, row_recv, col_recv,
           corner_recv, send_sem, recv_sem, p_sem, out_sem):
    my_row = lax.axis_index("rows")
    my_col = lax.axis_index("cols")

    def exists(d):
        dr, dc = DIRECTIONS[d]
        ok = None
        for here, step, count in ((my_row, dr, n_rows), (my_col, dc, n_cols)):
            if step:
                this = (here > 0) if step < 0 else (here < count - 1)
                ok = this if ok is None else jnp.logical_and(ok, this)
        return ok

    def device(d):
        dr, dc = DIRECTIONS[d]
        return {"rows": my_row + dr, "cols": my_col + dc}

    row_recv[...] = jnp.zeros_like(row_recv)
    col_recv[...] = jnp.zeros_like(col_recv)
    corner_recv[...] = jnp.zeros_like(corner_recv)

    barrier = pltpu.get_barrier_semaphore()
    count = jnp.int32(0)
    for d in range(8):
        @pl.when(exists(d))
        def _():
            pl.semaphore_signal(barrier, inc=1, device_id=device(d), device_id_type=MESH)
        count = count + exists(d).astype(jnp.int32)
    pl.semaphore_wait(barrier, count)

    def frame_copy(t, slot):
        return pltpu.make_async_copy(frames_ref.at[t], p_buf.at[slot], p_sem.at[slot])

    def out_copy(t, slot):
        return pltpu.make_async_copy(out_buf.at[slot], seq_ref.at[t], out_sem.at[slot])

    def halo_copy(slot, d):
        dr, dc = DIRECTIONS[d]
        if dr and dc:
            src, dst = corner_send.at[slot, d - 4], corner_recv.at[slot, opposite(d) - 4]
        elif dr:
            src, dst = row_send.at[slot, d], row_recv.at[slot, opposite(d)]
        else:
            src, dst = col_send.at[slot, d - 2], col_recv.at[slot, opposite(d) - 2]
        return pltpu.make_async_remote_copy(
            src_ref=src, dst_ref=dst, send_sem=send_sem.at[slot, d], recv_sem=recv_sem.at[slot, opposite(d)],
            device_id=device(d), device_id_type=MESH)

    def arrival(slot, d):
        if d >= 4:
            src, dst = corner_send.at[slot, d - 4], corner_recv.at[slot, d - 4]
        elif d < 2:
            src, dst = row_send.at[slot, d], row_recv.at[slot, d]
        else:
            src, dst = col_send.at[slot, d - 2], col_recv.at[slot, d - 2]
        return pltpu.make_async_remote_copy(
            src_ref=src, dst_ref=dst, send_sem=send_sem.at[slot, d], recv_sem=recv_sem.at[slot, d],
            device_id=device(d), device_id_type=MESH)

    frame_copy(0, 0).start()
    frame_copy(1, 1).start()
    x_buf[...] = jnp.zeros_like(x_buf)
    w_buf[...] = w_ref[...]

    side_cols = (0, 1, 2, 3, cols - 4, cols - 3, cols - 2, cols - 1)
    width = cols - 8

    for r in range(rows):
        x_buf[0, pl.ds(cell(r, 0), cols), :] = h0_ref[r].astype(F32)
        c_main[pl.ds(r * width, width), :] = c0_ref[r, 4:cols - 4, :]
    c_flat = c0_ref.reshape(rows * cols, 128)
    for i, c in enumerate(side_cols):
        c_side[pl.ds(i * rows, rows), :] = c_flat[pl.ds(c, rows, stride=cols), :]

    def lhs_of(slot, groups):
        parts = []
        for dy in range(3):
            for dx in range(3):
                pieces = []
                for r, c, length, vertical in groups:
                    start = cell(r + dy - 1, c + dx - 1)
                    index = pl.ds(start, length, stride=PITCH) if vertical else pl.ds(start, length)
                    pieces.append(x_buf[slot, index, :])
                parts.append(jnp.concatenate(pieces, axis=0) if len(pieces) > 1 else pieces[0])
        for dy in range(3):
            pieces = []
            for r, c, length, vertical in groups:
                start = (r + dy) * cols + c
                index = pl.ds(start, length, stride=cols) if vertical else pl.ds(start, length)
                pieces.append(p_buf[slot, index, :])
            parts.append(jnp.concatenate(pieces, axis=0) if len(pieces) > 1 else pieces[0])
        return jnp.concatenate(parts, axis=1).astype(BF16)

    def gates_of(slot, groups):
        return jnp.dot(lhs_of(slot, groups), w_buf[...], preferred_element_type=F32)

    def update(gates, c_prev):
        gi, gf, go, gg = (jnp.tanh(gates[:, 128 * k:128 * (k + 1)]) for k in range(4))
        c_next = 0.5 * ((gf * c_prev + c_prev) + (gi * gg + gg))
        return (0.5 * go + 0.5) * jnp.tanh(c_next), c_next

    def send_halo(slot, wanted=True):
        nxt = x_buf.at[slot]
        for k, r in enumerate((0, rows - 1)):
            row_send[slot, k] = nxt[pl.ds(cell(r, 0), cols), :].astype(BF16)
        for k, c in enumerate((0, cols - 1)):
            col_send[slot, k] = nxt[pl.ds(cell(0, c), rows, stride=PITCH), :].astype(BF16)
        for k, (dr, dc) in enumerate(DIRECTIONS[4:]):
            r = 0 if dr < 0 else rows - 1
            c = 0 if dc < 0 else cols - 1
            corner_send[slot, k] = jnp.broadcast_to(nxt[pl.ds(cell(r, c), 1), :], (16, 128)).astype(BF16)
        for d in range(8):
            @pl.when(jnp.logical_and(exists(d), wanted))
            def _():
                halo_copy(slot, d).start()

    def wait_halo(slot):
        for d in range(8):
            @pl.when(exists(d))
            def _():
                arrival(slot, d).wait_recv()
        now = x_buf.at[slot]
        for k, r in enumerate((-1, rows)):
            now[pl.ds(cell(r, 0), cols), :] = row_recv[slot, k].astype(F32)
        for k, c in enumerate((-1, cols)):
            now[pl.ds(cell(0, c), rows, stride=PITCH), :] = col_recv[slot, k].astype(F32)
        for k, (dr, dc) in enumerate(DIRECTIONS[4:]):
            r = -1 if dr < 0 else rows
            c = -1 if dc < 0 else cols
            now[pl.ds(cell(r, c), 1), :] = corner_recv[slot, k][0:1, :].astype(F32)

    def wait_sent(slot):
        for d in range(8):
            @pl.when(exists(d))
            def _():
                halo_copy(slot, d).wait_send()

    def side_run(i):
        return (0, side_cols[i], rows, True)

    def do_side(now, ids):
        gates = gates_of(now, [side_run(i) for i in ids])
        if len(ids) == ids[-1] - ids[0] + 1:
            c_index = pl.ds(ids[0] * rows, len(ids) * rows)
            h, c_next = update(gates, c_side[c_index, :])
            c_side[c_index, :] = c_next
        else:
            c_prev = jnp.concatenate([c_side[pl.ds(i * rows, rows), :] for i in ids], axis=0)
            h, c_next = update(gates, c_prev)
            for n, i in enumerate(ids):
                c_side[pl.ds(i * rows, rows), :] = c_next[n * rows:(n + 1) * rows]
        for n, i in enumerate(ids):
            x_buf[1 - now, pl.ds(cell(0, side_cols[i]), rows, stride=PITCH), :] = h[n * rows:(n + 1) * rows]

    def do_main(now, row_list):
        gates = gates_of(now, [(r, 4, width, False) for r in row_list])
        if len(row_list) == row_list[-1] - row_list[0] + 1:
            c_index = pl.ds(row_list[0] * width, len(row_list) * width)
            h, c_next = update(gates, c_main[c_index, :])
            c_main[c_index, :] = c_next
        else:
            c_prev = jnp.concatenate([c_main[pl.ds(r * width, width), :] for r in row_list], axis=0)
            h, c_next = update(gates, c_prev)
            for n, r in enumerate(row_list):
                c_main[pl.ds(r * width, width), :] = c_next[n * width:(n + 1) * width]
        for n, r in enumerate(row_list):
            x_buf[1 - now, pl.ds(cell(r, 4), width), :] = h[n * width:(n + 1) * width]

    def one_step(t, now):
        frame_copy(t, now).wait()
        wait_halo(now)

        @pl.when(t >= 1)
        def _():
            wait_sent(1 - now)

        do_side(now, (0, 1, 2, 3))
        do_side(now, (4, 5, 6, 7))
        do_main(now, (0, rows - 1))
        send_halo(1 - now, t + 1 < steps)
        inner = list(range(1, rows - 1))
        block = 12
        for at in range(0, len(inner), block):
            do_main(now, inner[at:at + block])

        @pl.when(t + 2 < steps)
        def _():
            frame_copy(t + 2, now).start()

        @pl.when(t >= 2)
        def _():
            out_copy(t - 2, now).wait()
        for r in range(rows):
            out_buf[now, r] = x_buf[1 - now, pl.ds(cell(r, 0), cols), :].astype(BF16)
        out_copy(t, now).start()

    send_halo(0)

    def two_steps(i, carry):
        one_step(2 * i, 0)
        one_step(2 * i + 1, 1)
        return carry

    lax.fori_loop(0, steps // 2, two_steps, 0)

    wait_sent(1)
    out_copy(steps - 2, 0).wait()
    out_copy(steps - 1, 1).wait()
    for r in range(rows):
        cout_ref[r, 4:cols - 4, :] = c_main[pl.ds(r * width, width), :]
    cout_flat = cout_ref.reshape(rows * cols, 128)
    for i, c in enumerate(side_cols):
        cout_flat[pl.ds(c, rows, stride=cols), :] = c_side[pl.ds(i * rows, rows), :]


def edge_exchange(tile_in, axis_name, axis_size, axis_dim, width):
    length = tile_in.shape[axis_dim]
    low_part = lax.slice_in_dim(tile_in, 0, width, axis=axis_dim)
    high_part = lax.slice_in_dim(tile_in, length - width, length, axis=axis_dim)
    forward = [(source, source + 1) for source in range(axis_size - 1)]
    backward = [(source + 1, source) for source in range(axis_size - 1)]
    from_prev = lax.ppermute(high_part, axis_name, forward)
    from_next = lax.ppermute(low_part, axis_name, backward)
    return jnp.concatenate([from_prev, tile_in, from_next], axis=axis_dim)


def solution(mesh):
    n_rows = mesh.shape["rows"]
    n_cols = mesh.shape["cols"]
    seq_spec = P(None, "dp", "rows", "cols", None)
    state_spec = P("dp", "rows", "cols", None)

    def local_run(frames, w_in, w_rec, gate_bias, h_init, c_init):
        steps, _, rows, cols, c_in = frames.shape
        hid = h_init.shape[-1]
        ext = edge_exchange(edge_exchange(frames, "rows", n_rows, 2, 1), "cols", n_cols, 3, 1)[:, 0]
        ones = jnp.zeros((steps, rows + 2, cols, 128 - 3 * c_in), BF16).at[..., :3].set(1)
        packed = jnp.concatenate([ext[:, :, dx:dx + cols] for dx in range(3)] + [ones], axis=-1)
        packed = packed.astype(F32).reshape(steps, (rows + 2) * cols, 128)

        scale = jnp.concatenate([jnp.full((3 * hid,), 0.5, F32), jnp.ones((hid,), F32)])
        bias = gate_bias * scale
        b0 = lax.reduce_precision(bias, 8, 7)
        b1 = lax.reduce_precision(bias - b0, 8, 7)
        b2 = lax.reduce_precision(bias - b0 - b1, 8, 7)
        w_pad = jnp.zeros((128 - 3 * c_in, 4 * hid), F32)
        blocks = [w_rec.astype(F32).reshape(9 * hid, 4 * hid) * scale]
        for dy in range(3):
            rest = w_pad if dy else jnp.concatenate([jnp.stack([b0, b1, b2]), w_pad[3:]], axis=0)
            blocks += [w_in[dy].astype(F32).reshape(3 * c_in, 4 * hid) * scale, rest]
        w_all = jnp.concatenate(blocks, axis=0).astype(BF16)

        vmem = pl.BlockSpec(memory_space=pltpu.VMEM)
        anywhere = pl.BlockSpec(memory_space=pl.ANY)
        seq, c_last = pl.pallas_call(
            functools.partial(kernel, steps, rows, cols, n_rows, n_cols),
            out_shape=(jax.ShapeDtypeStruct((steps, rows, cols, hid), BF16),
                       jax.ShapeDtypeStruct((rows, cols, hid), F32)),
            in_specs=[anywhere, vmem, vmem, vmem],
            out_specs=(anywhere, vmem),
            scratch_shapes=[
                pltpu.VMEM((2, (rows + 4) * PITCH, 128), F32),
                pltpu.VMEM((2, (rows + 2) * cols, 128), F32),
                pltpu.VMEM((1536, 4 * hid), BF16),
                pltpu.VMEM((rows * (cols - 8), 128), F32),
                pltpu.VMEM((rows * 8, 128), F32),
                pltpu.VMEM((2, rows, cols, 128), BF16),
                pltpu.VMEM((2, 2, cols, 128), BF16),
                pltpu.VMEM((2, 2, rows, 128), BF16),
                pltpu.VMEM((2, 4, 16, 128), BF16),
                pltpu.VMEM((2, 2, cols, 128), BF16),
                pltpu.VMEM((2, 2, rows, 128), BF16),
                pltpu.VMEM((2, 4, 16, 128), BF16),
                pltpu.SemaphoreType.DMA((2, 8)),
                pltpu.SemaphoreType.DMA((2, 8)),
                pltpu.SemaphoreType.DMA((2,)),
                pltpu.SemaphoreType.DMA((2,)),
            ],
            compiler_params=pltpu.CompilerParams(
                collective_id=0, has_side_effects=True, vmem_limit_bytes=48 * 2**20),
            name="convlstm",
        )(packed, w_all, h_init[0], c_init[0])
        return seq[:, None], c_last[None]

    return jax.shard_map(local_run, mesh=mesh, in_specs=(seq_spec, P(), P(), P(), state_spec, state_spec),
                         out_specs=(seq_spec, state_spec), check_vma=False)
```

```python
import functools

import jax
import jax.numpy as jnp
from jax import lax
from jax.experimental import pallas as pl
from jax.experimental.pallas import tpu as pltpu
from jax.sharding import PartitionSpec as P

MESH = pl.DeviceIdType.MESH
BF16 = jnp.bfloat16
F32 = jnp.float32
TDT = jnp.bfloat16

PITCH = 36
DIRECTIONS = ((-1, 0), (1, 0), (0, -1), (0, 1), (-1, -1), (-1, 1), (1, -1), (1, 1))
SIDE = 4


def cell(r, c):
    return (r + 1) * PITCH + c + 2


def pcell(r, c):
    return (r + 1) * PITCH + c


def kernel(steps, rows, cols, n_rows, n_cols, c_in, frames_ref, w_rec_ref, w_in_ref, bias_ref, h0_ref, c0_ref,
           seq_ref, cout_ref,
           x_buf, p_buf, w_buf, f_buf, f_side, c_main, c_side, c_col, c_row, out_buf, row_send, col_send,
           row_recv, col_recv, corner_recv, send_sem, recv_sem, f_sem, f_send_sem, f_recv_sem, out_sem):
    my_row = lax.axis_index("rows")
    my_col = lax.axis_index("cols")
    hid = x_buf.shape[-1]
    gates_n = 4 * hid
    packed = 3 * c_in
    width = cols - 2 * SIDE
    edge_cols = (0, cols - 1)
    edge_rows = (0, rows - 1)
    inner_side = tuple(range(1, SIDE)) + tuple(range(cols - SIDE, cols - 1))

    def exists(d):
        dr, dc = DIRECTIONS[d]
        ok = None
        for here, step, count in ((my_row, dr, n_rows), (my_col, dc, n_cols)):
            if step:
                this = (here > 0) if step < 0 else (here < count - 1)
                ok = this if ok is None else jnp.logical_and(ok, this)
        return ok

    def device(d):
        dr, dc = DIRECTIONS[d]
        return {"rows": my_row + dr, "cols": my_col + dc}

    def opposite(d):
        return DIRECTIONS.index((-DIRECTIONS[d][0], -DIRECTIONS[d][1]))

    def out_copy(t, slot):
        return pltpu.make_async_copy(out_buf.at[slot], seq_ref.at[t], out_sem.at[slot])

    def source(slot, d):
        dr, dc = DIRECTIONS[d]
        if dr and dc:
            return col_send.at[slot, 0 if dc < 0 else 1, pl.ds(0 if dr < 0 else rows - 16, 16)]
        return row_send.at[slot, d] if dr else col_send.at[slot, d - 2]

    def landing(slot, d):
        dr, dc = DIRECTIONS[d]
        if dr and dc:
            return corner_recv.at[slot, d - 4]
        return row_recv.at[slot, d] if dr else col_recv.at[slot, d - 2]

    def departure(slot, d):
        return pltpu.make_async_remote_copy(
            src_ref=source(slot, d), dst_ref=landing(slot, opposite(d)), send_sem=send_sem.at[slot, d],
            recv_sem=recv_sem.at[slot, opposite(d)], device_id=device(d), device_id_type=MESH)

    def arrival(slot, d):
        return pltpu.make_async_remote_copy(
            src_ref=source(slot, d), dst_ref=landing(slot, d), send_sem=send_sem.at[slot, d],
            recv_sem=recv_sem.at[slot, d], device_id=device(d), device_id_type=MESH)

    def frame_side(part, d, arriving=False):
        ts = pl.ds(0, 1) if part == 0 else pl.ds(1, steps - 1)
        k = d - 2
        at = k if arriving else 1 - k
        return pltpu.make_async_remote_copy(
            src_ref=frames_ref.at[ts, edge_cols[k]], dst_ref=f_side.at[at, ts], send_sem=f_send_sem.at[part, k],
            recv_sem=f_recv_sem.at[part, at], device_id=device(d), device_id_type=MESH)

    def frame_load(part):
        ts = pl.ds(0, 1) if part == 0 else pl.ds(1, steps - 1)
        return pltpu.make_async_copy(frames_ref.at[ts], f_buf.at[ts], f_sem.at[part])

    frame_load(0).start()
    frame_load(1).start()
    row_recv[...] = jnp.zeros_like(row_recv)
    col_recv[...] = jnp.zeros_like(col_recv)
    corner_recv[...] = jnp.zeros_like(corner_recv)
    f_side[...] = jnp.zeros_like(f_side)

    barrier = pltpu.get_barrier_semaphore()
    count = jnp.int32(0)
    for d in range(8):
        @pl.when(exists(d))
        def _():
            pl.semaphore_signal(barrier, inc=1, device_id=device(d), device_id_type=MESH)
        count = count + exists(d).astype(jnp.int32)
    pl.semaphore_wait(barrier, count)

    for part in (0, 1):
        for d in (2, 3):
            @pl.when(exists(d))
            def _():
                frame_side(part, d).start()

    for r in range(rows):
        x_buf[0, pl.ds(cell(r, 0), cols), :] = h0_ref[r].astype(F32)
    for r in range(1, rows - 1):
        c_main[pl.ds((r - 1) * width, width), :] = c0_ref[pl.ds(r * cols + SIDE, width), :]
    for i, c in enumerate(inner_side):
        c_side[pl.ds(i * rows, rows), :] = c0_ref[pl.ds(c, rows, stride=cols), :]
    for i, c in enumerate(edge_cols):
        c_col[pl.ds(i * rows, rows), :] = c0_ref[pl.ds(c, rows, stride=cols), :]
    for i, r in enumerate(edge_rows):
        c_row[pl.ds(i * cols, cols), :] = c0_ref[pl.ds(r * cols, cols), :]

    lane = lax.broadcasted_iota(jnp.int32, (1, gates_n), 1)
    scale = jnp.where(lane < 3 * hid, 0.5, 1.0)
    for at in range(0, 9 * hid, 128):
        w_buf[pl.ds(at, 128), :] = (w_rec_ref[pl.ds(at, 128), :].astype(F32) * scale).astype(BF16)
    bias = bias_ref[...] * scale
    b0 = bias.astype(BF16).astype(F32)
    b1 = (bias - b0).astype(BF16).astype(F32)
    b2 = bias - b0 - b1
    row = lax.broadcasted_iota(jnp.int32, (16, gates_n), 0)
    bias_rows = jnp.where(row == 0, b0, jnp.where(row == 1, b1, jnp.where(row == 2, b2, 0.0)))
    for dy in range(3):
        at = 9 * hid + 128 * dy
        w_buf[pl.ds(at, packed), :] = (w_in_ref[pl.ds(packed * dy, packed), :].astype(F32) * scale).astype(BF16)
        w_buf[pl.ds(at + packed, 128 - packed), :] = jnp.zeros((128 - packed, gates_n), BF16)
        if dy == 1:
            w_buf[pl.ds(at + packed, 16), :] = bias_rows.astype(BF16)

    row = lax.broadcasted_iota(jnp.int32, (128 - packed, rows), 0)
    ones = jnp.where(row < 3, 1.0, 0.0).astype(TDT)

    def pack_frame(t, slot):
        for c in range(cols):
            if c == 0:
                window = jnp.concatenate([f_side[0, t], f_buf[t, 0], f_buf[t, 1]], axis=0)
            elif c == cols - 1:
                window = jnp.concatenate([f_buf[t, c - 1], f_buf[t, c], f_side[1, t]], axis=0)
            else:
                window = f_buf[t, c - 1:c + 2].reshape(packed, rows)
            window = jnp.concatenate([window.astype(TDT), ones], axis=0)
            p_buf[slot, pl.ds(pcell(0, c), rows, stride=PITCH), :] = window.T.astype(F32)

    def lhs_of(slot, groups):
        parts = []
        for dy in range(3):
            for dx in range(3):
                pieces = []
                for r, c, length, vertical in groups:
                    start = cell(r + dy - 1, c + dx - 1)
                    index = pl.ds(start, length, stride=PITCH) if vertical else pl.ds(start, length)
                    pieces.append(x_buf[slot, index, :])
                parts.append(jnp.concatenate(pieces, axis=0) if len(pieces) > 1 else pieces[0])
        for dy in range(3):
            pieces = []
            for r, c, length, vertical in groups:
                start = pcell(r + dy - 1, c)
                index = pl.ds(start, length, stride=PITCH) if vertical else pl.ds(start, length)
                pieces.append(p_buf[slot, index, :])
            parts.append(jnp.concatenate(pieces, axis=0) if len(pieces) > 1 else pieces[0])
        return jnp.concatenate(parts, axis=1).astype(BF16)

    def update(slot, groups, c_ref, c_at):
        gates = jnp.dot(lhs_of(slot, groups), w_buf[...], preferred_element_type=F32)
        index = pl.ds(c_at, gates.shape[0])
        c_prev = c_ref[index, :]
        gi, gf, go, gg = (jnp.tanh(gates[:, hid * k:hid * (k + 1)]) for k in range(4))
        c_next = 0.5 * ((gf * c_prev + c_prev) + (gi * gg + gg))
        c_ref[index, :] = c_next
        h = (0.5 * go + 0.5) * jnp.tanh(c_next)
        at = 0
        for r, c, length, vertical in groups:
            start = cell(r, c)
            place = pl.ds(start, length, stride=PITCH) if vertical else pl.ds(start, length)
            x_buf[1 - slot, place, :] = h[at:at + length]
            at += length
        return h

    def stage_rows(slot, h_rows):
        for k, r in enumerate(edge_rows):
            row_send[slot, k, 0:cols] = h_rows[k].astype(BF16)
            row_send[slot, k, cols:2 * cols] = p_buf[slot, pl.ds(pcell(r, 0), cols), :].astype(BF16)

    def send_halo(slot, wanted):
        for d in range(8):
            @pl.when(jnp.logical_and(exists(d), wanted))
            def _():
                departure(slot, d).start()

    def receive_halo(slot):
        for d in range(8):
            @pl.when(exists(d))
            def _():
                arrival(slot, d).wait_recv()

    def unpack_halo(slot):
        for k, r in enumerate((-1, rows)):
            x_buf[slot, pl.ds(cell(r, 0), cols), :] = row_recv[slot, k, 0:cols].astype(F32)
            p_buf[slot, pl.ds(pcell(r, 0), cols), :] = row_recv[slot, k, cols:2 * cols].astype(F32)
        for k, c in enumerate((-1, cols)):
            x_buf[slot, pl.ds(cell(0, c), rows, stride=PITCH), :] = col_recv[slot, k].astype(F32)
        for k, (dr, dc) in enumerate(DIRECTIONS[4:]):
            r, pick = (-1, 15) if dr < 0 else (rows, 0)
            c = -1 if dc < 0 else cols
            x_buf[slot, pl.ds(cell(r, c), 1), :] = corner_recv[slot, k].astype(F32)[pick:pick + 1]

    def wait_sent(slot):
        for d in range(8):
            @pl.when(exists(d))
            def _():
                departure(slot, d).wait_send()

    def write_out(slot):
        for r in range(rows):
            out_buf[slot, r] = x_buf[slot, pl.ds(cell(r, 0), cols), :].astype(BF16)

    def main_rows(slot, first, last):
        update(slot, [(r, SIDE, width, False) for r in range(first, last)], c_main, (first - 1) * width)

    def one_step(t, now):
        pack_frame(jnp.minimum(t + 1, steps - 1), 1 - now)
        write_out(now)
        main_rows(now, 1, 13)
        main_rows(now, 13, 25)

        @pl.when(t >= 1)
        def _():
            out_copy(t - 1, now).start()
            wait_sent(1 - now)

        @pl.when(t >= 2)
        def _():
            out_copy(t - 2, 1 - now).wait()
        receive_halo(now)
        unpack_halo(now)

        h_col = update(now, [(0, c, rows, True) for c in edge_cols], c_col, 0)
        h_row = update(now, [(r, 0, cols, False) for r in edge_rows], c_row, 0)
        for k in range(2):
            col_send[1 - now, k] = h_col[k * rows:(k + 1) * rows].astype(BF16)
        stage_rows(1 - now, [h_row[k * cols:(k + 1) * cols] for k in range(2)])
        send_halo(1 - now, t + 1 < steps)

        update(now, [(0, c, rows, True) for c in inner_side[:SIDE - 1]], c_side, 0)
        update(now, [(0, c, rows, True) for c in inner_side[SIDE - 1:]], c_side, (SIDE - 1) * rows)
        main_rows(now, 25, 36)
        main_rows(now, 36, 47)

    frame_load(0).wait()
    for d in (2, 3):
        @pl.when(exists(d))
        def _():
            frame_side(0, d, True).wait_recv()
    pack_frame(0, 0)
    for k, c in enumerate(edge_cols):
        col_send[0, k] = x_buf[0, pl.ds(cell(0, c), rows, stride=PITCH), :].astype(BF16)
    stage_rows(0, [x_buf[0, pl.ds(cell(r, 0), cols), :] for r in edge_rows])
    send_halo(0, True)
    frame_load(1).wait()
    for d in (2, 3):
        @pl.when(exists(d))
        def _():
            frame_side(1, d, True).wait_recv()

    def two_steps(i, carry):
        one_step(2 * i, 0)
        one_step(2 * i + 1, 1)
        return carry

    lax.fori_loop(0, steps // 2, two_steps, 0)

    write_out(0)
    out_copy(steps - 1, 0).start()
    for r in range(1, rows - 1):
        cout_ref[pl.ds(r * cols + SIDE, width), :] = c_main[pl.ds((r - 1) * width, width), :]
    for i, c in enumerate(inner_side):
        cout_ref[pl.ds(c, rows, stride=cols), :] = c_side[pl.ds(i * rows, rows), :]
    for i, c in enumerate(edge_cols):
        cout_ref[pl.ds(c, rows, stride=cols), :] = c_col[pl.ds(i * rows, rows), :]
    for i, r in enumerate(edge_rows):
        cout_ref[pl.ds(r * cols, cols), :] = c_row[pl.ds(i * cols, cols), :]
    wait_sent(1)
    for part in (0, 1):
        for d in (2, 3):
            @pl.when(exists(d))
            def _():
                frame_side(part, d).wait_send()
    out_copy(steps - 2, 1).wait()
    out_copy(steps - 1, 0).wait()


def solution(mesh):
    n_rows = mesh.shape["rows"]
    n_cols = mesh.shape["cols"]
    seq_spec = P(None, "dp", "rows", "cols", None)
    state_spec = P("dp", "rows", "cols", None)

    def local_run(frames, w_in, w_rec, gate_bias, h_init, c_init):
        steps, _, rows, cols, c_in = frames.shape
        hid = h_init.shape[-1]
        vmem = pl.BlockSpec(memory_space=pltpu.VMEM)
        anywhere = pl.BlockSpec(memory_space=pl.ANY)
        seq, c_last = pl.pallas_call(
            functools.partial(kernel, steps, rows, cols, n_rows, n_cols, c_in),
            out_shape=(jax.ShapeDtypeStruct((steps, rows, cols, hid), BF16),
                       jax.ShapeDtypeStruct((rows * cols, hid), F32)),
            in_specs=[anywhere, vmem, vmem, vmem, vmem, vmem],
            out_specs=(anywhere, vmem),
            scratch_shapes=[
                pltpu.VMEM((2, (rows + 2) * PITCH, hid), F32),
                pltpu.VMEM((2, (rows + 2) * PITCH, 128), F32),
                pltpu.VMEM((9 * hid + 3 * 128, 4 * hid), BF16),
                pltpu.VMEM((steps, cols, c_in, rows), BF16),
                pltpu.VMEM((2, steps, c_in, rows), BF16),
                pltpu.VMEM(((rows - 2) * (cols - 2 * SIDE), hid), F32),
                pltpu.VMEM((rows * 2 * (SIDE - 1), hid), F32),
                pltpu.VMEM((rows * 2, hid), F32),
                pltpu.VMEM((cols * 2, hid), F32),
                pltpu.VMEM((2, rows, cols, hid), BF16),
                pltpu.VMEM((2, 2, 2 * cols, hid), BF16),
                pltpu.VMEM((2, 2, rows, hid), BF16),
                pltpu.VMEM((2, 2, 2 * cols, hid), BF16),
                pltpu.VMEM((2, 2, rows, hid), BF16),
                pltpu.VMEM((2, 4, 16, hid), BF16),
                pltpu.SemaphoreType.DMA((2, 8)),
                pltpu.SemaphoreType.DMA((2, 8)),
                pltpu.SemaphoreType.DMA((2,)),
                pltpu.SemaphoreType.DMA((2, 2)),
                pltpu.SemaphoreType.DMA((2, 2)),
                pltpu.SemaphoreType.DMA((2,)),
            ],
            compiler_params=pltpu.CompilerParams(
                collective_id=0, has_side_effects=True, vmem_limit_bytes=48 * 2**20),
            name="convlstm",
        )(jnp.transpose(frames[:, 0], (0, 2, 3, 1)), w_rec.reshape(9 * hid, 4 * hid),
          w_in.reshape(9 * c_in, 4 * hid), gate_bias.reshape(1, 4 * hid), h_init[0], c_init[0].reshape(rows * cols, hid))
        return seq[:, None], c_last.reshape(c_init.shape)

    return jax.shard_map(local_run, mesh=mesh, in_specs=(seq_spec, P(), P(), P(), state_spec, state_spec),
                         out_specs=(seq_spec, state_spec), check_vma=False)
```

```python
import functools

import jax
import jax.numpy as jnp
from jax import lax
from jax.experimental import pallas as pl
from jax.experimental.pallas import tpu as pltpu
from jax.sharding import PartitionSpec as P

MESH = pl.DeviceIdType.MESH
BF16 = jnp.bfloat16
F32 = jnp.float32
TDT = jnp.bfloat16

PITCH = 36
DIRECTIONS = ((-1, 0), (1, 0), (0, -1), (0, 1), (-1, -1), (-1, 1), (1, -1), (1, 1))
UNROLL = 4
BLOCK = 10
BESIDE = 41
SIDE = 4


def cell(r, c):
    return (r + 1) * PITCH + c + 2


def pcell(r, c):
    return (r + 1) * PITCH + c


def kernel(steps, rows, cols, n_rows, n_cols, c_in, frames_ref, w_rec_ref, w_in_ref, bias_ref, h0_ref, c0_ref,
           seq_low, seq_high, cout_ref,
           x_buf, p_buf, w_buf, bias_buf, f_buf, f_side, c_main, c_side, c_edge, row_send, col_send,
           row_recv, col_recv, corner_recv, send_sem, recv_sem, f_sem, f_send_sem, f_recv_sem, arg_sem):
    my_row = lax.axis_index("rows")
    my_col = lax.axis_index("cols")
    hid = x_buf.shape[-1]
    gates_n = 4 * hid
    packed = 3 * c_in
    width = cols - 2 * SIDE
    edge_cols = (0, cols - 1)
    edge_rows = (0, rows - 1)
    inner_side = tuple(range(1, SIDE)) + tuple(range(cols - SIDE, cols - 1))

    def exists(d):
        dr, dc = DIRECTIONS[d]
        ok = None
        for here, step, count in ((my_row, dr, n_rows), (my_col, dc, n_cols)):
            if step:
                this = (here > 0) if step < 0 else (here < count - 1)
                ok = this if ok is None else jnp.logical_and(ok, this)
        return ok

    def device(d):
        dr, dc = DIRECTIONS[d]
        return {"rows": my_row + dr, "cols": my_col + dc}

    def opposite(d):
        return DIRECTIONS.index((-DIRECTIONS[d][0], -DIRECTIONS[d][1]))

    def source(slot, d):
        dr, dc = DIRECTIONS[d]
        if dr and dc:
            return col_send.at[slot, 0 if dc < 0 else 1, pl.ds(0 if dr < 0 else rows - 16, 16)]
        return row_send.at[slot, d] if dr else col_send.at[slot, d - 2]

    def landing(slot, d):
        dr, dc = DIRECTIONS[d]
        if dr and dc:
            return corner_recv.at[slot, d - 4]
        return row_recv.at[slot, d] if dr else col_recv.at[slot, d - 2]

    def departure(slot, d):
        return pltpu.make_async_remote_copy(
            src_ref=source(slot, d), dst_ref=landing(slot, opposite(d)), send_sem=send_sem.at[slot, d],
            recv_sem=recv_sem.at[slot, opposite(d)], device_id=device(d), device_id_type=MESH)

    def arrival(slot, d):
        return pltpu.make_async_remote_copy(
            src_ref=source(slot, d), dst_ref=landing(slot, d), send_sem=send_sem.at[slot, d],
            recv_sem=recv_sem.at[slot, d], device_id=device(d), device_id_type=MESH)

    def frame_side(part, d, arriving=False):
        ts = pl.ds(0, 1) if part == 0 else pl.ds(1, steps - 1)
        k = d - 2
        at = k if arriving else 1 - k
        return pltpu.make_async_remote_copy(
            src_ref=f_buf.at[ts, edge_cols[k]], dst_ref=f_side.at[at, ts], send_sem=f_send_sem.at[part, k],
            recv_sem=f_recv_sem.at[part, at], device_id=device(d), device_id_type=MESH)

    def frame_load(part):
        ts = pl.ds(0, 1) if part == 0 else pl.ds(1, steps - 1)
        return pltpu.make_async_copy(frames_ref.at[ts], f_buf.at[ts], f_sem.at[part])

    loads = [(h0_ref.at[pl.ds(0, rows // 2)], seq_low.at[steps - 1]),
             (h0_ref.at[pl.ds(rows // 2, rows // 2)], seq_high.at[steps - 1]), (c0_ref, cout_ref), (w_rec_ref, w_buf.at[pl.ds(0, 9 * hid)]),
             (bias_ref, bias_buf)]
    loads += [(w_in_ref.at[pl.ds(packed * dy, packed)], w_buf.at[pl.ds(9 * hid + 128 * dy, packed)]) for dy in range(3)]
    loads = [pltpu.make_async_copy(src, dst, arg_sem.at[k]) for k, (src, dst) in enumerate(loads)]
    frame_load(0).start()
    for load in loads:
        load.start()
    frame_load(1).start()
    for slot in range(2):
        for r in (-1, rows):
            x_buf[slot, pl.ds(cell(r, -2), PITCH), :] = jnp.zeros((PITCH, hid), F32)
            p_buf[slot, pl.ds(pcell(r, 0), PITCH), :] = jnp.zeros((PITCH, 128), F32)
    row_recv[...] = jnp.zeros_like(row_recv)
    col_recv[...] = jnp.zeros_like(col_recv)
    corner_recv[...] = jnp.zeros_like(corner_recv)
    f_side[...] = jnp.zeros_like(f_side)

    barrier = pltpu.get_barrier_semaphore()
    count = jnp.int32(0)
    for d in range(8):
        @pl.when(exists(d))
        def _():
            pl.semaphore_signal(barrier, inc=1, device_id=device(d), device_id_type=MESH)
        count = count + exists(d).astype(jnp.int32)
    pl.semaphore_wait(barrier, count)

    def send_sides(part):
        frame_load(part).wait()
        for d in (2, 3):
            @pl.when(exists(d))
            def _():
                frame_side(part, d).start()

    def receive_sides(part):
        for d in (2, 3):
            @pl.when(exists(d))
            def _():
                frame_side(part, d, True).wait_recv()

    send_sides(0)
    for load in loads[:2]:
        load.wait()
    for r in range(rows):
        half, at = (seq_low, r) if r < rows // 2 else (seq_high, r - rows // 2)
        x_buf[0, pl.ds(cell(r, 0), cols), :] = half[steps - 1, at].astype(F32)
    loads[2].wait()
    c_edge_at = [(c, rows, cols) for c in edge_cols] + [(r * cols, cols, 1) for r in edge_rows]
    for r in range(1, rows - 1):
        c_main[pl.ds((r - 1) * width, width), :] = cout_ref[pl.ds(r * cols + SIDE, width), :]
    for i, c in enumerate(inner_side):
        c_side[pl.ds(i * rows, rows), :] = cout_ref[pl.ds(c, rows, stride=cols), :]
    at = 0
    for start, length, stride in c_edge_at:
        c_edge[pl.ds(at, length), :] = cout_ref[pl.ds(start, length, stride=stride), :]
        at += length
    send_sides(1)

    lane = lax.broadcasted_iota(jnp.int32, (1, gates_n), 1)
    scale = jnp.where(lane < 3 * hid, 0.5, 1.0)
    for load in loads[3:]:
        load.wait()
    for at in range(0, 9 * hid, 128):
        w_buf[pl.ds(at, 128), :] = (w_buf[pl.ds(at, 128), :].astype(F32) * scale).astype(BF16)
    bias = bias_buf[...] * scale
    b0 = bias.astype(BF16).astype(F32)
    b1 = (bias - b0).astype(BF16).astype(F32)
    b2 = bias - b0 - b1
    row = lax.broadcasted_iota(jnp.int32, (16, gates_n), 0)
    bias_rows = jnp.where(row == 0, b0, jnp.where(row == 1, b1, jnp.where(row == 2, b2, 0.0)))
    for dy in range(3):
        at = 9 * hid + 128 * dy
        w_buf[pl.ds(at, packed), :] = (w_buf[pl.ds(at, packed), :].astype(F32) * scale).astype(BF16)
        w_buf[pl.ds(at + packed, 128 - packed), :] = jnp.zeros((128 - packed, gates_n), BF16)
        if dy == 1:
            w_buf[pl.ds(at + packed, 16), :] = bias_rows.astype(BF16)

    row = lax.broadcasted_iota(jnp.int32, (128 - packed, rows), 0)
    ones = jnp.where(row < 3, 1.0, 0.0).astype(TDT)

    def pack_frame(t, slot):
        for c in range(cols):
            if c == 0:
                window = jnp.concatenate([f_side[0, t], f_buf[t, 0], f_buf[t, 1]], axis=0)
            elif c == cols - 1:
                window = jnp.concatenate([f_buf[t, c - 1], f_buf[t, c], f_side[1, t]], axis=0)
            else:
                window = f_buf[t, c - 1:c + 2].reshape(packed, rows)
            window = jnp.concatenate([window.astype(TDT), ones], axis=0)
            p_buf[slot, pl.ds(pcell(0, c), rows, stride=PITCH), :] = window.T.astype(F32)

    def lhs_of(slot, groups):
        parts = []
        for dy in range(3):
            for dx in range(3):
                pieces = []
                for r, c, length, vertical in groups:
                    start = cell(r + dy - 1, c + dx - 1)
                    index = pl.ds(start, length, stride=PITCH) if vertical else pl.ds(start, length)
                    pieces.append(x_buf[slot, index, :])
                parts.append(jnp.concatenate(pieces, axis=0) if len(pieces) > 1 else pieces[0])
        for dy in range(3):
            pieces = []
            for r, c, length, vertical in groups:
                start = pcell(r + dy - 1, c)
                index = pl.ds(start, length, stride=PITCH) if vertical else pl.ds(start, length)
                pieces.append(p_buf[slot, index, :])
            parts.append(jnp.concatenate(pieces, axis=0) if len(pieces) > 1 else pieces[0])
        return jnp.concatenate(parts, axis=1).astype(BF16)

    def gates_of(slot, groups):
        return jnp.dot(lhs_of(slot, groups), w_buf[...], preferred_element_type=F32)

    def finish(slot, groups, gates, c_ref, c_at):
        index = pl.ds(c_at, gates.shape[0])
        c_prev = c_ref[index, :]
        gi, gf, go, gg = (jnp.tanh(gates[:, hid * k:hid * (k + 1)]) for k in range(4))
        c_next = 0.5 * ((gf * c_prev + c_prev) + (gi * gg + gg))
        c_ref[index, :] = c_next
        h = (0.5 * go + 0.5) * jnp.tanh(c_next)
        at = 0
        for r, c, length, vertical in groups:
            start = cell(r, c)
            place = pl.ds(start, length, stride=PITCH) if vertical else pl.ds(start, length)
            x_buf[1 - slot, place, :] = h[at:at + length]
            at += length
        return h

    def update(slot, groups, c_ref, c_at):
        return finish(slot, groups, gates_of(slot, groups), c_ref, c_at)

    def stage_rows(slot, h_rows):
        for k, r in enumerate(edge_rows):
            row_send[slot, k, 0:cols] = h_rows[k].astype(BF16)
            row_send[slot, k, cols:2 * cols] = p_buf[slot, pl.ds(pcell(r, 0), cols), :].astype(BF16)

    def send_halo(slot, wanted):
        for d in range(8):
            @pl.when(jnp.logical_and(exists(d), wanted))
            def _():
                departure(slot, d).start()

    def receive_halo(slot):
        for d in range(8):
            @pl.when(exists(d))
            def _():
                arrival(slot, d).wait_recv()

    def unpack_halo(slot):
        for k, r in enumerate((-1, rows)):
            x_buf[slot, pl.ds(cell(r, 0), cols), :] = row_recv[slot, k, 0:cols].astype(F32)
            p_buf[slot, pl.ds(pcell(r, 0), cols), :] = row_recv[slot, k, cols:2 * cols].astype(F32)
        for k, c in enumerate((-1, cols)):
            x_buf[slot, pl.ds(cell(0, c), rows, stride=PITCH), :] = col_recv[slot, k].astype(F32)
        for k, (dr, dc) in enumerate(DIRECTIONS[4:]):
            r, pick = (-1, 15) if dr < 0 else (rows, 0)
            c = -1 if dc < 0 else cols
            x_buf[slot, pl.ds(cell(r, c), 1), :] = corner_recv[slot, k].astype(F32)[pick:pick + 1]

    def wait_sent(slot):
        for d in range(8):
            @pl.when(exists(d))
            def _():
                departure(slot, d).wait_send()

    def write_out(t, slot):
        for r in range(rows):
            half, at = (seq_low, r) if r < rows // 2 else (seq_high, r - rows // 2)
            half[t, at] = x_buf[slot, pl.ds(cell(r, 0), cols), :].astype(BF16)

    def run_of(first, last):
        return [(r, SIDE, width, False) for r in range(first, last)]

    def main_rows(slot, first, last):
        update(slot, run_of(first, last), c_main, (first - 1) * width)

    edge_groups = [(0, c, rows, True) for c in edge_cols] + [(r, 0, cols, False) for r in edge_rows]

    def one_step(t, now):
        pack_frame(jnp.minimum(t + 1, steps - 1), 1 - now)
        write_out(jnp.maximum(t - 1, 0), now)
        for at in range(1, BESIDE, BLOCK):
            main_rows(now, at, min(at + BLOCK, BESIDE))
        update(now, [(0, c, rows, True) for c in inner_side[:SIDE - 1]], c_side, 0)
        update(now, [(0, c, rows, True) for c in inner_side[SIDE - 1:]], c_side, (SIDE - 1) * rows)

        @pl.when(t >= 1)
        def _():
            wait_sent(1 - now)
        receive_halo(now)
        unpack_halo(now)

        edge_gates = gates_of(now, edge_groups)
        gates = gates_of(now, run_of(BESIDE, rows - 1))
        h = finish(now, edge_groups, edge_gates, c_edge, 0)
        for k in range(2):
            col_send[1 - now, k] = h[k * rows:(k + 1) * rows].astype(BF16)
        stage_rows(1 - now, [h[2 * rows + k * cols:2 * rows + (k + 1) * cols] for k in range(2)])
        send_halo(1 - now, t + 1 < steps)
        finish(now, run_of(BESIDE, rows - 1), gates, c_main, (BESIDE - 1) * width)

    receive_sides(0)
    pack_frame(0, 0)
    for k, c in enumerate(edge_cols):
        col_send[0, k] = x_buf[0, pl.ds(cell(0, c), rows, stride=PITCH), :].astype(BF16)
    stage_rows(0, [x_buf[0, pl.ds(cell(r, 0), cols), :] for r in edge_rows])
    send_halo(0, True)
    receive_sides(1)

    def trip(i, carry):
        for k in range(UNROLL):
            one_step(UNROLL * i + k, k % 2)
        return carry

    lax.fori_loop(0, steps // UNROLL, trip, 0)

    write_out(steps - 1, 0)
    for r in range(1, rows - 1):
        cout_ref[pl.ds(r * cols + SIDE, width), :] = c_main[pl.ds((r - 1) * width, width), :]
    for i, c in enumerate(inner_side):
        cout_ref[pl.ds(c, rows, stride=cols), :] = c_side[pl.ds(i * rows, rows), :]
    at = 0
    for start, length, stride in c_edge_at:
        cout_ref[pl.ds(start, length, stride=stride), :] = c_edge[pl.ds(at, length), :]
        at += length
    wait_sent(1)
    for part in (0, 1):
        for d in (2, 3):
            @pl.when(exists(d))
            def _():
                frame_side(part, d).wait_send()


def solution(mesh):
    n_rows = mesh.shape["rows"]
    n_cols = mesh.shape["cols"]
    seq_spec = P(None, "dp", "rows", "cols", None)
    state_spec = P("dp", "rows", "cols", None)

    def local_run(frames, w_in, w_rec, gate_bias, h_init, c_init):
        steps, _, rows, cols, c_in = frames.shape
        hid = h_init.shape[-1]
        vmem = pl.BlockSpec(memory_space=pltpu.VMEM)
        args = (jnp.transpose(frames[:, 0], (0, 2, 3, 1)), w_rec.reshape(9 * hid, 4 * hid),
                w_in.reshape(9 * c_in, 4 * hid), gate_bias.reshape(1, 4 * hid), h_init[0],
                c_init[0].reshape(rows * cols, hid))
        hbm = pl.BlockSpec(memory_space=pltpu.HBM)
        low, high, c_last = pl.pallas_call(
            functools.partial(kernel, steps, rows, cols, n_rows, n_cols, c_in),
            out_shape=(jax.ShapeDtypeStruct((steps, rows // 2, cols, hid), BF16),) * 2 + (
                jax.ShapeDtypeStruct((rows * cols, hid), F32),),
            in_specs=[hbm] * 6,
            out_specs=(vmem,) * 3,
            scratch_shapes=[
                pltpu.VMEM((2, (rows + 2) * PITCH, hid), F32),
                pltpu.VMEM((2, (rows + 2) * PITCH, 128), F32),
                pltpu.VMEM((9 * hid + 3 * 128, 4 * hid), BF16),
                pltpu.VMEM((1, 4 * hid), F32),
                pltpu.VMEM((steps, cols, c_in, rows), BF16),
                pltpu.VMEM((2, steps, c_in, rows), BF16),
                pltpu.VMEM(((rows - 2) * (cols - 2 * SIDE), hid), F32),
                pltpu.VMEM((rows * 2 * (SIDE - 1), hid), F32),
                pltpu.VMEM(((rows + cols) * 2, hid), F32),
                pltpu.VMEM((2, 2, 2 * cols, hid), BF16),
                pltpu.VMEM((2, 2, rows, hid), BF16),
                pltpu.VMEM((2, 2, 2 * cols, hid), BF16),
                pltpu.VMEM((2, 2, rows, hid), BF16),
                pltpu.VMEM((2, 4, 16, hid), BF16),
                pltpu.SemaphoreType.DMA((2, 8)),
                pltpu.SemaphoreType.DMA((2, 8)),
                pltpu.SemaphoreType.DMA((2,)),
                pltpu.SemaphoreType.DMA((2, 2)),
                pltpu.SemaphoreType.DMA((2, 2)),
                pltpu.SemaphoreType.DMA((8,)),
            ],
            compiler_params=pltpu.CompilerParams(
                collective_id=0, has_side_effects=True, vmem_limit_bytes=24 * 2**20),
            name="convlstm",
        )(*(pltpu.with_memory_space_constraint(x, pltpu.HBM) for x in args))
        seq = jnp.concatenate([low, high], axis=1)
        return seq[:, None], c_last.reshape(c_init.shape)

    return jax.shard_map(local_run, mesh=mesh, in_specs=(seq_spec, P(), P(), P(), state_spec, state_spec),
                         out_specs=(seq_spec, state_spec), check_vma=False)
```

```python
import functools

import jax
import jax.numpy as jnp
from jax import lax
from jax.experimental import pallas as pl
from jax.experimental.pallas import tpu as pltpu
from jax.sharding import PartitionSpec as P

MESH = pl.DeviceIdType.MESH
BF16 = jnp.bfloat16
F32 = jnp.float32
TDT = jnp.bfloat16

PITCH = 36
DIRECTIONS = ((-1, 0), (1, 0), (0, -1), (0, 1), (-1, -1), (-1, 1), (1, -1), (1, 1))
BLOCK = 11
SIDE = 4


def cell(r, c):
    return (r + 2) * PITCH + c + 2


def pcell(r, c):
    return (r + 2) * PITCH + c + 1


def kernel(steps, rows, cols, n_rows, n_cols, c_in, frames_ref, w_rec_ref, w_in_ref, bias_ref, h0_ref, c0_ref,
           seq_low, seq_high, cout_ref,
           x_buf, p_buf, w_buf, bias_buf, f_buf, f_side, c_main, c_col, c_row, ring_row, ring_col,
           row_send, col_send, crow_send, ccol_send,
           row_recv, col_recv, corner_recv, crow_recv, ccol_recv, ccorner_recv,
           send_sem, recv_sem, f_sem, f_send_sem, f_recv_sem, arg_sem):
    my_row = lax.axis_index("rows")
    my_col = lax.axis_index("cols")
    hid = x_buf.shape[-1]
    gates_n = 4 * hid
    packed = 3 * c_in
    width = cols - 2 * SIDE
    half = rows // 2
    long = rows + 8
    side_cols = tuple(range(SIDE)) + tuple(range(cols - SIDE, cols))
    edge_rows = (0, 1, rows - 2, rows - 1)

    def exists(d):
        dr, dc = DIRECTIONS[d]
        ok = None
        for here, step, count in ((my_row, dr, n_rows), (my_col, dc, n_cols)):
            if step:
                this = (here > 0) if step < 0 else (here < count - 1)
                ok = this if ok is None else jnp.logical_and(ok, this)
        return ok

    def device(d):
        dr, dc = DIRECTIONS[d]
        return {"rows": my_row + dr, "cols": my_col + dc}

    def opposite(d):
        return DIRECTIONS.index((-DIRECTIONS[d][0], -DIRECTIONS[d][1]))

    def source(slot, d, kind):
        dr, dc = DIRECTIONS[d]
        if dr and dc:
            k = 0 if dc < 0 else 1
            if kind:
                return ccol_send.at[slot, k, pl.ds(0 if dr < 0 else rows - 8, 8)]
            return col_send.at[slot, k, :, pl.ds(0 if dr < 0 else rows - 16, 16)]
        if dr:
            return (crow_send if kind else row_send).at[slot, d]
        return (ccol_send if kind else col_send).at[slot, d - 2]

    def landing(slot, d, kind):
        dr, dc = DIRECTIONS[d]
        if dr and dc:
            return (ccorner_recv if kind else corner_recv).at[slot, d - 4]
        if dr:
            return (crow_recv if kind else row_recv).at[slot, d]
        return (ccol_recv if kind else col_recv).at[slot, d - 2]

    def departure(slot, d, kind):
        return pltpu.make_async_remote_copy(
            src_ref=source(slot, d, kind), dst_ref=landing(slot, opposite(d), kind), send_sem=send_sem.at[slot, kind, d],
            recv_sem=recv_sem.at[slot, kind, opposite(d)], device_id=device(d), device_id_type=MESH)

    def arrival(slot, d, kind):
        return pltpu.make_async_remote_copy(
            src_ref=source(slot, d, kind), dst_ref=landing(slot, d, kind), send_sem=send_sem.at[slot, kind, d],
            recv_sem=recv_sem.at[slot, kind, d], device_id=device(d), device_id_type=MESH)

    def frame_part(part):
        return pl.ds(0, 2) if part == 0 else pl.ds(2, steps - 2)

    def frame_side(part, d, arriving=False):
        ts = frame_part(part)
        k = d - 2
        at = k if arriving else 1 - k
        return pltpu.make_async_remote_copy(
            src_ref=f_buf.at[ts, pl.ds(0 if k == 0 else cols - 2, 2)], dst_ref=f_side.at[at, ts],
            send_sem=f_send_sem.at[part, k], recv_sem=f_recv_sem.at[part, at], device_id=device(d), device_id_type=MESH)

    def frame_load(part):
        ts = frame_part(part)
        return pltpu.make_async_copy(frames_ref.at[ts], f_buf.at[ts], f_sem.at[part])

    loads = [(h0_ref.at[pl.ds(0, half)], seq_low.at[steps - 1]), (h0_ref.at[pl.ds(half, half)], seq_high.at[steps - 1]),
             (c0_ref, cout_ref), (w_rec_ref, w_buf.at[pl.ds(0, 9 * hid)]), (bias_ref, bias_buf)]
    loads += [(w_in_ref.at[pl.ds(packed * dy, packed)], w_buf.at[pl.ds(9 * hid + 128 * dy, packed)]) for dy in range(3)]
    loads = [pltpu.make_async_copy(src, dst, arg_sem.at[k]) for k, (src, dst) in enumerate(loads)]
    frame_load(0).start()
    for load in loads:
        load.start()
    frame_load(1).start()
    for ref in (row_recv, col_recv, corner_recv, crow_recv, ccol_recv, ccorner_recv, f_side):
        ref[...] = jnp.zeros_like(ref)
    for slot in range(2):
        x_buf[slot, pl.ds(0, 2 * PITCH), :] = jnp.zeros((2 * PITCH, hid), F32)
        x_buf[slot, pl.ds((rows + 2) * PITCH, 10 * PITCH), :] = jnp.zeros((10 * PITCH, hid), F32)
    for slot in range(4):
        p_buf[slot, pl.ds(0, 2 * PITCH), :] = jnp.zeros((2 * PITCH, 128), F32)
        p_buf[slot, pl.ds((rows + 2) * PITCH, 10 * PITCH), :] = jnp.zeros((10 * PITCH, 128), F32)
    ring_col[...] = jnp.zeros_like(ring_col)

    barrier = pltpu.get_barrier_semaphore()
    count = jnp.int32(0)
    for d in range(8):
        @pl.when(exists(d))
        def _():
            pl.semaphore_signal(barrier, inc=1, device_id=device(d), device_id_type=MESH)
        count = count + exists(d).astype(jnp.int32)
    pl.semaphore_wait(barrier, count)

    def send_sides(part):
        frame_load(part).wait()
        for d in (2, 3):
            @pl.when(exists(d))
            def _():
                frame_side(part, d).start()

    def receive_sides(part):
        for d in (2, 3):
            @pl.when(exists(d))
            def _():
                frame_side(part, d, True).wait_recv()

    send_sides(0)
    for load in loads[:2]:
        load.wait()
    for r in range(rows):
        part, at = (seq_low, r) if r < half else (seq_high, r - half)
        x_buf[0, pl.ds(cell(r, 0), cols), :] = part[steps - 1, at].astype(F32)
    loads[2].wait()
    for r in range(2, rows - 2):
        c_main[pl.ds((r - 2) * width, width), :] = cout_ref[pl.ds(r * cols + SIDE, width), :]
    for i, c in enumerate(side_cols):
        c_col[pl.ds(i * rows, rows), :] = cout_ref[pl.ds(c, rows, stride=cols), :]
    for i, r in enumerate(edge_rows):
        c_row[pl.ds(i * cols, cols), :] = cout_ref[pl.ds(r * cols, cols), :]
    send_sides(1)

    lane = lax.broadcasted_iota(jnp.int32, (1, gates_n), 1)
    scale = jnp.where(lane < 3 * hid, 0.5, 1.0)
    for load in loads[3:]:
        load.wait()
    for at in range(0, 9 * hid, 128):
        w_buf[pl.ds(at, 128), :] = (w_buf[pl.ds(at, 128), :].astype(F32) * scale).astype(BF16)
    bias = bias_buf[...] * scale
    b0 = bias.astype(BF16).astype(F32)
    b1 = (bias - b0).astype(BF16).astype(F32)
    b2 = bias - b0 - b1
    row = lax.broadcasted_iota(jnp.int32, (16, gates_n), 0)
    bias_rows = jnp.where(row == 0, b0, jnp.where(row == 1, b1, jnp.where(row == 2, b2, 0.0)))
    for dy in range(3):
        at = 9 * hid + 128 * dy
        w_buf[pl.ds(at, packed), :] = (w_buf[pl.ds(at, packed), :].astype(F32) * scale).astype(BF16)
        w_buf[pl.ds(at + packed, 128 - packed), :] = jnp.zeros((128 - packed, gates_n), BF16)
        if dy == 1:
            w_buf[pl.ds(at + packed, 16), :] = bias_rows.astype(BF16)

    row = lax.broadcasted_iota(jnp.int32, (128 - packed, rows), 0)
    ones = jnp.where(row < 3, 1.0, 0.0).astype(BF16)

    def pack_frame(t, slot):
        for c in range(-1, cols + 1):
            pieces = []
            for k in range(c - 1, c + 2):
                if k < 0:
                    pieces.append(f_side[0, t, k + 2])
                elif k < cols:
                    pieces.append(f_buf[t, k])
                else:
                    pieces.append(f_side[1, t, k - cols])
            window = jnp.concatenate(pieces + [ones], axis=0)
            p_buf[slot, pl.ds(pcell(0, c), rows, stride=PITCH), :] = window.T.astype(F32)

    def run_index(start, length, vertical):
        return pl.ds(start, length, stride=PITCH) if vertical else pl.ds(start, length)

    def gates_of(slot, p_slot, groups):
        parts = []
        for dy in range(3):
            for dx in range(3):
                pieces = [x_buf[slot, run_index(cell(r + dy - 1, c + dx - 1), length, vertical), :]
                          for r, c, length, vertical in groups]
                parts.append(jnp.concatenate(pieces, axis=0) if len(pieces) > 1 else pieces[0])
        for dy in range(3):
            pieces = [p_buf[p_slot, run_index(pcell(r + dy - 1, c), length, vertical), :]
                      for r, c, length, vertical in groups]
            parts.append(jnp.concatenate(pieces, axis=0) if len(pieces) > 1 else pieces[0])
        lhs = jnp.concatenate(parts, axis=1).astype(BF16)
        return jnp.dot(lhs, w_buf[...], preferred_element_type=F32)

    def finish(slot, groups, gates, c_ref, c_at, mask=None):
        index = pl.ds(c_at, gates.shape[0])
        c_prev = c_ref[index, :]
        gi, gf, go, gg = (jnp.tanh(gates[:, hid * k:hid * (k + 1)]) for k in range(4))
        c_next = 0.5 * ((gf * c_prev + c_prev) + (gi * gg + gg))
        h = (0.5 * go + 0.5) * jnp.tanh(c_next)
        if mask is None:
            c_ref[index, :] = c_next
        else:
            h = h * mask
        at = 0
        for r, c, length, vertical in groups:
            x_buf[1 - slot, run_index(cell(r, c), length, vertical), :] = h[at:at + length]
            at += length

    def update(slot, p_slot, groups, c_ref, c_at):
        finish(slot, groups, gates_of(slot, p_slot, groups), c_ref, c_at)

    def stage(slot, p_first):
        state = x_buf.at[0]
        for k, r in enumerate((0, rows - 2)):
            for n in range(2):
                row_send[slot, k, n * cols:(n + 1) * cols] = state[pl.ds(cell(r + n, 0), cols), :].astype(BF16)
            at = 2 * cols
            row_send[slot, k, at:at + 2 * PITCH] = p_buf[p_first, pl.ds(pcell(r, -1), 2 * PITCH), :].astype(BF16)
            at += 2 * PITCH
            r_one = 0 if k == 0 else rows - 1
            row_send[slot, k, at:at + PITCH] = p_buf[p_first + 1, pl.ds(pcell(r_one, -1), PITCH), :].astype(BF16)
            crow_send[slot, k] = c_row[pl.ds((0 if k == 0 else 3) * cols, cols), :]
        for k, c in enumerate((0, cols - 2)):
            for n in range(2):
                col_send[slot, k, n] = state[pl.ds(cell(0, c + n), rows, stride=PITCH), :].astype(BF16)
            ccol_send[slot, k] = c_col[pl.ds((0 if k == 0 else 2 * SIDE - 1) * rows, rows), :]

    def send_halo(slot, wanted):
        for d in range(8):
            @pl.when(jnp.logical_and(exists(d), wanted))
            def _():
                departure(slot, d, 0).start()
                departure(slot, d, 1).start()

    def receive_halo(slot):
        for d in range(8):
            @pl.when(exists(d))
            def _():
                arrival(slot, d, 0).wait_recv()
                arrival(slot, d, 1).wait_recv()

    def unpack_halo(slot, p_first):
        state = x_buf.at[0]
        for k, r in enumerate((-2, rows)):
            for n in range(2):
                state[pl.ds(cell(r + n, 0), cols), :] = row_recv[slot, k, n * cols:(n + 1) * cols].astype(F32)
            at = 2 * cols
            p_buf[p_first, pl.ds(pcell(r, -1), 2 * PITCH), :] = row_recv[slot, k, at:at + 2 * PITCH].astype(F32)
            at += 2 * PITCH
            r_one = -1 if k == 0 else rows
            p_buf[p_first + 1, pl.ds(pcell(r_one, -1), PITCH), :] = row_recv[slot, k, at:at + PITCH].astype(F32)
            ring_row[pl.ds(k * cols, cols), :] = crow_recv[slot, k]
        for k, c in enumerate((-2, cols)):
            for n in range(2):
                state[pl.ds(cell(0, c + n), rows, stride=PITCH), :] = col_recv[slot, k, n].astype(F32)
            ring_col[pl.ds(k * long + 1, rows), :] = ccol_recv[slot, k]
        for k, (dr, dc) in enumerate(DIRECTIONS[4:]):
            r, pick = (-2, 14) if dr < 0 else (rows, 0)
            c = -2 if dc < 0 else cols
            for n in range(2):
                state[pl.ds(cell(r, c + n), 2, stride=PITCH), :] = corner_recv[slot, k, n].astype(F32)[pick:pick + 2]
            at = (0 if dc < 0 else long) + (0 if dr < 0 else rows + 1)
            pick = 7 if dr < 0 else 0
            ring_col[pl.ds(at, 1), :] = ccorner_recv[slot, k][pick:pick + 1]

    def wait_sent(slot):
        for d in range(8):
            @pl.when(exists(d))
            def _():
                departure(slot, d, 0).wait_send()
                departure(slot, d, 1).wait_send()

    def write_out(t, slot):
        for r in range(rows):
            part, at = (seq_low, r) if r < half else (seq_high, r - half)
            part[t, at] = x_buf[slot, pl.ds(cell(r, 0), cols), :].astype(BF16)

    def main_run(first, last):
        return [(r, SIDE, width, False) for r in range(first, last)]

    def main_rows(slot, p_slot, first, last):
        update(slot, p_slot, main_run(first, last), c_main, (first - 2) * width)

    def side_run(*ids):
        return [(0, side_cols[i], rows, True) for i in ids]

    there = [jnp.where(exists(d), 1.0, 0.0).astype(F32) for d in range(4)]
    place = lax.broadcasted_iota(jnp.int32, (long, hid), 0)
    ends = jnp.where(place == 0, there[0], jnp.where(place == rows + 1, there[1], 1.0))
    ring_mask = jnp.concatenate([ends * there[2], ends * there[3],
                                 jnp.full((cols, hid), 1.0, F32) * there[0], jnp.full((cols, hid), 1.0, F32) * there[1]],
                                axis=0)
    ring_col_run = [(-1, -1, long, True), (-1, cols, long, True)]
    ring_row_run = [(-1, 0, cols, False), (rows, 0, cols, False)]
    row_run = [(r, 0, cols, False) for r in edge_rows]
    n_long = 2 * long
    last = 2 * SIDE - 1

    def pair(m, now):
        t = 2 * m
        pa = 2 * now
        other = 2 * (1 - now)
        pack_frame(jnp.minimum(t + 2, steps - 2), other)
        pack_frame(jnp.minimum(t + 3, steps - 1), other + 1)
        write_out(jnp.maximum(t - 1, 0), 0)
        for at in range(2, rows - 2, BLOCK):
            main_rows(0, pa, at, at + BLOCK)
        update(0, pa, side_run(1, 2, 3), c_col, rows)
        update(0, pa, side_run(last - 3, last - 2, last - 1), c_col, (last - 3) * rows)

        @pl.when(m >= 1)
        def _():
            wait_sent(1 - now)
        receive_halo(now)
        unpack_halo(now, pa)

        own = side_run(0) + side_run(last) + row_run
        own_gates = gates_of(0, pa, own)
        ring_gates = gates_of(0, pa, ring_col_run + ring_row_run)
        beside = gates_of(1, pa + 1, main_run(13, 21))
        finish(0, side_run(0), own_gates[:rows], c_col, 0)
        finish(0, side_run(last), own_gates[rows:2 * rows], c_col, last * rows)
        finish(0, row_run, own_gates[2 * rows:], c_row, 0)
        finish(0, ring_col_run, ring_gates[:n_long], ring_col, 0, ring_mask[:n_long])
        finish(0, ring_row_run, ring_gates[n_long:], ring_row, 0, ring_mask[n_long:])
        for i, r in ((0, 0), (3, rows - 1)):
            for first in (1, last - 3):
                c_col[pl.ds(first * rows + r, 3, stride=rows), :] = c_row[pl.ds(i * cols + side_cols[first], 3), :]
        finish(1, main_run(13, 21), beside, c_main, (13 - 2) * width)
        left = side_run(0, 1) + side_run(last - 1, last)
        edge_gates = gates_of(1, pa + 1, left + row_run)
        beside = gates_of(1, pa + 1, main_run(21, 29))
        finish(1, side_run(0, 1), edge_gates[:2 * rows], c_col, 0)
        finish(1, side_run(last - 1, last), edge_gates[2 * rows:4 * rows], c_col, (last - 1) * rows)
        finish(1, row_run, edge_gates[4 * rows:], c_row, 0)
        stage(1 - now, other)
        send_halo(1 - now, t + 2 < steps)

        finish(1, main_run(21, 29), beside, c_main, (21 - 2) * width)
        write_out(t, 1)
        main_rows(1, pa + 1, 2, 13)
        main_rows(1, pa + 1, 29, 38)
        main_rows(1, pa + 1, 38, 46)
        update(1, pa + 1, side_run(2, 3), c_col, 2 * rows)
        update(1, pa + 1, side_run(last - 3, last - 2), c_col, (last - 3) * rows)

    receive_sides(0)
    pack_frame(0, 0)
    pack_frame(1, 1)
    stage(0, 0)
    send_halo(0, True)
    receive_sides(1)

    def trip(i, carry):
        pair(2 * i, 0)
        pair(2 * i + 1, 1)
        return carry

    lax.fori_loop(0, steps // 4, trip, 0)

    write_out(steps - 1, 0)
    for r in range(2, rows - 2):
        cout_ref[pl.ds(r * cols + SIDE, width), :] = c_main[pl.ds((r - 2) * width, width), :]
    for i, c in enumerate(side_cols):
        cout_ref[pl.ds(c, rows, stride=cols), :] = c_col[pl.ds(i * rows, rows), :]
    for i, r in enumerate(edge_rows):
        cout_ref[pl.ds(r * cols, cols), :] = c_row[pl.ds(i * cols, cols), :]
    wait_sent(1)
    for part in (0, 1):
        for d in (2, 3):
            @pl.when(exists(d))
            def _():
                frame_side(part, d).wait_send()


def solution(mesh):
    n_rows = mesh.shape["rows"]
    n_cols = mesh.shape["cols"]
    seq_spec = P(None, "dp", "rows", "cols", None)
    state_spec = P("dp", "rows", "cols", None)

    def local_run(frames, w_in, w_rec, gate_bias, h_init, c_init):
        steps, _, rows, cols, c_in = frames.shape
        hid = h_init.shape[-1]
        row_words = 2 * cols + 3 * PITCH + 4
        vmem = pl.BlockSpec(memory_space=pltpu.VMEM)
        args = (jnp.transpose(frames[:, 0], (0, 2, 3, 1)), w_rec.reshape(9 * hid, 4 * hid),
                w_in.reshape(9 * c_in, 4 * hid), gate_bias.reshape(1, 4 * hid), h_init[0],
                c_init[0].reshape(rows * cols, hid))
        hbm = pl.BlockSpec(memory_space=pltpu.HBM)
        low, high, c_last = pl.pallas_call(
            functools.partial(kernel, steps, rows, cols, n_rows, n_cols, c_in),
            out_shape=(jax.ShapeDtypeStruct((steps, rows // 2, cols, hid), BF16),) * 2 + (
                jax.ShapeDtypeStruct((rows * cols, hid), F32),),
            in_specs=[hbm] * 6,
            out_specs=(vmem,) * 3,
            scratch_shapes=[
                pltpu.VMEM((2, (rows + 12) * PITCH, hid), F32),
                pltpu.VMEM((4, (rows + 12) * PITCH, 128), F32),
                pltpu.VMEM((9 * hid + 3 * 128, 4 * hid), BF16),
                pltpu.VMEM((1, 4 * hid), F32),
                pltpu.VMEM((steps, cols, c_in, rows), BF16),
                pltpu.VMEM((2, steps, 2, c_in, rows), BF16),
                pltpu.VMEM(((rows - 4) * (cols - 2 * SIDE), hid), F32),
                pltpu.VMEM((rows * 2 * SIDE, hid), F32),
                pltpu.VMEM((cols * 4, hid), F32),
                pltpu.VMEM((cols * 2, hid), F32),
                pltpu.VMEM(((rows + 8) * 2, hid), F32),
                pltpu.VMEM((2, 2, row_words, hid), BF16),
                pltpu.VMEM((2, 2, 2, rows, hid), BF16),
                pltpu.VMEM((2, 2, cols, hid), F32),
                pltpu.VMEM((2, 2, rows, hid), F32),
                pltpu.VMEM((2, 2, row_words, hid), BF16),
                pltpu.VMEM((2, 2, 2, rows, hid), BF16),
                pltpu.VMEM((2, 4, 2, 16, hid), BF16),
                pltpu.VMEM((2, 2, cols, hid), F32),
                pltpu.VMEM((2, 2, rows, hid), F32),
                pltpu.VMEM((2, 4, 8, hid), F32),
                pltpu.SemaphoreType.DMA((2, 2, 8)),
                pltpu.SemaphoreType.DMA((2, 2, 8)),
                pltpu.SemaphoreType.DMA((2,)),
                pltpu.SemaphoreType.DMA((2, 2)),
                pltpu.SemaphoreType.DMA((2, 2)),
                pltpu.SemaphoreType.DMA((8,)),
            ],
            compiler_params=pltpu.CompilerParams(
                collective_id=0, has_side_effects=True, vmem_limit_bytes=24 * 2**20),
            name="convlstm",
        )(*(pltpu.with_memory_space_constraint(x, pltpu.HBM) for x in args))
        seq = jnp.concatenate([low, high], axis=1)
        return seq[:, None], c_last.reshape(c_init.shape)

    return jax.shard_map(local_run, mesh=mesh, in_specs=(seq_spec, P(), P(), P(), state_spec, state_spec),
                         out_specs=(seq_spec, state_spec), check_vma=False)
```

```python
import functools

import jax
import jax.numpy as jnp
from jax import lax
from jax.experimental import pallas as pl
from jax.experimental.pallas import tpu as pltpu
from jax.sharding import PartitionSpec as P

MESH = pl.DeviceIdType.MESH
BF16 = jnp.bfloat16
F32 = jnp.float32
TDT = jnp.bfloat16

PITCH = 36
DIRECTIONS = ((-1, 0), (1, 0), (0, -1), (0, 1), (-1, -1), (-1, 1), (1, -1), (1, 1))
CHUNK = 3
BLOCK = 11
SIDE = 4


def cell(r, c):
    return (r + 2) * PITCH + c + 2


def pcell(r, c):
    return (r + 2) * PITCH + c + 1


def kernel(steps, rows, cols, n_rows, n_cols, c_in, frames_ref, w_rec_ref, w_in_ref, bias_ref, h0_ref, c0_ref,
           seq_ref, cout_ref,
           x_buf, p_buf, w_buf, bias_buf, f_buf, f_side, c_main, c_col, c_row, ring_row, ring_col,
           row_send, col_send, corner_send, crow_send, ccol_send,
           row_recv, col_recv, corner_recv, crow_recv, ccol_recv,
           send_sem, recv_sem, f_sem, f_send_sem, f_recv_sem, arg_sem):
    my_row = lax.axis_index("rows")
    my_col = lax.axis_index("cols")
    hid = x_buf.shape[-1]
    gates_n = 4 * hid
    packed = 3 * c_in
    width = cols - 2 * SIDE
    long = rows + 8
    side_cols = tuple(range(SIDE)) + tuple(range(cols - SIDE, cols))
    last = len(side_cols) - 1
    edge_rows = (0, 1, rows - 2, rows - 1)

    def exists(d):
        dr, dc = DIRECTIONS[d]
        ok = None
        for here, step, count in ((my_row, dr, n_rows), (my_col, dc, n_cols)):
            if step:
                this = (here > 0) if step < 0 else (here < count - 1)
                ok = this if ok is None else jnp.logical_and(ok, this)
        return ok

    def device(d):
        dr, dc = DIRECTIONS[d]
        return {"rows": my_row + dr, "cols": my_col + dc}

    def opposite(d):
        return DIRECTIONS.index((-DIRECTIONS[d][0], -DIRECTIONS[d][1]))

    def source(slot, d, kind):
        dr, dc = DIRECTIONS[d]
        if dr and dc:
            return corner_send.at[slot, d - 4]
        if dr:
            return (crow_send if kind else row_send).at[slot, d]
        return (ccol_send if kind else col_send).at[slot, d - 2]

    def landing(slot, d, kind):
        dr, dc = DIRECTIONS[d]
        if dr and dc:
            return corner_recv.at[slot, d - 4]
        if dr:
            return (crow_recv if kind else row_recv).at[slot, d]
        return (ccol_recv if kind else col_recv).at[slot, d - 2]

    def departure(slot, d, kind):
        return pltpu.make_async_remote_copy(
            src_ref=source(slot, d, kind), dst_ref=landing(slot, opposite(d), kind), send_sem=send_sem.at[slot, kind, d],
            recv_sem=recv_sem.at[slot, kind, opposite(d)], device_id=device(d), device_id_type=MESH)

    def arrival(slot, d, kind):
        return pltpu.make_async_remote_copy(
            src_ref=source(slot, d, kind), dst_ref=landing(slot, d, kind), send_sem=send_sem.at[slot, kind, d],
            recv_sem=recv_sem.at[slot, kind, d], device_id=device(d), device_id_type=MESH)

    def frame_part(part):
        return pl.ds(0, 2) if part == 0 else pl.ds(2, steps - 2)

    def frame_side(part, d, arriving=False):
        ts = frame_part(part)
        k = d - 2
        at = k if arriving else 1 - k
        return pltpu.make_async_remote_copy(
            src_ref=f_buf.at[ts, pl.ds(0 if k == 0 else cols - 2, 2)], dst_ref=f_side.at[at, ts],
            send_sem=f_send_sem.at[part, k], recv_sem=f_recv_sem.at[part, at], device_id=device(d), device_id_type=MESH)

    def frame_load(part):
        ts = frame_part(part)
        return pltpu.make_async_copy(frames_ref.at[ts], f_buf.at[ts], f_sem.at[part])

    loads = [(h0_ref, seq_ref.at[steps - 1]), (c0_ref, cout_ref), (w_rec_ref, w_buf.at[pl.ds(0, 9 * hid)]), (bias_ref, bias_buf)]
    loads += [(w_in_ref.at[pl.ds(packed * dy, packed)], w_buf.at[pl.ds(9 * hid + 128 * dy, packed)]) for dy in range(3)]
    loads = [pltpu.make_async_copy(src, dst, arg_sem.at[k]) for k, (src, dst) in enumerate(loads)]
    frame_load(0).start()
    for load in loads:
        load.start()
    frame_load(1).start()
    for ref in (row_recv, col_recv, corner_recv, crow_recv, ccol_recv, f_side):
        ref[...] = jnp.zeros_like(ref)
    for slot in range(2):
        x_buf[slot, pl.ds(0, 2 * PITCH), :] = jnp.zeros((2 * PITCH, hid), F32)
        x_buf[slot, pl.ds((rows + 2) * PITCH, 10 * PITCH), :] = jnp.zeros((10 * PITCH, hid), F32)
    for slot in range(4):
        p_buf[slot, pl.ds(0, 2 * PITCH), :] = jnp.zeros((2 * PITCH, 128), F32)
        p_buf[slot, pl.ds((rows + 2) * PITCH, 10 * PITCH), :] = jnp.zeros((10 * PITCH, 128), F32)
    ring_col[...] = jnp.zeros_like(ring_col)

    barrier = pltpu.get_barrier_semaphore()
    count = jnp.int32(0)
    for d in range(8):
        @pl.when(exists(d))
        def _():
            pl.semaphore_signal(barrier, inc=1, device_id=device(d), device_id_type=MESH)
        count = count + exists(d).astype(jnp.int32)
    pl.semaphore_wait(barrier, count)

    def send_sides(part):
        frame_load(part).wait()
        for d in (2, 3):
            @pl.when(exists(d))
            def _():
                frame_side(part, d).start()

    def receive_sides(part):
        for d in (2, 3):
            @pl.when(exists(d))
            def _():
                frame_side(part, d, True).wait_recv()

    send_sides(0)
    loads[0].wait()
    for r in range(rows):
        x_buf[0, pl.ds(cell(r, 0), cols), :] = seq_ref[steps - 1, r].astype(F32)
    loads[1].wait()
    for r in range(2, rows - 2):
        c_main[pl.ds((r - 2) * width, width), :] = cout_ref[pl.ds(r * cols + SIDE, width), :]
    for i, c in enumerate(side_cols):
        c_col[pl.ds(i * rows, rows), :] = cout_ref[pl.ds(c, rows, stride=cols), :]
    for i, r in enumerate(edge_rows):
        c_row[pl.ds(i * cols, cols), :] = cout_ref[pl.ds(r * cols, cols), :]
    send_sides(1)

    lane = lax.broadcasted_iota(jnp.int32, (1, gates_n), 1)
    scale = jnp.where(lane < 3 * hid, 0.5, 1.0)
    for load in loads[2:]:
        load.wait()
    for at in range(0, 9 * hid, 128):
        w_buf[pl.ds(at, 128), :] = (w_buf[pl.ds(at, 128), :].astype(F32) * scale).astype(BF16)
    bias = bias_buf[...] * scale
    b0 = bias.astype(BF16).astype(F32)
    b1 = (bias - b0).astype(BF16).astype(F32)
    b2 = bias - b0 - b1
    row = lax.broadcasted_iota(jnp.int32, (16, gates_n), 0)
    bias_rows = jnp.where(row == 0, b0, jnp.where(row == 1, b1, jnp.where(row == 2, b2, 0.0)))
    for dy in range(3):
        at = 9 * hid + 128 * dy
        w_buf[pl.ds(at, packed), :] = (w_buf[pl.ds(at, packed), :].astype(F32) * scale).astype(BF16)
        w_buf[pl.ds(at + packed, 128 - packed), :] = jnp.zeros((128 - packed, gates_n), BF16)
        if dy == 1:
            w_buf[pl.ds(at + packed, 16), :] = bias_rows.astype(BF16)

    row = lax.broadcasted_iota(jnp.int32, (128 - packed, rows), 0)
    ones = jnp.where(row < 3, 1.0, 0.0).astype(BF16)

    def pack_frame(t, slot):
        for c in range(-1, cols + 1):
            pieces = []
            for k in range(c - 1, c + 2):
                if k < 0:
                    pieces.append(f_side[0, t, k + 2])
                elif k < cols:
                    pieces.append(f_buf[t, k])
                else:
                    pieces.append(f_side[1, t, k - cols])
            window = jnp.concatenate(pieces + [ones], axis=0)
            p_buf[slot, pl.ds(pcell(0, c), rows, stride=PITCH), :] = window.T.astype(F32)

    def run_index(start, length, vertical):
        return pl.ds(start, length, stride=PITCH) if vertical else pl.ds(start, length)

    def gates_of(slot, p_slot, groups):
        parts = []
        for dy in range(3):
            for dx in range(3):
                pieces = [x_buf[slot, run_index(cell(r + dy - 1, c + dx - 1), length, vertical), :]
                          for r, c, length, vertical in groups]
                parts.append(jnp.concatenate(pieces, axis=0) if len(pieces) > 1 else pieces[0])
        for dy in range(3):
            pieces = [p_buf[p_slot, run_index(pcell(r + dy - 1, c), length, vertical), :]
                      for r, c, length, vertical in groups]
            parts.append(jnp.concatenate(pieces, axis=0) if len(pieces) > 1 else pieces[0])
        lhs = jnp.concatenate(parts, axis=1).astype(BF16)
        return jnp.dot(lhs, w_buf[...], preferred_element_type=F32)

    def finish(slot, groups, gates, c_ref, c_at, mask=None):
        index = pl.ds(c_at, gates.shape[0])
        c_prev = c_ref[index, :]
        gi, gf, go, gg = (jnp.tanh(gates[:, hid * k:hid * (k + 1)]) for k in range(4))
        c_next = 0.5 * ((gf * c_prev + c_prev) + (gi * gg + gg))
        h = (0.5 * go + 0.5) * jnp.tanh(c_next)
        if mask is None:
            c_ref[index, :] = c_next
        else:
            h = h * mask
        at = 0
        for r, c, length, vertical in groups:
            x_buf[1 - slot, run_index(cell(r, c), length, vertical), :] = h[at:at + length]
            at += length

    def update(slot, p_slot, groups, c_ref, c_at):
        finish(slot, groups, gates_of(slot, p_slot, groups), c_ref, c_at)

    def stage(slot, p_first):
        state = x_buf.at[0]
        for k, r in enumerate((0, rows - 2)):
            for n in range(2):
                row_send[slot, k, n * cols:(n + 1) * cols] = state[pl.ds(cell(r + n, 0), cols), :].astype(BF16)
            at = 2 * cols
            row_send[slot, k, at:at + 2 * PITCH] = p_buf[p_first, pl.ds(pcell(r, -1), 2 * PITCH), :].astype(BF16)
            at += 2 * PITCH
            r_one = 0 if k == 0 else rows - 1
            row_send[slot, k, at:at + PITCH] = p_buf[p_first + 1, pl.ds(pcell(r_one, -1), PITCH), :].astype(BF16)
            crow_send[slot, k] = c_row[pl.ds((0 if k == 0 else 3) * cols, cols), :]
        for k, c in enumerate((0, cols - 2)):
            for n in range(2):
                col_send[slot, k, n] = state[pl.ds(cell(0, c + n), rows, stride=PITCH), :].astype(BF16)
            ccol_send[slot, k] = c_col[pl.ds((0 if k == 0 else last) * rows, rows), :]
        for k, (dr, dc) in enumerate(DIRECTIONS[4:]):
            r, c = (0 if dr < 0 else rows - 2), (0 if dc < 0 else cols - 2)
            for n in range(2):
                corner = state[pl.ds(cell(r + n, c), 2), :].astype(BF16).astype(F32)
                corner_send[slot, k, 2 * n:2 * n + 2] = corner
            c_at = (0 if dr < 0 else 3 * cols) + (0 if dc < 0 else cols - 1)
            corner_send[slot, k, 4:5] = c_row[pl.ds(c_at, 1), :]

    def each_copy(act, slot, wanted=None):
        for kind in range(2):
            for d in range(8 if kind == 0 else 4):
                @pl.when(exists(d) if wanted is None else jnp.logical_and(exists(d), wanted))
                def _():
                    act(slot, d, kind)

    def send_halo(slot, wanted=None):
        each_copy(lambda *which: departure(*which).start(), slot, wanted)

    def receive_halo(slot):
        each_copy(lambda *which: arrival(*which).wait_recv(), slot)

    def wait_sent(slot):
        each_copy(lambda *which: departure(*which).wait_send(), slot)

    def unpack_halo(slot, p_first):
        state = x_buf.at[0]
        for k, r in enumerate((-2, rows)):
            for n in range(2):
                state[pl.ds(cell(r + n, 0), cols), :] = row_recv[slot, k, n * cols:(n + 1) * cols].astype(F32)
            at = 2 * cols
            p_buf[p_first, pl.ds(pcell(r, -1), 2 * PITCH), :] = row_recv[slot, k, at:at + 2 * PITCH].astype(F32)
            at += 2 * PITCH
            r_one = -1 if k == 0 else rows
            p_buf[p_first + 1, pl.ds(pcell(r_one, -1), PITCH), :] = row_recv[slot, k, at:at + PITCH].astype(F32)
            ring_row[pl.ds(k * cols, cols), :] = crow_recv[slot, k]
        for k, c in enumerate((-2, cols)):
            for n in range(2):
                state[pl.ds(cell(0, c + n), rows, stride=PITCH), :] = col_recv[slot, k, n].astype(F32)
            ring_col[pl.ds(k * long + 1, rows), :] = ccol_recv[slot, k]
        for k, (dr, dc) in enumerate(DIRECTIONS[4:]):
            r, c = (-2 if dr < 0 else rows), (-2 if dc < 0 else cols)
            for n in range(2):
                state[pl.ds(cell(r + n, c), 2), :] = corner_recv[slot, k, 2 * n:2 * n + 2]
            at = (0 if dc < 0 else long) + (0 if dr < 0 else rows + 1)
            ring_col[pl.ds(at, 1), :] = corner_recv[slot, k, 4:5]

    def write_out(t, slot):
        for r in range(rows):
            seq_ref[t, r] = x_buf[slot, pl.ds(cell(r, 0), cols), :].astype(BF16)

    def main_run(first, last):
        return [(r, SIDE, width, False) for r in range(first, last)]

    def main_rows(slot, p_slot, first, last):
        update(slot, p_slot, main_run(first, last), c_main, (first - 2) * width)

    def side_run(*ids):
        return [(0, side_cols[i], rows, True) for i in ids]

    there = [jnp.where(exists(d), 1.0, 0.0).astype(F32) for d in range(4)]
    place = lax.broadcasted_iota(jnp.int32, (long, hid), 0)
    ends = jnp.where(place == 0, there[0], jnp.where(place == rows + 1, there[1], 1.0))
    ring_mask = jnp.concatenate([ends * there[2], ends * there[3],
                                 jnp.full((cols, hid), 1.0, F32) * there[0], jnp.full((cols, hid), 1.0, F32) * there[1]],
                                axis=0)
    ring_col_run = [(-1, -1, long, True), (-1, cols, long, True)]
    ring_row_run = [(-1, 0, cols, False), (rows, 0, cols, False)]
    row_run = [(r, 0, cols, False) for r in edge_rows]
    n_long = 2 * long

    def pair(m, now):
        t = 2 * m
        pa = 2 * now
        other = 2 * (1 - now)
        pack_frame(jnp.minimum(t + 2, steps - 2), other)
        pack_frame(jnp.minimum(t + 3, steps - 1), other + 1)
        write_out(jnp.maximum(t - 1, 0), 0)
        for at in range(2, rows - 2, BLOCK):
            main_rows(0, pa, at, at + BLOCK)
        update(0, pa, side_run(1, 2, 3), c_col, rows)
        update(0, pa, side_run(last - 3, last - 2, last - 1), c_col, (last - 3) * rows)

        @pl.when(m >= 1)
        def _():
            wait_sent(1 - now)
        receive_halo(now)
        unpack_halo(now, pa)

        own = side_run(0) + side_run(last) + row_run
        own_gates = gates_of(0, pa, own)
        ring_gates = gates_of(0, pa, ring_col_run + ring_row_run)
        beside = gates_of(1, pa + 1, main_run(13, 21))
        finish(0, side_run(0), own_gates[:rows], c_col, 0)
        finish(0, side_run(last), own_gates[rows:2 * rows], c_col, last * rows)
        finish(0, row_run, own_gates[2 * rows:], c_row, 0)
        finish(0, ring_col_run, ring_gates[:n_long], ring_col, 0, ring_mask[:n_long])
        finish(0, ring_row_run, ring_gates[n_long:], ring_row, 0, ring_mask[n_long:])
        for i, r in ((0, 0), (3, rows - 1)):
            for first in (1, last - 3):
                c_col[pl.ds(first * rows + r, 3, stride=rows), :] = c_row[pl.ds(i * cols + side_cols[first], 3), :]
        finish(1, main_run(13, 21), beside, c_main, (13 - 2) * width)
        left = side_run(0, 1) + side_run(last - 1, last)
        edge_gates = gates_of(1, pa + 1, left + row_run)
        beside = gates_of(1, pa + 1, main_run(21, 29))
        finish(1, side_run(0, 1), edge_gates[:2 * rows], c_col, 0)
        finish(1, side_run(last - 1, last), edge_gates[2 * rows:4 * rows], c_col, (last - 1) * rows)
        finish(1, row_run, edge_gates[4 * rows:], c_row, 0)
        stage(1 - now, other)
        send_halo(1 - now, t + 2 < steps)

        finish(1, main_run(21, 29), beside, c_main, (21 - 2) * width)
        write_out(t, 1)
        main_rows(1, pa + 1, 2, 13)
        main_rows(1, pa + 1, 29, 38)
        main_rows(1, pa + 1, 38, 46)
        update(1, pa + 1, side_run(2, 3), c_col, 2 * rows)
        update(1, pa + 1, side_run(last - 3, last - 2), c_col, (last - 3) * rows)

    receive_sides(0)
    pack_frame(0, 0)
    pack_frame(1, 1)
    stage(0, 0)
    send_halo(0)
    receive_sides(1)

    def trip(i, carry):
        pair(2 * i, 0)
        pair(2 * i + 1, 1)
        return carry

    lax.fori_loop(0, steps // 4, trip, 0)

    write_out(steps - 1, 0)
    for r in range(2, rows - 2):
        cout_ref[pl.ds(r * cols + SIDE, width), :] = c_main[pl.ds((r - 2) * width, width), :]
    for i, c in enumerate(side_cols):
        cout_ref[pl.ds(c, rows, stride=cols), :] = c_col[pl.ds(i * rows, rows), :]
    for i, r in enumerate(edge_rows):
        cout_ref[pl.ds(r * cols, cols), :] = c_row[pl.ds(i * cols, cols), :]
    wait_sent(1)
    for part in (0, 1):
        for d in (2, 3):
            @pl.when(exists(d))
            def _():
                frame_side(part, d).wait_send()


def write_back(seq_in, c_in, seq_out, c_out, sem):
    copies = [pltpu.make_async_copy(seq_in.at[pl.ds(t, CHUNK)], seq_out.at[pl.ds(t, CHUNK)], sem.at[1 + t // CHUNK])
              for t in range(0, seq_in.shape[0], CHUNK)]
    copies.append(pltpu.make_async_copy(c_in, c_out, sem.at[0]))
    for copy in copies:
        copy.start()
    for copy in copies:
        copy.wait()


def solution(mesh):
    n_rows = mesh.shape["rows"]
    n_cols = mesh.shape["cols"]
    seq_spec = P(None, "dp", "rows", "cols", None)
    state_spec = P("dp", "rows", "cols", None)

    def local_run(frames, w_in, w_rec, gate_bias, h_init, c_init):
        steps, _, rows, cols, c_in = frames.shape
        hid = h_init.shape[-1]
        row_words = 2 * cols + 3 * PITCH + 4
        both = (2, 2)
        vmem = pl.BlockSpec(memory_space=pltpu.VMEM)
        args = (jnp.transpose(frames[:, 0], (0, 2, 3, 1)), w_rec.reshape(9 * hid, 4 * hid),
                w_in.reshape(9 * c_in, 4 * hid), gate_bias.reshape(1, 4 * hid), h_init[0],
                c_init[0].reshape(rows * cols, hid))
        hbm = pl.BlockSpec(memory_space=pltpu.HBM)
        seq, c_last = pl.pallas_call(
            functools.partial(kernel, steps, rows, cols, n_rows, n_cols, c_in),
            out_shape=(jax.ShapeDtypeStruct((steps, rows, cols, hid), BF16),
                       jax.ShapeDtypeStruct((rows * cols, hid), F32)),
            in_specs=[hbm] * 6,
            out_specs=(vmem, vmem),
            scratch_shapes=[
                pltpu.VMEM((2, (rows + 12) * PITCH, hid), F32),
                pltpu.VMEM((4, (rows + 12) * PITCH, 128), F32),
                pltpu.VMEM((9 * hid + 3 * 128, 4 * hid), BF16),
                pltpu.VMEM((1, 4 * hid), F32),
                pltpu.VMEM((steps, cols, c_in, rows), BF16),
                pltpu.VMEM((2, steps, 2, c_in, rows), BF16),
                pltpu.VMEM(((rows - 4) * (cols - 2 * SIDE), hid), F32),
                pltpu.VMEM((rows * 2 * SIDE, hid), F32),
                pltpu.VMEM((cols * 4, hid), F32),
                pltpu.VMEM((cols * 2, hid), F32),
                pltpu.VMEM(((rows + 8) * 2, hid), F32),
                pltpu.VMEM((*both, row_words, hid), BF16),
                pltpu.VMEM((*both, 2, rows, hid), BF16),
                pltpu.VMEM((2, 4, 8, hid), F32),
                pltpu.VMEM((*both, cols, hid), F32),
                pltpu.VMEM((*both, rows, hid), F32),
                pltpu.VMEM((*both, row_words, hid), BF16),
                pltpu.VMEM((*both, 2, rows, hid), BF16),
                pltpu.VMEM((2, 4, 8, hid), F32),
                pltpu.VMEM((*both, cols, hid), F32),
                pltpu.VMEM((*both, rows, hid), F32),
                pltpu.SemaphoreType.DMA((*both, 8)),
                pltpu.SemaphoreType.DMA((*both, 8)),
                pltpu.SemaphoreType.DMA((2,)),
                pltpu.SemaphoreType.DMA(both),
                pltpu.SemaphoreType.DMA(both),
                pltpu.SemaphoreType.DMA((7,)),
            ],
            compiler_params=pltpu.CompilerParams(
                collective_id=0, has_side_effects=True, vmem_limit_bytes=24 * 2**20),
            name="convlstm",
        )(*(pltpu.with_memory_space_constraint(x, pltpu.HBM) for x in args))
        seq, c_last = pl.pallas_call(
            write_back,
            out_shape=(jax.ShapeDtypeStruct(seq.shape, BF16), jax.ShapeDtypeStruct(c_last.shape, F32)),
            in_specs=[vmem] * 2,
            out_specs=(hbm, hbm),
            scratch_shapes=[pltpu.SemaphoreType.DMA((2 + steps // CHUNK,))],
            compiler_params=pltpu.CompilerParams(vmem_limit_bytes=2**20),
            name="write_back",
        )(seq, c_last)
        return seq[:, None], c_last.reshape(c_init.shape)

    return jax.shard_map(local_run, mesh=mesh, in_specs=(seq_spec, P(), P(), P(), state_spec, state_spec),
                         out_specs=(seq_spec, state_spec), check_vma=False)
```

```python
import functools

import jax
import jax.numpy as jnp
from jax import lax
from jax.experimental import pallas as pl
from jax.experimental.pallas import tpu as pltpu
from jax.sharding import PartitionSpec as P

MESH = pl.DeviceIdType.MESH
LANES = 128
BF16 = jnp.bfloat16
F32 = jnp.float32
TDT = jnp.bfloat16

PITCH = 36
DIRECTIONS = ((-1, 0), (1, 0), (0, -1), (0, 1), (-1, -1), (-1, 1), (1, -1), (1, 1))
CHUNK = 2
FIRST, STOP = 13, 29
BLOCK = 11
SIDE = 4


def cell(r, c):
    return (r + 2) * PITCH + c + 2


def pcell(r, c):
    return (r + 2) * PITCH + c + 1


def exists(d, n_rows, n_cols):
    dr, dc = DIRECTIONS[d]
    ok = None
    for here, step, count in ((lax.axis_index("rows"), dr, n_rows), (lax.axis_index("cols"), dc, n_cols)):
        if step:
            this = (here > 0) if step < 0 else (here < count - 1)
            ok = this if ok is None else jnp.logical_and(ok, this)
    return ok


class Tile:
    def __init__(self, sizes, x_buf, p_buf, w_buf, c_main, c_col, c_row, ring_row, ring_col):
        self.steps, self.rows, self.cols, self.n_rows, self.n_cols, self.c_in = sizes
        self.x_buf, self.p_buf, self.w_buf = x_buf, p_buf, w_buf
        self.c_main, self.c_col, self.c_row = c_main, c_col, c_row
        self.ring_row, self.ring_col = ring_row, ring_col
        self.hid = x_buf.shape[-1]
        self.width = self.cols - 2 * SIDE
        self.long = self.rows + 8
        self.side_cols = tuple(range(SIDE)) + tuple(range(self.cols - SIDE, self.cols))
        self.edge_rows = (0, 1, self.rows - 2, self.rows - 1)
        self.last = len(self.side_cols) - 1

    def run_index(self, start, length, vertical):
        return pl.ds(start, length, stride=PITCH) if vertical else pl.ds(start, length)

    def gates_of(self, slot, p_slot, groups):
        parts = []
        for dy in range(3):
            for dx in range(3):
                pieces = [self.x_buf[slot, self.run_index(cell(r + dy - 1, c + dx - 1), length, vertical), :]
                          for r, c, length, vertical in groups]
                parts.append(jnp.concatenate(pieces, axis=0) if len(pieces) > 1 else pieces[0])
        for dy in range(3):
            pieces = [self.p_buf[p_slot, self.run_index(pcell(r + dy - 1, c), length, vertical), :]
                      for r, c, length, vertical in groups]
            parts.append(jnp.concatenate(pieces, axis=0) if len(pieces) > 1 else pieces[0])
        lhs = jnp.concatenate(parts, axis=1).astype(BF16)
        return jnp.dot(lhs, self.w_buf[...], preferred_element_type=F32)

    def finish(self, slot, groups, gates, c_ref, c_at, mask=None):
        index = pl.ds(c_at, gates.shape[0])
        c_prev = c_ref[index, :]
        gi, gf, go, gg = (jnp.tanh(gates[:, self.hid * k:self.hid * (k + 1)]) for k in range(4))
        c_next = 0.5 * ((gf * c_prev + c_prev) + (gi * gg + gg))
        h = (0.5 * go + 0.5) * jnp.tanh(c_next)
        if mask is None:
            c_ref[index, :] = c_next
        else:
            h = h * mask
        at = 0
        for r, c, length, vertical in groups:
            self.x_buf[1 - slot, self.run_index(cell(r, c), length, vertical), :] = h[at:at + length]
            at += length

    def update(self, slot, p_slot, groups, c_ref, c_at):
        self.finish(slot, groups, self.gates_of(slot, p_slot, groups), c_ref, c_at)

    def main_run(self, first, stop):
        return [(r, SIDE, self.width, False) for r in range(first, stop)]

    def side_run(self, *ids):
        return [(0, self.side_cols[i], self.rows, True) for i in ids]

    def main_rows(self, slot, p_slot, first, stop):
        self.update(slot, p_slot, self.main_run(first, stop), self.c_main, (first - 2) * self.width)

    def write_out(self, slot, ref):
        for r in range(self.rows):
            ref[r] = self.x_buf[slot, pl.ds(cell(r, 0), self.cols), :].astype(BF16)

    def before_wait(self, pa, write):
        rows, last = self.rows, self.last
        for at in range(2, rows - 2, BLOCK):
            self.main_rows(0, pa, at, at + BLOCK)
        self.update(0, pa, self.side_run(1, 2, 3), self.c_col, rows)
        self.update(0, pa, self.side_run(last - 3, last - 2, last - 1), self.c_col, (last - 3) * rows)
        write()
        for first, stop in ((3, FIRST), (STOP, rows - 11), (rows - 11, rows - 3)):
            self.main_rows(1, pa + 1, first, stop)

    def after_wait(self, pa, send):
        rows, cols, last = self.rows, self.cols, self.last
        there = [jnp.where(exists(d, self.n_rows, self.n_cols), 1.0, 0.0).astype(F32) for d in range(4)]
        place = lax.broadcasted_iota(jnp.int32, (self.long, self.hid), 0)
        ends = jnp.where(place == 0, there[0], jnp.where(place == rows + 1, there[1], 1.0))
        ring_col_run = [(-1, -1, self.long, True), (-1, cols, self.long, True)]
        ring_row_run = [(-1, 0, cols, False), (rows, 0, cols, False)]
        row_run = [(r, 0, cols, False) for r in self.edge_rows]
        n_long = 2 * self.long
        middle = (FIRST + STOP) // 2
        c_col, c_row, c_main, finish = self.c_col, self.c_row, self.c_main, self.finish

        own = self.side_run(0) + self.side_run(last) + row_run
        own_gates = self.gates_of(0, pa, own)
        ring_gates = self.gates_of(0, pa, ring_col_run + ring_row_run)
        run = self.main_run(FIRST, middle)
        beside = self.gates_of(1, pa + 1, run)
        finish(0, self.side_run(0), own_gates[:rows], c_col, 0)
        finish(0, self.side_run(last), own_gates[rows:2 * rows], c_col, last * rows)
        finish(0, row_run, own_gates[2 * rows:], c_row, 0)
        mask = jnp.concatenate([ends * there[2], ends * there[3]], axis=0)
        finish(0, ring_col_run, ring_gates[:n_long], self.ring_col, 0, mask)
        mask = jnp.concatenate([jnp.full((cols, self.hid), 1.0, F32) * there[k] for k in range(2)], axis=0)
        finish(0, ring_row_run, ring_gates[n_long:], self.ring_row, 0, mask)
        for i, r in ((0, 0), (3, rows - 1)):
            for first in (1, last - 3):
                c_col[pl.ds(first * rows + r, 3, stride=rows), :] = c_row[pl.ds(i * cols + self.side_cols[first], 3), :]
        finish(1, run, beside, c_main, (FIRST - 2) * self.width)
        edge_gates = self.gates_of(1, pa + 1, self.side_run(0, 1, last - 1, last) + row_run)
        run = self.main_run(middle, STOP)
        beside = self.gates_of(1, pa + 1, run)
        finish(1, self.side_run(0, 1), edge_gates[:2 * rows], c_col, 0)
        finish(1, self.side_run(last - 1, last), edge_gates[2 * rows:4 * rows], c_col, (last - 1) * rows)
        finish(1, row_run, edge_gates[4 * rows:], c_row, 0)
        send()

        finish(1, run, beside, c_main, (middle - 2) * self.width)
        runs = [(self.side_run(2, 3), c_col, 2 * rows), (self.side_run(last - 3, last - 2), c_col, (last - 3) * rows),
                (self.main_run(2, 3), c_main, 0), (self.main_run(rows - 3, rows - 2), c_main, (rows - 5) * self.width)]
        gates = self.gates_of(1, pa + 1, sum((run for run, _, _ in runs), []))
        at = 0
        for run, c_ref, c_at in runs:
            size = sum(length for _, _, length, _ in run)
            finish(1, run, gates[at:at + size], c_ref, c_at)
            at += size


def kernel(sizes, frames_ref, w_rec_ref, w_in_ref, bias_ref, h0_ref, c0_ref,
           seq_ref, x_buf, p_buf, w_buf, c_main, c_col, c_row, ring_row, ring_col,
           bias_buf, f_buf, f_side, c_buf, row_send, col_send, corner_send, crow_send, ccol_send,
           row_recv, col_recv, corner_recv, crow_recv, ccol_recv,
           send_sem, recv_sem, f_sem, f_send_sem, f_recv_sem, arg_sem):
    tile = Tile(sizes, x_buf, p_buf, w_buf, c_main, c_col, c_row, ring_row, ring_col)
    steps, rows, cols, n_rows, n_cols, c_in = sizes
    hid, width, long, last = tile.hid, tile.width, tile.long, tile.last
    side_cols, edge_rows = tile.side_cols, tile.edge_rows
    gates_n = 4 * hid
    packed = 3 * c_in
    my_row = lax.axis_index("rows")
    my_col = lax.axis_index("cols")

    def device(d):
        dr, dc = DIRECTIONS[d]
        return {"rows": my_row + dr, "cols": my_col + dc}

    def opposite(d):
        return DIRECTIONS.index((-DIRECTIONS[d][0], -DIRECTIONS[d][1]))

    def source(slot, d, kind):
        dr, dc = DIRECTIONS[d]
        if dr and dc:
            return corner_send.at[slot, d - 4]
        if dr:
            return (crow_send if kind else row_send).at[slot, d]
        return (ccol_send if kind else col_send).at[slot, d - 2]

    def landing(slot, d, kind):
        dr, dc = DIRECTIONS[d]
        if dr and dc:
            return corner_recv.at[slot, d - 4]
        if dr:
            return (crow_recv if kind else row_recv).at[slot, d]
        return (ccol_recv if kind else col_recv).at[slot, d - 2]

    def departure(slot, d, kind):
        return pltpu.make_async_remote_copy(
            src_ref=source(slot, d, kind), dst_ref=landing(slot, opposite(d), kind), send_sem=send_sem.at[slot, kind, d],
            recv_sem=recv_sem.at[slot, kind, opposite(d)], device_id=device(d), device_id_type=MESH)

    def arrival(slot, d, kind):
        return pltpu.make_async_remote_copy(
            src_ref=source(slot, d, kind), dst_ref=landing(slot, d, kind), send_sem=send_sem.at[slot, kind, d],
            recv_sem=recv_sem.at[slot, kind, d], device_id=device(d), device_id_type=MESH)

    def frame_part(part):
        return pl.ds(0, 2) if part == 0 else pl.ds(2, steps - 2)

    def frame_side(part, d, arriving=False):
        ts = frame_part(part)
        k = d - 2
        at = k if arriving else 1 - k
        return pltpu.make_async_remote_copy(
            src_ref=f_buf.at[ts, pl.ds(0 if k == 0 else cols - 2, 2)], dst_ref=f_side.at[at, ts],
            send_sem=f_send_sem.at[part, k], recv_sem=f_recv_sem.at[part, at], device_id=device(d), device_id_type=MESH)

    def frame_load(part):
        ts = frame_part(part)
        return pltpu.make_async_copy(frames_ref.at[ts], f_buf.at[ts], f_sem.at[part])

    loads = [(h0_ref, seq_ref.at[steps - 1]), (c0_ref, c_buf), (w_rec_ref, w_buf.at[pl.ds(0, 9 * hid)]), (bias_ref, bias_buf)]
    loads += [(w_in_ref.at[pl.ds(packed * dy, packed)], w_buf.at[pl.ds(9 * hid + LANES * dy, packed)]) for dy in range(3)]
    loads = [pltpu.make_async_copy(src, dst, arg_sem.at[k]) for k, (src, dst) in enumerate(loads)]
    frame_load(0).start()
    for load in loads:
        load.start()
    frame_load(1).start()
    for ref in (row_recv, col_recv, corner_recv, crow_recv, ccol_recv, f_side):
        ref[...] = jnp.zeros_like(ref)
    for slot in range(2):
        x_buf[slot, pl.ds(0, 2 * PITCH), :] = jnp.zeros((2 * PITCH, hid), F32)
        x_buf[slot, pl.ds((rows + 2) * PITCH, 10 * PITCH), :] = jnp.zeros((10 * PITCH, hid), F32)
    for slot in range(4):
        p_buf[slot, pl.ds(0, 2 * PITCH), :] = jnp.zeros((2 * PITCH, LANES), F32)
        p_buf[slot, pl.ds((rows + 2) * PITCH, 10 * PITCH), :] = jnp.zeros((10 * PITCH, LANES), F32)
    ring_col[...] = jnp.zeros_like(ring_col)

    barrier = pltpu.get_barrier_semaphore()
    count = jnp.int32(0)
    for d in range(8):
        @pl.when(exists(d, n_rows, n_cols))
        def _():
            pl.semaphore_signal(barrier, inc=1, device_id=device(d), device_id_type=MESH)
        count = count + exists(d, n_rows, n_cols).astype(jnp.int32)
    pl.semaphore_wait(barrier, count)

    def send_sides(part):
        frame_load(part).wait()
        for d in (2, 3):
            @pl.when(exists(d, n_rows, n_cols))
            def _():
                frame_side(part, d).start()

    def receive_sides(part):
        for d in (2, 3):
            @pl.when(exists(d, n_rows, n_cols))
            def _():
                frame_side(part, d, True).wait_recv()

    send_sides(0)
    loads[0].wait()
    for r in range(rows):
        x_buf[0, pl.ds(cell(r, 0), cols), :] = seq_ref[steps - 1, r].astype(F32)
    loads[1].wait()
    for r in range(2, rows - 2):
        c_main[pl.ds((r - 2) * width, width), :] = c_buf[pl.ds(r * cols + SIDE, width), :]
    for i, c in enumerate(side_cols):
        c_col[pl.ds(i * rows, rows), :] = c_buf[pl.ds(c, rows, stride=cols), :]
    for i, r in enumerate(edge_rows):
        c_row[pl.ds(i * cols, cols), :] = c_buf[pl.ds(r * cols, cols), :]
    send_sides(1)

    lane = lax.broadcasted_iota(jnp.int32, (1, gates_n), 1)
    scale = jnp.where(lane < 3 * hid, 0.5, 1.0)
    for load in loads[2:]:
        load.wait()
    for at in range(0, 9 * hid, LANES):
        w_buf[pl.ds(at, LANES), :] = (w_buf[pl.ds(at, LANES), :].astype(F32) * scale).astype(BF16)
    bias = bias_buf[...] * scale
    b0 = bias.astype(BF16).astype(F32)
    b1 = (bias - b0).astype(BF16).astype(F32)
    b2 = bias - b0 - b1
    row = lax.broadcasted_iota(jnp.int32, (16, gates_n), 0)
    bias_rows = jnp.where(row == 0, b0, jnp.where(row == 1, b1, jnp.where(row == 2, b2, 0.0)))
    for dy in range(3):
        at = 9 * hid + LANES * dy
        w_buf[pl.ds(at, packed), :] = (w_buf[pl.ds(at, packed), :].astype(F32) * scale).astype(BF16)
        w_buf[pl.ds(at + packed, LANES - packed), :] = jnp.zeros((LANES - packed, gates_n), BF16)
        if dy == 1:
            w_buf[pl.ds(at + packed, 16), :] = bias_rows.astype(BF16)

    row = lax.broadcasted_iota(jnp.int32, (LANES - packed, rows), 0)
    ones = jnp.where(row < 3, 1.0, 0.0).astype(BF16)

    def pack_frame(t, slot):
        for c in range(-1, cols + 1):
            pieces = []
            for k in range(c - 1, c + 2):
                if k < 0:
                    pieces.append(f_side[0, t, k + 2])
                elif k < cols:
                    pieces.append(f_buf[t, k])
                else:
                    pieces.append(f_side[1, t, k - cols])
            window = jnp.concatenate(pieces + [ones], axis=0)
            p_buf[slot, pl.ds(pcell(0, c), rows, stride=PITCH), :] = window.T.astype(F32)

    def stage(slot, p_first):
        state = x_buf.at[0]
        for k, r in enumerate((0, rows - 2)):
            for n in range(2):
                row_send[slot, k, n * cols:(n + 1) * cols] = state[pl.ds(cell(r + n, 0), cols), :].astype(BF16)
            at = 2 * cols
            row_send[slot, k, at:at + 2 * PITCH] = p_buf[p_first, pl.ds(pcell(r, -1), 2 * PITCH), :].astype(BF16)
            at += 2 * PITCH
            r_one = 0 if k == 0 else rows - 1
            row_send[slot, k, at:at + PITCH] = p_buf[p_first + 1, pl.ds(pcell(r_one, -1), PITCH), :].astype(BF16)
            crow_send[slot, k] = c_row[pl.ds((0 if k == 0 else 3) * cols, cols), :]
        for k, c in enumerate((0, cols - 2)):
            for n in range(2):
                col_send[slot, k, n] = state[pl.ds(cell(0, c + n), rows, stride=PITCH), :].astype(BF16)
            ccol_send[slot, k] = c_col[pl.ds((0 if k == 0 else last) * rows, rows), :]
        for k, (dr, dc) in enumerate(DIRECTIONS[4:]):
            r, c = (0 if dr < 0 else rows - 2), (0 if dc < 0 else cols - 2)
            for n in range(2):
                corner = state[pl.ds(cell(r + n, c), 2), :].astype(BF16).astype(F32)
                corner_send[slot, k, 2 * n:2 * n + 2] = corner
            c_at = (0 if dr < 0 else 3 * cols) + (0 if dc < 0 else cols - 1)
            corner_send[slot, k, 4:5] = c_row[pl.ds(c_at, 1), :]

    def each_copy(act, slot, wanted=None):
        for kind in range(2):
            for d in range(8 if kind == 0 else 4):
                @pl.when(exists(d, n_rows, n_cols) if wanted is None else jnp.logical_and(exists(d, n_rows, n_cols), wanted))
                def _():
                    act(slot, d, kind)

    def send_halo(slot, wanted=None):
        each_copy(lambda *which: departure(*which).start(), slot, wanted)

    def receive_halo(slot):
        each_copy(lambda *which: arrival(*which).wait_recv(), slot)

    def wait_sent(slot):
        each_copy(lambda *which: departure(*which).wait_send(), slot)

    def unpack_halo(slot, p_first):
        state = x_buf.at[0]
        for k, r in enumerate((-2, rows)):
            for n in range(2):
                state[pl.ds(cell(r + n, 0), cols), :] = row_recv[slot, k, n * cols:(n + 1) * cols].astype(F32)
            at = 2 * cols
            p_buf[p_first, pl.ds(pcell(r, -1), 2 * PITCH), :] = row_recv[slot, k, at:at + 2 * PITCH].astype(F32)
            at += 2 * PITCH
            r_one = -1 if k == 0 else rows
            p_buf[p_first + 1, pl.ds(pcell(r_one, -1), PITCH), :] = row_recv[slot, k, at:at + PITCH].astype(F32)
            ring_row[pl.ds(k * cols, cols), :] = crow_recv[slot, k]
        for k, c in enumerate((-2, cols)):
            for n in range(2):
                state[pl.ds(cell(0, c + n), rows, stride=PITCH), :] = col_recv[slot, k, n].astype(F32)
            ring_col[pl.ds(k * long + 1, rows), :] = ccol_recv[slot, k]
        for k, (dr, dc) in enumerate(DIRECTIONS[4:]):
            r, c = (-2 if dr < 0 else rows), (-2 if dc < 0 else cols)
            for n in range(2):
                state[pl.ds(cell(r + n, c), 2), :] = corner_recv[slot, k, 2 * n:2 * n + 2]
            at = (0 if dc < 0 else long) + (0 if dr < 0 else rows + 1)
            ring_col[pl.ds(at, 1), :] = corner_recv[slot, k, 4:5]

    receive_sides(0)
    pack_frame(0, 0)
    pack_frame(1, 1)
    stage(0, 0)
    send_halo(0)
    receive_sides(1)

    def before(m, now):
        t = 2 * m
        other = 2 * (1 - now)
        pack_frame(jnp.minimum(t + 2, steps - 2), other)
        pack_frame(jnp.minimum(t + 3, steps - 1), other + 1)
        tile.before_wait(2 * now, lambda: tile.write_out(0, seq_ref.at[jnp.maximum(t - 1, 0)]))

        @pl.when(m >= 1)
        def _():
            wait_sent(1 - now)
        receive_halo(now)
        unpack_halo(now, 2 * now)

    def pair(m, now):
        def send():
            stage(1 - now, 2 * (1 - now))
            send_halo(1 - now)

        before(m, now)
        tile.after_wait(2 * now, send)
        tile.write_out(1, seq_ref.at[2 * m])

    def trip(i, carry):
        pair(2 * i, 0)
        pair(2 * i + 1, 1)
        return carry

    n_pairs = steps // 2
    lax.fori_loop(0, (n_pairs - 1) // 2, trip, 0)
    for m in range(n_pairs - 2 + n_pairs % 2, n_pairs - 1):
        pair(m, m % 2)
    before(n_pairs - 1, (n_pairs - 1) % 2)
    wait_sent((n_pairs - 1) % 2)
    for part in (0, 1):
        for d in (2, 3):
            @pl.when(exists(d, n_rows, n_cols))
            def _():
                frame_side(part, d).wait_send()


def finish_kernel(sizes, seq_in, x_in, p_buf, w_buf, c_main_in, c_col_in, c_row_in, ring_row, ring_col,
                  seq_out, c_out, x_buf, c_main, c_col, c_row, out_buf, c_buf, sem):
    tile = Tile(sizes, x_buf, p_buf, w_buf, c_main, c_col, c_row, ring_row, ring_col)
    steps, rows, cols = sizes[:3]
    copies = [pltpu.make_async_copy(seq_in.at[pl.ds(t, CHUNK)], seq_out.at[pl.ds(t, CHUNK)], sem.at[t // CHUNK])
              for t in range(0, steps - 2, CHUNK)]
    for copy in copies:
        copy.start()
    tile.after_wait(2 * ((steps // 2 - 1) % 2), lambda: None)
    for slot in range(2):
        tile.write_out(1 - slot, out_buf.at[slot])
    for r in range(2, rows - 2):
        c_buf[pl.ds(r * cols + SIDE, tile.width), :] = c_main[pl.ds((r - 2) * tile.width, tile.width), :]
    for i, c in enumerate(tile.side_cols):
        c_buf[pl.ds(c, rows, stride=cols), :] = c_col[pl.ds(i * rows, rows), :]
    for i, r in enumerate(tile.edge_rows):
        c_buf[pl.ds(r * cols, cols), :] = c_row[pl.ds(i * cols, cols), :]
    tail = [pltpu.make_async_copy(out_buf, seq_out.at[pl.ds(steps - 2, 2)], sem.at[steps // CHUNK]),
            pltpu.make_async_copy(c_buf, c_out, sem.at[steps // CHUNK + 1])]
    for copy in tail:
        copy.start()
    for copy in copies + tail:
        copy.wait()


def solution(mesh):
    n_rows = mesh.shape["rows"]
    n_cols = mesh.shape["cols"]
    seq_spec = P(None, "dp", "rows", "cols", None)
    state_spec = P("dp", "rows", "cols", None)

    def local_run(frames, w_in, w_rec, gate_bias, h_init, c_init):
        steps, _, rows, cols, c_in = frames.shape
        hid = h_init.shape[-1]
        row_words = 2 * cols + 3 * PITCH + 4
        both = (2, 2)
        vmem = pl.BlockSpec(memory_space=pltpu.VMEM)
        args = (jnp.transpose(frames[:, 0], (0, 2, 3, 1)), w_rec.reshape(9 * hid, 4 * hid),
                w_in.reshape(9 * c_in, 4 * hid), gate_bias.reshape(1, 4 * hid), h_init[0],
                c_init[0].reshape(rows * cols, hid))
        hbm = pl.BlockSpec(memory_space=pltpu.HBM)
        sizes = (steps, rows, cols, n_rows, n_cols, c_in)

        def wide(*shape):
            return jax.ShapeDtypeStruct((*shape, hid), F32)

        state = (wide(2, (rows + 12) * PITCH), wide(4, (rows + 12) * PITCH),
                 jax.ShapeDtypeStruct((9 * hid + 3 * hid, 4 * hid), BF16), wide((rows - 4) * (cols - 2 * SIDE)),
                 wide(rows * 2 * SIDE), wide(cols * 4), wide(cols * 2), wide((rows + 8) * 2))
        seq_shape = jax.ShapeDtypeStruct((steps, rows, cols, hid), BF16)
        seq, *held = pl.pallas_call(
            functools.partial(kernel, sizes),
            out_shape=(seq_shape, *state),
            in_specs=[hbm] * 6,
            out_specs=(vmem,) * 9,
            scratch_shapes=[
                pltpu.VMEM((1, 4 * hid), F32),
                pltpu.VMEM((steps, cols, c_in, rows), BF16),
                pltpu.VMEM((2, steps, 2, c_in, rows), BF16),
                pltpu.VMEM((rows * cols, hid), F32),
                *[shape for _ in both for shape in (
                    pltpu.VMEM((*both, row_words, hid), BF16),
                    pltpu.VMEM((*both, 2, rows, hid), BF16),
                    pltpu.VMEM((2, 4, 8, hid), F32),
                    pltpu.VMEM((*both, cols, hid), F32),
                    pltpu.VMEM((*both, rows, hid), F32))],
                pltpu.SemaphoreType.DMA((*both, 8)),
                pltpu.SemaphoreType.DMA((*both, 8)),
                pltpu.SemaphoreType.DMA((2,)),
                pltpu.SemaphoreType.DMA(both),
                pltpu.SemaphoreType.DMA(both),
                pltpu.SemaphoreType.DMA((7,)),
            ],
            compiler_params=pltpu.CompilerParams(
                collective_id=0, has_side_effects=True, vmem_limit_bytes=14 * 2**20),
            name="convlstm",
        )(*(pltpu.with_memory_space_constraint(x, pltpu.HBM) for x in args))
        changed = (0, 3, 4, 5)
        seq, c_last, *_ = pl.pallas_call(
            functools.partial(finish_kernel, sizes),
            out_shape=(seq_shape, wide(rows * cols), *(state[k] for k in changed)),
            in_specs=[vmem] * 9,
            out_specs=(hbm, hbm, *[vmem] * len(changed)),
            input_output_aliases={1 + k: 2 + n for n, k in enumerate(changed)},
            scratch_shapes=[
                pltpu.VMEM((2, rows, cols, hid), BF16),
                pltpu.VMEM((rows * cols, hid), F32),
                pltpu.SemaphoreType.DMA((steps // CHUNK + 2,)),
            ],
            compiler_params=pltpu.CompilerParams(vmem_limit_bytes=6 * 2**20),
            name="finish",
        )(seq, *held)
        return seq[:, None], c_last.reshape(c_init.shape)

    return jax.shard_map(local_run, mesh=mesh, in_specs=(seq_spec, P(), P(), P(), state_spec, state_spec),
                         out_specs=(seq_spec, state_spec), check_vma=False)
```

```python
import functools

import jax
import jax.numpy as jnp
from jax import lax
from jax.experimental import pallas as pl
from jax.experimental.pallas import tpu as pltpu
from jax.sharding import PartitionSpec as P

MESH = pl.DeviceIdType.MESH
LANES = 128
BF16 = jnp.bfloat16
F32 = jnp.float32
TDT = jnp.bfloat16

PITCH = 36
DIRECTIONS = ((-1, 0), (1, 0), (0, -1), (0, 1), (-1, -1), (-1, 1), (1, -1), (1, 1))
CHUNK = 2
PARTS = (4, 12)
FIRST, STOP = 13, 29
BLOCK = 11
SIDE = 4


def cell(r, c):
    return (r + 2) * PITCH + c + 2


def pcell(r, c):
    return (r + 2) * PITCH + c + 1


def exists(d, n_rows, n_cols):
    dr, dc = DIRECTIONS[d]
    ok = None
    for here, step, count in ((lax.axis_index("rows"), dr, n_rows), (lax.axis_index("cols"), dc, n_cols)):
        if step:
            this = (here > 0) if step < 0 else (here < count - 1)
            ok = this if ok is None else jnp.logical_and(ok, this)
    return ok


class Tile:
    def __init__(self, sizes, x_buf, p_buf, w_buf, c_main, c_col, c_row, ring_row, ring_col):
        self.steps, self.rows, self.cols, self.n_rows, self.n_cols, self.c_in = sizes
        self.x_buf, self.p_buf, self.w_buf = x_buf, p_buf, w_buf
        self.c_main, self.c_col, self.c_row = c_main, c_col, c_row
        self.ring_row, self.ring_col = ring_row, ring_col
        self.hid = x_buf.shape[-1]
        self.width = self.cols - 2 * SIDE
        self.long = self.rows + 8
        self.side_cols = tuple(range(SIDE)) + tuple(range(self.cols - SIDE, self.cols))
        self.edge_rows = (0, 1, self.rows - 2, self.rows - 1)
        self.last = len(self.side_cols) - 1

    def run_index(self, start, length, vertical):
        return pl.ds(start, length, stride=PITCH) if vertical else pl.ds(start, length)

    def gates_of(self, slot, p_slot, groups):
        parts = []
        for dy in range(3):
            for dx in range(3):
                pieces = [self.x_buf[slot, self.run_index(cell(r + dy - 1, c + dx - 1), length, vertical), :]
                          for r, c, length, vertical in groups]
                parts.append(jnp.concatenate(pieces, axis=0) if len(pieces) > 1 else pieces[0])
        for dy in range(3):
            pieces = [self.p_buf[p_slot, self.run_index(pcell(r + dy - 1, c), length, vertical), :]
                      for r, c, length, vertical in groups]
            parts.append(jnp.concatenate(pieces, axis=0) if len(pieces) > 1 else pieces[0])
        lhs = jnp.concatenate(parts, axis=1).astype(BF16)
        return jnp.dot(lhs, self.w_buf[...], preferred_element_type=F32)

    def finish(self, slot, groups, gates, c_ref, c_at, mask=None):
        index = pl.ds(c_at, gates.shape[0])
        c_prev = c_ref[index, :]
        gi, gf, go, gg = (jnp.tanh(gates[:, self.hid * k:self.hid * (k + 1)]) for k in range(4))
        c_next = 0.5 * ((gf * c_prev + c_prev) + (gi * gg + gg))
        h = (0.5 * go + 0.5) * jnp.tanh(c_next)
        if mask is None:
            c_ref[index, :] = c_next
        else:
            h = h * mask
        at = 0
        for r, c, length, vertical in groups:
            self.x_buf[1 - slot, self.run_index(cell(r, c), length, vertical), :] = h[at:at + length]
            at += length

    def update(self, slot, p_slot, groups, c_ref, c_at):
        self.finish(slot, groups, self.gates_of(slot, p_slot, groups), c_ref, c_at)

    def main_run(self, first, stop):
        return [(r, SIDE, self.width, False) for r in range(first, stop)]

    def side_run(self, *ids):
        return [(0, self.side_cols[i], self.rows, True) for i in ids]

    def main_rows(self, slot, p_slot, first, stop):
        self.update(slot, p_slot, self.main_run(first, stop), self.c_main, (first - 2) * self.width)

    def write_out(self, slot, ref):
        for r in range(self.rows):
            ref[r] = self.x_buf[slot, pl.ds(cell(r, 0), self.cols), :].astype(BF16)

    def before_wait(self, pa, write):
        rows, last = self.rows, self.last
        for at in range(2, rows - 2, BLOCK):
            self.main_rows(0, pa, at, at + BLOCK)
        self.update(0, pa, self.side_run(1, 2, 3), self.c_col, rows)
        self.update(0, pa, self.side_run(last - 3, last - 2, last - 1), self.c_col, (last - 3) * rows)
        write()
        for first, stop in ((3, FIRST), (STOP, rows - 11), (rows - 11, rows - 3)):
            self.main_rows(1, pa + 1, first, stop)

    def after_wait(self, pa, send):
        rows, cols, last = self.rows, self.cols, self.last
        there = [exists(d, self.n_rows, self.n_cols).astype(jnp.int32).astype(F32) for d in range(4)]
        place = lax.broadcasted_iota(jnp.int32, (self.long, self.hid), 0)
        ends = jnp.where(place == 0, there[0], jnp.where(place == rows + 1, there[1], 1.0))
        ring_col_run = [(-1, -1, self.long, True), (-1, cols, self.long, True)]
        ring_row_run = [(-1, 0, cols, False), (rows, 0, cols, False)]
        row_run = [(r, 0, cols, False) for r in self.edge_rows]
        n_long = 2 * self.long
        middle = (FIRST + STOP) // 2
        c_col, c_row, c_main, finish = self.c_col, self.c_row, self.c_main, self.finish

        own = self.side_run(0) + self.side_run(last) + row_run
        own_gates = self.gates_of(0, pa, own)
        ring_gates = self.gates_of(0, pa, ring_col_run + ring_row_run)
        run = self.main_run(FIRST, middle)
        beside = self.gates_of(1, pa + 1, run)
        finish(0, self.side_run(0), own_gates[:rows], c_col, 0)
        finish(0, self.side_run(last), own_gates[rows:2 * rows], c_col, last * rows)
        finish(0, row_run, own_gates[2 * rows:], c_row, 0)
        mask = jnp.concatenate([ends * there[2], ends * there[3]], axis=0)
        finish(0, ring_col_run, ring_gates[:n_long], self.ring_col, 0, mask)
        mask = jnp.concatenate([jnp.full((cols, self.hid), 1.0, F32) * there[k] for k in range(2)], axis=0)
        finish(0, ring_row_run, ring_gates[n_long:], self.ring_row, 0, mask)
        for i, r in ((0, 0), (3, rows - 1)):
            for first in (1, last - 3):
                c_col[pl.ds(first * rows + r, 3, stride=rows), :] = c_row[pl.ds(i * cols + self.side_cols[first], 3), :]
        finish(1, run, beside, c_main, (FIRST - 2) * self.width)
        edge_gates = self.gates_of(1, pa + 1, self.side_run(0, 1, last - 1, last) + row_run)
        run = self.main_run(middle, STOP)
        beside = self.gates_of(1, pa + 1, run)
        finish(1, self.side_run(0, 1), edge_gates[:2 * rows], c_col, 0)
        finish(1, self.side_run(last - 1, last), edge_gates[2 * rows:4 * rows], c_col, (last - 1) * rows)
        finish(1, row_run, edge_gates[4 * rows:], c_row, 0)
        send()

        finish(1, run, beside, c_main, (middle - 2) * self.width)
        runs = [(self.side_run(2, 3), c_col, 2 * rows), (self.side_run(last - 3, last - 2), c_col, (last - 3) * rows),
                (self.main_run(2, 3), c_main, 0), (self.main_run(rows - 3, rows - 2), c_main, (rows - 5) * self.width)]
        gates = self.gates_of(1, pa + 1, sum((run for run, _, _ in runs), []))
        at = 0
        for run, c_ref, c_at in runs:
            size = sum(length for _, _, length, _ in run)
            finish(1, run, gates[at:at + size], c_ref, c_at)
            at += size


def kernel(sizes, frames_ref, w_rec_ref, w_in_ref, bias_ref, h0_ref, c0_ref,
           seq_ref, x_buf, p_buf, w_buf, c_main, c_col, c_row, ring_row, ring_col,
           bias_buf, f_buf, f_side, c_buf, row_send, col_send, corner_send, crow_send, ccol_send,
           row_recv, col_recv, corner_recv, crow_recv, ccol_recv,
           send_sem, recv_sem, f_sem, f_send_sem, f_recv_sem, arg_sem):
    tile = Tile(sizes, x_buf, p_buf, w_buf, c_main, c_col, c_row, ring_row, ring_col)
    steps, rows, cols, n_rows, n_cols, c_in = sizes
    hid, width, long, last = tile.hid, tile.width, tile.long, tile.last
    side_cols, edge_rows = tile.side_cols, tile.edge_rows
    gates_n = 4 * hid
    packed = 3 * c_in
    my_row = lax.axis_index("rows")
    my_col = lax.axis_index("cols")

    def device(d):
        dr, dc = DIRECTIONS[d]
        return {"rows": my_row + dr, "cols": my_col + dc}

    def opposite(d):
        return DIRECTIONS.index((-DIRECTIONS[d][0], -DIRECTIONS[d][1]))

    def source(slot, d, kind):
        dr, dc = DIRECTIONS[d]
        if dr and dc:
            return corner_send.at[slot, d - 4]
        if dr:
            return (crow_send if kind else row_send).at[slot, d]
        return (ccol_send if kind else col_send).at[slot, d - 2]

    def landing(slot, d, kind):
        dr, dc = DIRECTIONS[d]
        if dr and dc:
            return corner_recv.at[slot, d - 4]
        if dr:
            return (crow_recv if kind else row_recv).at[slot, d]
        return (ccol_recv if kind else col_recv).at[slot, d - 2]

    def departure(slot, d, kind):
        return pltpu.make_async_remote_copy(
            src_ref=source(slot, d, kind), dst_ref=landing(slot, opposite(d), kind), send_sem=send_sem.at[slot, kind, d],
            recv_sem=recv_sem.at[slot, kind, opposite(d)], device_id=device(d), device_id_type=MESH)

    def arrival(slot, d, kind):
        return pltpu.make_async_remote_copy(
            src_ref=source(slot, d, kind), dst_ref=landing(slot, d, kind), send_sem=send_sem.at[slot, kind, d],
            recv_sem=recv_sem.at[slot, kind, d], device_id=device(d), device_id_type=MESH)

    def frame_part(part):
        first, stop = (0, *PARTS, steps)[part:part + 2]
        return pl.ds(first, stop - first)

    def frame_side(part, d, arriving=False):
        ts = frame_part(part)
        k = d - 2
        at = k if arriving else 1 - k
        return pltpu.make_async_remote_copy(
            src_ref=f_buf.at[ts, pl.ds(0 if k == 0 else cols - 2, 2)], dst_ref=f_side.at[at, ts],
            send_sem=f_send_sem.at[part, k], recv_sem=f_recv_sem.at[part, at], device_id=device(d), device_id_type=MESH)

    def frame_load(part):
        ts = frame_part(part)
        return pltpu.make_async_copy(frames_ref.at[ts], f_buf.at[ts], f_sem.at[part])

    parts = range(len(PARTS) + 1)
    loads = [(h0_ref, seq_ref.at[steps - 1]), (c0_ref, c_buf), (w_rec_ref, w_buf.at[pl.ds(0, 9 * hid)]), (bias_ref, bias_buf)]
    loads += [(w_in_ref.at[pl.ds(packed * dy, packed)], w_buf.at[pl.ds(9 * hid + LANES * dy, packed)]) for dy in range(3)]
    loads = [pltpu.make_async_copy(src, dst, arg_sem.at[k]) for k, (src, dst) in enumerate(loads)]
    frame_load(0).start()
    for load in loads:
        load.start()
    for part in parts[1:]:
        frame_load(part).start()
    for ref in (row_recv, col_recv, corner_recv, crow_recv, ccol_recv, f_side):
        ref[...] = jnp.zeros_like(ref)
    for slot in range(2):
        x_buf[slot, pl.ds(0, 2 * PITCH), :] = jnp.zeros((2 * PITCH, hid), F32)
        x_buf[slot, pl.ds((rows + 2) * PITCH, 10 * PITCH), :] = jnp.zeros((10 * PITCH, hid), F32)
    for slot in range(4):
        p_buf[slot, pl.ds(0, 2 * PITCH), :] = jnp.zeros((2 * PITCH, LANES), F32)
        p_buf[slot, pl.ds((rows + 2) * PITCH, 10 * PITCH), :] = jnp.zeros((10 * PITCH, LANES), F32)
    ring_col[...] = jnp.zeros_like(ring_col)

    barrier = pltpu.get_barrier_semaphore()
    count = jnp.int32(0)
    for d in range(8):
        @pl.when(exists(d, n_rows, n_cols))
        def _():
            pl.semaphore_signal(barrier, inc=1, device_id=device(d), device_id_type=MESH)
        count = count + exists(d, n_rows, n_cols).astype(jnp.int32)
    pl.semaphore_wait(barrier, count)

    def send_sides(part):
        frame_load(part).wait()
        for d in (2, 3):
            @pl.when(exists(d, n_rows, n_cols))
            def _():
                frame_side(part, d).start()

    def receive_sides(part):
        for d in (2, 3):
            @pl.when(exists(d, n_rows, n_cols))
            def _():
                frame_side(part, d, True).wait_recv()

    send_sides(0)
    loads[0].wait()
    for r in range(rows):
        x_buf[0, pl.ds(cell(r, 0), cols), :] = seq_ref[steps - 1, r].astype(F32)
    loads[1].wait()
    for r in range(2, rows - 2):
        c_main[pl.ds((r - 2) * width, width), :] = c_buf[pl.ds(r * cols + SIDE, width), :]
    for i, c in enumerate(side_cols):
        c_col[pl.ds(i * rows, rows), :] = c_buf[pl.ds(c, rows, stride=cols), :]
    for i, r in enumerate(edge_rows):
        c_row[pl.ds(i * cols, cols), :] = c_buf[pl.ds(r * cols, cols), :]

    lane = lax.broadcasted_iota(jnp.int32, (1, gates_n), 1)
    scale = jnp.where(lane < 3 * hid, 0.5, 1.0)
    for load in loads[2:]:
        load.wait()
    for at in range(0, 9 * hid, LANES):
        w_buf[pl.ds(at, LANES), :] = (w_buf[pl.ds(at, LANES), :].astype(F32) * scale).astype(BF16)
    bias = bias_buf[...] * scale
    b0 = bias.astype(BF16).astype(F32)
    b1 = (bias - b0).astype(BF16).astype(F32)
    b2 = bias - b0 - b1
    row = lax.broadcasted_iota(jnp.int32, (16, gates_n), 0)
    bias_rows = jnp.where(row == 0, b0, jnp.where(row == 1, b1, jnp.where(row == 2, b2, 0.0)))
    for dy in range(3):
        at = 9 * hid + LANES * dy
        w_buf[pl.ds(at, packed), :] = (w_buf[pl.ds(at, packed), :].astype(F32) * scale).astype(BF16)
        w_buf[pl.ds(at + packed, LANES - packed), :] = jnp.zeros((LANES - packed, gates_n), BF16)
        if dy == 1:
            w_buf[pl.ds(at + packed, 16), :] = bias_rows.astype(BF16)

    row = lax.broadcasted_iota(jnp.int32, (LANES - packed, rows), 0)
    ones = (row < 3).astype(F32).astype(BF16)

    def pack_frame(t, slot):
        for c in range(-1, cols + 1):
            pieces = []
            for k in range(c - 1, c + 2):
                if k < 0:
                    pieces.append(f_side[0, t, k + 2])
                elif k < cols:
                    pieces.append(f_buf[t, k])
                else:
                    pieces.append(f_side[1, t, k - cols])
            window = jnp.concatenate(pieces + [ones], axis=0)
            p_buf[slot, pl.ds(pcell(0, c), rows, stride=PITCH), :] = window.T.astype(F32)

    def stage(slot, p_first):
        state = x_buf.at[0]
        for k, r in enumerate((0, rows - 2)):
            for n in range(2):
                row_send[slot, k, n * cols:(n + 1) * cols] = state[pl.ds(cell(r + n, 0), cols), :].astype(BF16)
            at = 2 * cols
            row_send[slot, k, at:at + 2 * PITCH] = p_buf[p_first, pl.ds(pcell(r, -1), 2 * PITCH), :].astype(BF16)
            at += 2 * PITCH
            r_one = 0 if k == 0 else rows - 1
            row_send[slot, k, at:at + PITCH] = p_buf[p_first + 1, pl.ds(pcell(r_one, -1), PITCH), :].astype(BF16)
            crow_send[slot, k] = c_row[pl.ds((0 if k == 0 else 3) * cols, cols), :]
        for k, c in enumerate((0, cols - 2)):
            for n in range(2):
                col_send[slot, k, n] = state[pl.ds(cell(0, c + n), rows, stride=PITCH), :].astype(BF16)
            ccol_send[slot, k] = c_col[pl.ds((0 if k == 0 else last) * rows, rows), :]
        for k, (dr, dc) in enumerate(DIRECTIONS[4:]):
            r, c = (0 if dr < 0 else rows - 2), (0 if dc < 0 else cols - 2)
            for n in range(2):
                corner = state[pl.ds(cell(r + n, c), 2), :].astype(BF16).astype(F32)
                corner_send[slot, k, 2 * n:2 * n + 2] = corner
            c_at = (0 if dr < 0 else 3 * cols) + (0 if dc < 0 else cols - 1)
            corner_send[slot, k, 4:5] = c_row[pl.ds(c_at, 1), :]

    def each_copy(act, slot, wanted=None):
        for kind in range(2):
            for d in range(8 if kind == 0 else 4):
                @pl.when(exists(d, n_rows, n_cols) if wanted is None else jnp.logical_and(exists(d, n_rows, n_cols), wanted))
                def _():
                    act(slot, d, kind)

    def send_halo(slot, wanted=None):
        each_copy(lambda *which: departure(*which).start(), slot, wanted)

    def receive_halo(slot):
        each_copy(lambda *which: arrival(*which).wait_recv(), slot)

    def wait_sent(slot):
        each_copy(lambda *which: departure(*which).wait_send(), slot)

    def unpack_halo(slot, p_first):
        state = x_buf.at[0]
        for k, r in enumerate((-2, rows)):
            for n in range(2):
                state[pl.ds(cell(r + n, 0), cols), :] = row_recv[slot, k, n * cols:(n + 1) * cols].astype(F32)
            at = 2 * cols
            p_buf[p_first, pl.ds(pcell(r, -1), 2 * PITCH), :] = row_recv[slot, k, at:at + 2 * PITCH].astype(F32)
            at += 2 * PITCH
            r_one = -1 if k == 0 else rows
            p_buf[p_first + 1, pl.ds(pcell(r_one, -1), PITCH), :] = row_recv[slot, k, at:at + PITCH].astype(F32)
            ring_row[pl.ds(k * cols, cols), :] = crow_recv[slot, k]
        for k, c in enumerate((-2, cols)):
            for n in range(2):
                state[pl.ds(cell(0, c + n), rows, stride=PITCH), :] = col_recv[slot, k, n].astype(F32)
            ring_col[pl.ds(k * long + 1, rows), :] = ccol_recv[slot, k]
        for k, (dr, dc) in enumerate(DIRECTIONS[4:]):
            r, c = (-2 if dr < 0 else rows), (-2 if dc < 0 else cols)
            for n in range(2):
                state[pl.ds(cell(r + n, c), 2), :] = corner_recv[slot, k, 2 * n:2 * n + 2]
            at = (0 if dc < 0 else long) + (0 if dr < 0 else rows + 1)
            ring_col[pl.ds(at, 1), :] = corner_recv[slot, k, 4:5]

    receive_sides(0)
    pack_frame(0, 0)
    pack_frame(1, 1)
    stage(0, 0)
    send_halo(0)
    send_sides(1)

    def before(m, now):
        t = 2 * m
        other = 2 * (1 - now)
        pack_frame(jnp.minimum(t + 2, steps - 2), other)
        pack_frame(jnp.minimum(t + 3, steps - 1), other + 1)
        tile.before_wait(2 * now, lambda: tile.write_out(0, seq_ref.at[jnp.maximum(t - 1, 0)]))

        @pl.when(m >= 1)
        def _():
            wait_sent(1 - now)
        receive_halo(now)
        unpack_halo(now, 2 * now)

    def pair(m, now):
        def send():
            stage(1 - now, 2 * (1 - now))
            send_halo(1 - now)
            if now == 0:
                @pl.when(m == 0)
                def _():
                    receive_sides(1)
                    send_sides(2)

                @pl.when(m == 2)
                def _():
                    receive_sides(2)

        before(m, now)
        tile.after_wait(2 * now, send)
        tile.write_out(1, seq_ref.at[2 * m])

    def trip(i, carry):
        pair(2 * i, 0)
        pair(2 * i + 1, 1)
        return carry

    n_pairs = steps // 2
    lax.fori_loop(0, (n_pairs - 1) // 2, trip, 0)
    for m in range(n_pairs - 2 + n_pairs % 2, n_pairs - 1):
        pair(m, m % 2)
    before(n_pairs - 1, (n_pairs - 1) % 2)
    wait_sent((n_pairs - 1) % 2)
    for part in parts:
        for d in (2, 3):
            @pl.when(exists(d, n_rows, n_cols))
            def _():
                frame_side(part, d).wait_send()


def finish_kernel(sizes, seq_in, x_in, p_buf, w_buf, c_main_in, c_col_in, c_row_in, ring_row, ring_col,
                  seq_out, c_out, x_buf, c_main, c_col, c_row, out_buf, c_buf, sem):
    tile = Tile(sizes, x_buf, p_buf, w_buf, c_main, c_col, c_row, ring_row, ring_col)
    steps, rows, cols = sizes[:3]
    copies = [pltpu.make_async_copy(seq_in.at[pl.ds(t, CHUNK)], seq_out.at[pl.ds(t, CHUNK)], sem.at[t // CHUNK])
              for t in range(0, steps - 2, CHUNK)]
    for copy in copies:
        copy.start()
    tail = [pltpu.make_async_copy(out_buf.at[k], seq_out.at[steps - 2 + k], sem.at[(steps - 2) // CHUNK + k])
            for k in range(2)]

    def first_done():
        tile.write_out(1, out_buf.at[0])
        tail[0].start()

    tile.after_wait(2 * ((steps // 2 - 1) % 2), first_done)
    tile.write_out(0, out_buf.at[1])
    tail[1].start()
    for r in range(2, rows - 2):
        c_buf[pl.ds(r * cols + SIDE, tile.width), :] = c_main[pl.ds((r - 2) * tile.width, tile.width), :]
    for i, c in enumerate(tile.side_cols):
        c_buf[pl.ds(c, rows, stride=cols), :] = c_col[pl.ds(i * rows, rows), :]
    for i, r in enumerate(tile.edge_rows):
        c_buf[pl.ds(r * cols, cols), :] = c_row[pl.ds(i * cols, cols), :]
    c_copy = pltpu.make_async_copy(c_buf, c_out, sem.at[steps // CHUNK + 1])
    c_copy.start()
    for copy in (*copies, *tail, c_copy):
        copy.wait()


def solution(mesh):
    n_rows = mesh.shape["rows"]
    n_cols = mesh.shape["cols"]
    seq_spec = P(None, "dp", "rows", "cols", None)
    state_spec = P("dp", "rows", "cols", None)

    def local_run(frames, w_in, w_rec, gate_bias, h_init, c_init):
        steps, _, rows, cols, c_in = frames.shape
        hid = h_init.shape[-1]
        row_words = 2 * cols + 3 * PITCH + 4
        both = (2, 2)
        vmem = pl.BlockSpec(memory_space=pltpu.VMEM)
        args = (jnp.transpose(frames[:, 0], (0, 2, 3, 1)), w_rec.reshape(9 * hid, 4 * hid),
                w_in.reshape(9 * c_in, 4 * hid), gate_bias.reshape(1, 4 * hid), h_init[0],
                c_init[0].reshape(rows * cols, hid))
        hbm = pl.BlockSpec(memory_space=pltpu.HBM)
        sizes = (steps, rows, cols, n_rows, n_cols, c_in)

        def wide(*shape):
            return jax.ShapeDtypeStruct((*shape, hid), F32)

        state = (wide(2, (rows + 12) * PITCH), wide(4, (rows + 12) * PITCH),
                 jax.ShapeDtypeStruct((9 * hid + 3 * hid, 4 * hid), BF16), wide((rows - 4) * (cols - 2 * SIDE)),
                 wide(rows * 2 * SIDE), wide(cols * 4), wide(cols * 2), wide((rows + 8) * 2))
        seq_shape = jax.ShapeDtypeStruct((steps, rows, cols, hid), BF16)
        seq, *held = pl.pallas_call(
            functools.partial(kernel, sizes),
            out_shape=(seq_shape, *state),
            in_specs=[hbm] * 6,
            out_specs=(vmem,) * 9,
            scratch_shapes=[
                pltpu.VMEM((1, 4 * hid), F32),
                pltpu.VMEM((steps, cols, c_in, rows), BF16),
                pltpu.VMEM((2, steps, 2, c_in, rows), BF16),
                pltpu.VMEM((rows * cols, hid), F32),
                *[shape for _ in both for shape in (
                    pltpu.VMEM((*both, row_words, hid), BF16),
                    pltpu.VMEM((*both, 2, rows, hid), BF16),
                    pltpu.VMEM((2, 4, 8, hid), F32),
                    pltpu.VMEM((*both, cols, hid), F32),
                    pltpu.VMEM((*both, rows, hid), F32))],
                pltpu.SemaphoreType.DMA((*both, 8)),
                pltpu.SemaphoreType.DMA((*both, 8)),
                pltpu.SemaphoreType.DMA((len(PARTS) + 1,)),
                pltpu.SemaphoreType.DMA((len(PARTS) + 1, 2)),
                pltpu.SemaphoreType.DMA((len(PARTS) + 1, 2)),
                pltpu.SemaphoreType.DMA((7,)),
            ],
            compiler_params=pltpu.CompilerParams(
                collective_id=0, has_side_effects=True, vmem_limit_bytes=14 * 2**20),
            name="convlstm",
        )(*(pltpu.with_memory_space_constraint(x, pltpu.HBM) for x in args))
        changed = (0, 3, 4, 5)
        seq, c_last, *_ = pl.pallas_call(
            functools.partial(finish_kernel, sizes),
            out_shape=(seq_shape, wide(rows * cols), *(state[k] for k in changed)),
            in_specs=[vmem] * 9,
            out_specs=(hbm, hbm, *[vmem] * len(changed)),
            input_output_aliases={1 + k: 2 + n for n, k in enumerate(changed)},
            scratch_shapes=[
                pltpu.VMEM((2, rows, cols, hid), BF16),
                pltpu.VMEM((rows * cols, hid), F32),
                pltpu.SemaphoreType.DMA((steps // CHUNK + 2,)),
            ],
            compiler_params=pltpu.CompilerParams(vmem_limit_bytes=6 * 2**20),
            name="finish",
        )(seq, *held)
        return seq[:, None], c_last.reshape(c_init.shape)

    return jax.shard_map(local_run, mesh=mesh, in_specs=(seq_spec, P(), P(), P(), state_spec, state_spec),
                         out_specs=(seq_spec, state_spec), check_vma=False)
```

```python
import functools

import jax
import jax.numpy as jnp
from jax import lax
from jax.experimental import pallas as pl
from jax.experimental.pallas import tpu as pltpu
from jax.sharding import PartitionSpec as P

MESH = pl.DeviceIdType.MESH
LANES = 128
BF16 = jnp.bfloat16
F32 = jnp.float32
TDT = jnp.bfloat16

PITCH = 36
DIRECTIONS = ((-1, 0), (1, 0), (0, -1), (0, 1), (-1, -1), (-1, 1), (1, -1), (1, 1))
CHUNK = 2
PARTS = (4, 12)
FIRST, STOP = 15, 27
BLOCK = 11
SIDE = 4


def cell(r, c):
    return (r + 2) * PITCH + c + 2


def pcell(r, c):
    return (r + 2) * PITCH + c + 1


def exists(d, n_rows, n_cols):
    dr, dc = DIRECTIONS[d]
    ok = None
    for here, step, count in ((lax.axis_index("rows"), dr, n_rows), (lax.axis_index("cols"), dc, n_cols)):
        if step:
            this = (here > 0) if step < 0 else (here < count - 1)
            ok = this if ok is None else jnp.logical_and(ok, this)
    return ok


class Tile:
    def __init__(self, sizes, x_buf, p_buf, w_buf, c_main, c_col, c_row, ring_row, ring_col):
        self.steps, self.rows, self.cols, self.n_rows, self.n_cols, self.c_in = sizes
        self.x_buf, self.p_buf, self.w_buf = x_buf, p_buf, w_buf
        self.c_main, self.c_col, self.c_row = c_main, c_col, c_row
        self.ring_row, self.ring_col = ring_row, ring_col
        self.hid = x_buf.shape[-1]
        self.width = self.cols - 2 * SIDE
        self.long = self.rows + 8
        self.side_cols = tuple(range(SIDE)) + tuple(range(self.cols - SIDE, self.cols))
        self.edge_rows = (0, 1, self.rows - 2, self.rows - 1)
        self.last = len(self.side_cols) - 1

    def run_index(self, start, length, vertical):
        return pl.ds(start, length, stride=PITCH) if vertical else pl.ds(start, length)

    def gates_of(self, slot, p_slot, groups):
        parts = []
        for dy in range(3):
            for dx in range(3):
                pieces = [self.x_buf[slot, self.run_index(cell(r + dy - 1, c + dx - 1), length, vertical), :]
                          for r, c, length, vertical in groups]
                parts.append(jnp.concatenate(pieces, axis=0) if len(pieces) > 1 else pieces[0])
        for dy in range(3):
            pieces = [self.p_buf[p_slot, self.run_index(pcell(r + dy - 1, c), length, vertical), :]
                      for r, c, length, vertical in groups]
            parts.append(jnp.concatenate(pieces, axis=0) if len(pieces) > 1 else pieces[0])
        lhs = jnp.concatenate(parts, axis=1).astype(BF16)
        return jnp.dot(lhs, self.w_buf[...], preferred_element_type=F32)

    def finish(self, slot, groups, gates, c_ref, c_at, mask=None):
        index = pl.ds(c_at, gates.shape[0])
        c_prev = c_ref[index, :]
        gi, gf, go, gg = (jnp.tanh(gates[:, self.hid * k:self.hid * (k + 1)]) for k in range(4))
        c_next = 0.5 * ((gf * c_prev + c_prev) + (gi * gg + gg))
        h = (0.5 * go + 0.5) * jnp.tanh(c_next)
        if mask is None:
            c_ref[index, :] = c_next
        else:
            h = h * mask
        at = 0
        for r, c, length, vertical in groups:
            self.x_buf[1 - slot, self.run_index(cell(r, c), length, vertical), :] = h[at:at + length]
            at += length

    def update(self, slot, p_slot, groups, c_ref, c_at):
        self.finish(slot, groups, self.gates_of(slot, p_slot, groups), c_ref, c_at)

    def main_run(self, first, stop):
        return [(r, SIDE, self.width, False) for r in range(first, stop)]

    def side_run(self, *ids):
        return [(0, self.side_cols[i], self.rows, True) for i in ids]

    def main_rows(self, slot, p_slot, first, stop):
        self.update(slot, p_slot, self.main_run(first, stop), self.c_main, (first - 2) * self.width)

    def write_out(self, slot, ref):
        for r in range(self.rows):
            ref[r] = self.x_buf[slot, pl.ds(cell(r, 0), self.cols), :].astype(BF16)

    def before_wait(self, pa, write):
        rows, last = self.rows, self.last
        for at in range(2, rows - 2, BLOCK):
            self.main_rows(0, pa, at, at + BLOCK)
        self.update(0, pa, self.side_run(1, 2, 3), self.c_col, rows)
        self.update(0, pa, self.side_run(last - 3, last - 2, last - 1), self.c_col, (last - 3) * rows)
        write()
        for first, stop in ((3, FIRST), (STOP, rows - 11), (rows - 11, rows - 3)):
            self.main_rows(1, pa + 1, first, stop)

    def after_wait(self, pa, send=lambda: None):
        rows, cols, last = self.rows, self.cols, self.last
        there = [exists(d, self.n_rows, self.n_cols).astype(jnp.int32).astype(F32) for d in range(4)]
        place = lax.broadcasted_iota(jnp.int32, (self.long, self.hid), 0)
        ends = jnp.where(place == 0, there[0], jnp.where(place == rows + 1, there[1], 1.0))
        ring_col_run = [(-1, -1, self.long, True), (-1, cols, self.long, True)]
        ring_row_run = [(-1, 0, cols, False), (rows, 0, cols, False)]
        row_run = [(r, 0, cols, False) for r in self.edge_rows]
        n_long = 2 * self.long
        middle = (FIRST + STOP) // 2
        c_col, c_row, c_main, finish = self.c_col, self.c_row, self.c_main, self.finish

        own = self.side_run(0) + self.side_run(last) + row_run
        own_gates = self.gates_of(0, pa, own)
        ring_gates = self.gates_of(0, pa, ring_col_run + ring_row_run)
        run = self.main_run(FIRST, middle)
        beside = self.gates_of(1, pa + 1, run)
        finish(0, self.side_run(0), own_gates[:rows], c_col, 0)
        finish(0, self.side_run(last), own_gates[rows:2 * rows], c_col, last * rows)
        finish(0, row_run, own_gates[2 * rows:], c_row, 0)
        mask = jnp.concatenate([ends * there[2], ends * there[3]], axis=0)
        finish(0, ring_col_run, ring_gates[:n_long], self.ring_col, 0, mask)
        mask = jnp.concatenate([jnp.full((cols, self.hid), 1.0, F32) * there[k] for k in range(2)], axis=0)
        finish(0, ring_row_run, ring_gates[n_long:], self.ring_row, 0, mask)
        for i, r in ((0, 0), (3, rows - 1)):
            for first in (1, last - 3):
                c_col[pl.ds(first * rows + r, 3, stride=rows), :] = c_row[pl.ds(i * cols + self.side_cols[first], 3), :]
        finish(1, run, beside, c_main, (FIRST - 2) * self.width)
        edge_gates = self.gates_of(1, pa + 1, self.side_run(0, 1, last - 1, last) + row_run)
        run = self.main_run(middle, STOP)
        beside = self.gates_of(1, pa + 1, run)
        finish(1, self.side_run(0, 1), edge_gates[:2 * rows], c_col, 0)
        finish(1, self.side_run(last - 1, last), edge_gates[2 * rows:4 * rows], c_col, (last - 1) * rows)
        finish(1, row_run, edge_gates[4 * rows:], c_row, 0)
        send()

        finish(1, run, beside, c_main, (middle - 2) * self.width)
        runs = [(self.side_run(2, 3), c_col, 2 * rows), (self.side_run(last - 3, last - 2), c_col, (last - 3) * rows),
                (self.main_run(2, 3), c_main, 0), (self.main_run(rows - 3, rows - 2), c_main, (rows - 5) * self.width)]
        gates = self.gates_of(1, pa + 1, sum((run for run, _, _ in runs), []))
        at = 0
        for run, c_ref, c_at in runs:
            size = sum(length for _, _, length, _ in run)
            finish(1, run, gates[at:at + size], c_ref, c_at)
            at += size


def kernel(sizes, frames_ref, w_rec_ref, w_in_ref, bias_ref, h0_ref, c0_ref,
           seq_ref, x_buf, p_buf, w_buf, c_main, c_col, c_row, ring_row, ring_col,
           bias_buf, f_buf, f_side, c_buf, row_send, col_send, corner_send, crow_send, ccol_send,
           row_recv, col_recv, corner_recv, crow_recv, ccol_recv,
           send_sem, recv_sem, f_sem, f_send_sem, f_recv_sem, arg_sem):
    tile = Tile(sizes, x_buf, p_buf, w_buf, c_main, c_col, c_row, ring_row, ring_col)
    steps, rows, cols, n_rows, n_cols, c_in = sizes
    hid, width, long, last = tile.hid, tile.width, tile.long, tile.last
    side_cols, edge_rows = tile.side_cols, tile.edge_rows
    gates_n = 4 * hid
    packed = 3 * c_in
    my_row = lax.axis_index("rows")
    my_col = lax.axis_index("cols")

    def device(d):
        dr, dc = DIRECTIONS[d]
        return {"rows": my_row + dr, "cols": my_col + dc}

    def opposite(d):
        return DIRECTIONS.index((-DIRECTIONS[d][0], -DIRECTIONS[d][1]))

    def source(slot, d, kind):
        dr, dc = DIRECTIONS[d]
        if dr and dc:
            return corner_send.at[slot, d - 4]
        if dr:
            return (crow_send if kind else row_send).at[slot, d]
        return (ccol_send if kind else col_send).at[slot, d - 2]

    def landing(slot, d, kind):
        dr, dc = DIRECTIONS[d]
        if dr and dc:
            return corner_recv.at[slot, d - 4]
        if dr:
            return (crow_recv if kind else row_recv).at[slot, d]
        return (ccol_recv if kind else col_recv).at[slot, d - 2]

    def departure(slot, d, kind):
        return pltpu.make_async_remote_copy(
            src_ref=source(slot, d, kind), dst_ref=landing(slot, opposite(d), kind), send_sem=send_sem.at[slot, kind, d],
            recv_sem=recv_sem.at[slot, kind, opposite(d)], device_id=device(d), device_id_type=MESH)

    def arrival(slot, d, kind):
        return pltpu.make_async_remote_copy(
            src_ref=source(slot, d, kind), dst_ref=landing(slot, d, kind), send_sem=send_sem.at[slot, kind, d],
            recv_sem=recv_sem.at[slot, kind, d], device_id=device(d), device_id_type=MESH)

    def frame_part(part):
        first, stop = (0, *PARTS, steps)[part:part + 2]
        return pl.ds(first, stop - first)

    def frame_side(part, d, arriving=False):
        ts = frame_part(part)
        k = d - 2
        at = k if arriving else 1 - k
        return pltpu.make_async_remote_copy(
            src_ref=f_buf.at[ts, pl.ds(0 if k == 0 else cols - 2, 2)], dst_ref=f_side.at[at, ts],
            send_sem=f_send_sem.at[part, k], recv_sem=f_recv_sem.at[part, at], device_id=device(d), device_id_type=MESH)

    def frame_load(part):
        ts = frame_part(part)
        return pltpu.make_async_copy(frames_ref.at[ts], f_buf.at[ts], f_sem.at[part])

    parts = range(len(PARTS) + 1)
    loads = [(h0_ref, seq_ref.at[steps - 1]), (c0_ref, c_buf), (w_rec_ref, w_buf.at[pl.ds(0, 9 * hid)]), (bias_ref, bias_buf)]
    loads += [(w_in_ref.at[pl.ds(packed * dy, packed)], w_buf.at[pl.ds(9 * hid + LANES * dy, packed)]) for dy in range(3)]
    loads = [pltpu.make_async_copy(src, dst, arg_sem.at[k]) for k, (src, dst) in enumerate(loads)]
    frame_load(0).start()
    for load in loads:
        load.start()
    for part in parts[1:]:
        frame_load(part).start()
    for ref in (row_recv, col_recv, corner_recv, crow_recv, ccol_recv, f_side):
        ref[...] = jnp.zeros_like(ref)
    for slot in range(2):
        x_buf[slot, pl.ds(0, 2 * PITCH), :] = jnp.zeros((2 * PITCH, hid), F32)
        x_buf[slot, pl.ds((rows + 2) * PITCH, 10 * PITCH), :] = jnp.zeros((10 * PITCH, hid), F32)
    for slot in range(4):
        p_buf[slot, pl.ds(0, 2 * PITCH), :] = jnp.zeros((2 * PITCH, LANES), F32)
        p_buf[slot, pl.ds((rows + 2) * PITCH, 10 * PITCH), :] = jnp.zeros((10 * PITCH, LANES), F32)
    ring_col[...] = jnp.zeros_like(ring_col)

    barrier = pltpu.get_barrier_semaphore()
    count = jnp.int32(0)
    for d in range(8):
        @pl.when(exists(d, n_rows, n_cols))
        def _():
            pl.semaphore_signal(barrier, inc=1, device_id=device(d), device_id_type=MESH)
        count = count + exists(d, n_rows, n_cols).astype(jnp.int32)
    pl.semaphore_wait(barrier, count)

    def send_sides(part):
        frame_load(part).wait()
        for d in (2, 3):
            @pl.when(exists(d, n_rows, n_cols))
            def _():
                frame_side(part, d).start()

    def receive_sides(part):
        for d in (2, 3):
            @pl.when(exists(d, n_rows, n_cols))
            def _():
                frame_side(part, d, True).wait_recv()

    send_sides(0)
    loads[0].wait()
    for r in range(rows):
        x_buf[0, pl.ds(cell(r, 0), cols), :] = seq_ref[steps - 1, r].astype(F32)
    loads[1].wait()
    for r in range(2, rows - 2):
        c_main[pl.ds((r - 2) * width, width), :] = c_buf[pl.ds(r * cols + SIDE, width), :]
    for i, c in enumerate(side_cols):
        c_col[pl.ds(i * rows, rows), :] = c_buf[pl.ds(c, rows, stride=cols), :]
    for i, r in enumerate(edge_rows):
        c_row[pl.ds(i * cols, cols), :] = c_buf[pl.ds(r * cols, cols), :]

    lane = lax.broadcasted_iota(jnp.int32, (1, gates_n), 1)
    scale = jnp.where(lane < 3 * hid, 0.5, 1.0)
    for load in loads[2:]:
        load.wait()
    for at in range(0, 9 * hid, LANES):
        w_buf[pl.ds(at, LANES), :] = (w_buf[pl.ds(at, LANES), :].astype(F32) * scale).astype(BF16)
    bias = bias_buf[...] * scale
    b0 = bias.astype(BF16).astype(F32)
    b1 = (bias - b0).astype(BF16).astype(F32)
    b2 = bias - b0 - b1
    row = lax.broadcasted_iota(jnp.int32, (16, gates_n), 0)
    bias_rows = jnp.where(row == 0, b0, jnp.where(row == 1, b1, jnp.where(row == 2, b2, 0.0)))
    for dy in range(3):
        at = 9 * hid + LANES * dy
        w_buf[pl.ds(at, packed), :] = (w_buf[pl.ds(at, packed), :].astype(F32) * scale).astype(BF16)
        w_buf[pl.ds(at + packed, LANES - packed), :] = jnp.zeros((LANES - packed, gates_n), BF16)
        if dy == 1:
            w_buf[pl.ds(at + packed, 16), :] = bias_rows.astype(BF16)

    row = lax.broadcasted_iota(jnp.int32, (LANES - packed, rows), 0)
    ones = (row < 3).astype(F32).astype(BF16)

    def pack_frame(t, slot):
        for c in range(-1, cols + 1):
            pieces = []
            for k in range(c - 1, c + 2):
                if k < 0:
                    pieces.append(f_side[0, t, k + 2])
                elif k < cols:
                    pieces.append(f_buf[t, k])
                else:
                    pieces.append(f_side[1, t, k - cols])
            window = jnp.concatenate(pieces + [ones], axis=0)
            p_buf[slot, pl.ds(pcell(0, c), rows, stride=PITCH), :] = window.T.astype(F32)

    def stage(slot, p_first):
        state = x_buf.at[0]
        for k, r in enumerate((0, rows - 2)):
            for n in range(2):
                row_send[slot, k, n * cols:(n + 1) * cols] = state[pl.ds(cell(r + n, 0), cols), :].astype(BF16)
            at = 2 * cols
            row_send[slot, k, at:at + 2 * PITCH] = p_buf[p_first, pl.ds(pcell(r, -1), 2 * PITCH), :].astype(BF16)
            at += 2 * PITCH
            r_one = 0 if k == 0 else rows - 1
            row_send[slot, k, at:at + PITCH] = p_buf[p_first + 1, pl.ds(pcell(r_one, -1), PITCH), :].astype(BF16)
            crow_send[slot, k] = c_row[pl.ds((0 if k == 0 else 3) * cols, cols), :]
        for k, c in enumerate((0, cols - 2)):
            for n in range(2):
                col_send[slot, k, n] = state[pl.ds(cell(0, c + n), rows, stride=PITCH), :].astype(BF16)
            ccol_send[slot, k] = c_col[pl.ds((0 if k == 0 else last) * rows, rows), :]
        for k, (dr, dc) in enumerate(DIRECTIONS[4:]):
            r, c = (0 if dr < 0 else rows - 2), (0 if dc < 0 else cols - 2)
            for n in range(2):
                corner = state[pl.ds(cell(r + n, c), 2), :].astype(BF16).astype(F32)
                corner_send[slot, k, 2 * n:2 * n + 2] = corner
            c_at = (0 if dr < 0 else 3 * cols) + (0 if dc < 0 else cols - 1)
            corner_send[slot, k, 4:5] = c_row[pl.ds(c_at, 1), :]

    def each_copy(act, slot, wanted=None):
        for kind in range(2):
            for d in range(8 if kind == 0 else 4):
                @pl.when(exists(d, n_rows, n_cols) if wanted is None else jnp.logical_and(exists(d, n_rows, n_cols), wanted))
                def _():
                    act(slot, d, kind)

    def send_halo(slot, wanted=None):
        each_copy(lambda *which: departure(*which).start(), slot, wanted)

    def receive_halo(slot):
        each_copy(lambda *which: arrival(*which).wait_recv(), slot)

    def wait_sent(slot):
        each_copy(lambda *which: departure(*which).wait_send(), slot)

    def unpack_halo(slot, p_first):
        state = x_buf.at[0]
        for k, r in enumerate((-2, rows)):
            for n in range(2):
                state[pl.ds(cell(r + n, 0), cols), :] = row_recv[slot, k, n * cols:(n + 1) * cols].astype(F32)
            at = 2 * cols
            p_buf[p_first, pl.ds(pcell(r, -1), 2 * PITCH), :] = row_recv[slot, k, at:at + 2 * PITCH].astype(F32)
            at += 2 * PITCH
            r_one = -1 if k == 0 else rows
            p_buf[p_first + 1, pl.ds(pcell(r_one, -1), PITCH), :] = row_recv[slot, k, at:at + PITCH].astype(F32)
            ring_row[pl.ds(k * cols, cols), :] = crow_recv[slot, k]
        for k, c in enumerate((-2, cols)):
            for n in range(2):
                state[pl.ds(cell(0, c + n), rows, stride=PITCH), :] = col_recv[slot, k, n].astype(F32)
            ring_col[pl.ds(k * long + 1, rows), :] = ccol_recv[slot, k]
        for k, (dr, dc) in enumerate(DIRECTIONS[4:]):
            r, c = (-2 if dr < 0 else rows), (-2 if dc < 0 else cols)
            for n in range(2):
                state[pl.ds(cell(r + n, c), 2), :] = corner_recv[slot, k, 2 * n:2 * n + 2]
            at = (0 if dc < 0 else long) + (0 if dr < 0 else rows + 1)
            ring_col[pl.ds(at, 1), :] = corner_recv[slot, k, 4:5]

    receive_sides(0)
    pack_frame(0, 0)
    pack_frame(1, 1)
    stage(0, 0)
    send_halo(0)
    send_sides(1)

    def before(m, now):
        t = 2 * m
        other = 2 * (1 - now)
        pack_frame(jnp.minimum(t + 2, steps - 2), other)
        pack_frame(jnp.minimum(t + 3, steps - 1), other + 1)
        tile.before_wait(2 * now, lambda: tile.write_out(0, seq_ref.at[jnp.maximum(t - 1, 0)]))

        @pl.when(m >= 1)
        def _():
            wait_sent(1 - now)
        receive_halo(now)
        unpack_halo(now, 2 * now)

    def pair(m, now):
        def send():
            stage(1 - now, 2 * (1 - now))
            send_halo(1 - now)
            if now == 0:
                @pl.when(m == 0)
                def _():
                    receive_sides(1)
                    send_sides(2)

                @pl.when(m == 2)
                def _():
                    receive_sides(2)

        before(m, now)
        tile.after_wait(2 * now, send)
        tile.write_out(1, seq_ref.at[2 * m])

    def trip(i, carry):
        pair(2 * i, 0)
        pair(2 * i + 1, 1)
        return carry

    n_pairs = steps // 2
    lax.fori_loop(0, (n_pairs - 1) // 2, trip, 0)
    for m in range(n_pairs - 2 + n_pairs % 2, n_pairs - 1):
        pair(m, m % 2)
    before(n_pairs - 1, (n_pairs - 1) % 2)
    wait_sent((n_pairs - 1) % 2)
    for part in parts:
        for d in (2, 3):
            @pl.when(exists(d, n_rows, n_cols))
            def _():
                frame_side(part, d).wait_send()


def finish_kernel(sizes, seq_in, x_in, p_buf, w_buf, c_main_in, c_col_in, c_row_in, ring_row, ring_col,
                  seq_out, c_out, x_buf, c_main, c_col, c_row, out_buf, c_buf, sem):
    tile = Tile(sizes, x_buf, p_buf, w_buf, c_main, c_col, c_row, ring_row, ring_col)
    steps, rows, cols = sizes[:3]
    copies = [pltpu.make_async_copy(seq_in.at[pl.ds(t, CHUNK)], seq_out.at[pl.ds(t, CHUNK)], sem.at[t // CHUNK])
              for t in range(0, steps - 2, CHUNK)]
    for copy in copies:
        copy.start()
    tail = [pltpu.make_async_copy(out_buf.at[k], seq_out.at[steps - 2 + k], sem.at[(steps - 2) // CHUNK + k])
            for k in range(2)]

    tile.after_wait(2 * ((steps // 2 - 1) % 2))
    for k in range(2):
        tile.write_out(1 - k, out_buf.at[k])
        tail[k].start()
    for r in range(2, rows - 2):
        c_buf[pl.ds(r * cols + SIDE, tile.width), :] = c_main[pl.ds((r - 2) * tile.width, tile.width), :]
    for i, c in enumerate(tile.side_cols):
        c_buf[pl.ds(c, rows, stride=cols), :] = c_col[pl.ds(i * rows, rows), :]
    for i, r in enumerate(tile.edge_rows):
        c_buf[pl.ds(r * cols, cols), :] = c_row[pl.ds(i * cols, cols), :]
    c_copy = pltpu.make_async_copy(c_buf, c_out, sem.at[steps // CHUNK + 1])
    c_copy.start()
    for copy in (*copies, *tail, c_copy):
        copy.wait()


def solution(mesh):
    n_rows = mesh.shape["rows"]
    n_cols = mesh.shape["cols"]
    seq_spec = P(None, "dp", "rows", "cols", None)
    state_spec = P("dp", "rows", "cols", None)

    def local_run(frames, w_in, w_rec, gate_bias, h_init, c_init):
        steps, _, rows, cols, c_in = frames.shape
        hid = h_init.shape[-1]
        row_words = 2 * cols + 3 * PITCH + 4
        both = (2, 2)
        vmem = pl.BlockSpec(memory_space=pltpu.VMEM)
        args = (jnp.transpose(frames[:, 0], (0, 2, 3, 1)), w_rec.reshape(9 * hid, 4 * hid),
                w_in.reshape(9 * c_in, 4 * hid), gate_bias.reshape(1, 4 * hid), h_init[0],
                c_init[0].reshape(rows * cols, hid))
        hbm = pl.BlockSpec(memory_space=pltpu.HBM)
        sizes = (steps, rows, cols, n_rows, n_cols, c_in)

        def wide(*shape):
            return jax.ShapeDtypeStruct((*shape, hid), F32)

        state = (wide(2, (rows + 12) * PITCH), wide(4, (rows + 12) * PITCH),
                 jax.ShapeDtypeStruct((9 * hid + 3 * hid, 4 * hid), BF16), wide((rows - 4) * (cols - 2 * SIDE)),
                 wide(rows * 2 * SIDE), wide(cols * 4), wide(cols * 2), wide((rows + 8) * 2))
        seq_shape = jax.ShapeDtypeStruct((steps, rows, cols, hid), BF16)
        seq, *held = pl.pallas_call(
            functools.partial(kernel, sizes),
            out_shape=(seq_shape, *state),
            in_specs=[hbm] * 6,
            out_specs=(vmem,) * 9,
            scratch_shapes=[
                pltpu.VMEM((1, 4 * hid), F32),
                pltpu.VMEM((steps, cols, c_in, rows), BF16),
                pltpu.VMEM((2, steps, 2, c_in, rows), BF16),
                pltpu.VMEM((rows * cols, hid), F32),
                *[shape for _ in both for shape in (
                    pltpu.VMEM((*both, row_words, hid), BF16),
                    pltpu.VMEM((*both, 2, rows, hid), BF16),
                    pltpu.VMEM((2, 4, 8, hid), F32),
                    pltpu.VMEM((*both, cols, hid), F32),
                    pltpu.VMEM((*both, rows, hid), F32))],
                pltpu.SemaphoreType.DMA((*both, 8)),
                pltpu.SemaphoreType.DMA((*both, 8)),
                pltpu.SemaphoreType.DMA((len(PARTS) + 1,)),
                pltpu.SemaphoreType.DMA((len(PARTS) + 1, 2)),
                pltpu.SemaphoreType.DMA((len(PARTS) + 1, 2)),
                pltpu.SemaphoreType.DMA((7,)),
            ],
            compiler_params=pltpu.CompilerParams(
                collective_id=0, has_side_effects=True, vmem_limit_bytes=14 * 2**20),
            name="convlstm",
        )(*(pltpu.with_memory_space_constraint(x, pltpu.HBM) for x in args))
        changed = (0, 3, 4, 5)
        seq, c_last, *_ = pl.pallas_call(
            functools.partial(finish_kernel, sizes),
            out_shape=(seq_shape, wide(rows * cols), *(state[k] for k in changed)),
            in_specs=[vmem] * 9,
            out_specs=(hbm, hbm, *[vmem] * len(changed)),
            input_output_aliases={1 + k: 2 + n for n, k in enumerate(changed)},
            scratch_shapes=[
                pltpu.VMEM((2, rows, cols, hid), BF16),
                pltpu.VMEM((rows * cols, hid), F32),
                pltpu.SemaphoreType.DMA((steps // CHUNK + 2,)),
            ],
            compiler_params=pltpu.CompilerParams(vmem_limit_bytes=6 * 2**20),
            name="finish",
        )(seq, *held)
        return seq[:, None], c_last.reshape(c_init.shape)

    return jax.shard_map(local_run, mesh=mesh, in_specs=(seq_spec, P(), P(), P(), state_spec, state_spec),
                         out_specs=(seq_spec, state_spec), check_vma=False)
```

```python
import functools

import jax
import jax.numpy as jnp
from jax import lax
from jax.experimental import pallas as pl
from jax.experimental.pallas import tpu as pltpu
from jax.sharding import PartitionSpec as P

MESH = pl.DeviceIdType.MESH
LANES = 128
BF16 = jnp.bfloat16
F32 = jnp.float32
TDT = jnp.bfloat16

PITCH = 36
DIRECTIONS = ((-1, 0), (1, 0), (0, -1), (0, 1), (-1, -1), (-1, 1), (1, -1), (1, 1))
CHUNK = 2
PARTS = (4, 12)
FIRST, STOP = 13, 29
BLOCK = 11
SIDE = 4


def cell(r, c):
    return (r + 2) * PITCH + c + 2


def pcell(r, c):
    return (r + 2) * PITCH + c + 1


def exists(d, n_rows, n_cols):
    dr, dc = DIRECTIONS[d]
    ok = None
    for here, step, count in ((lax.axis_index("rows"), dr, n_rows), (lax.axis_index("cols"), dc, n_cols)):
        if step:
            this = (here > 0) if step < 0 else (here < count - 1)
            ok = this if ok is None else jnp.logical_and(ok, this)
    return ok


class Tile:
    def __init__(self, sizes, x_buf, p_buf, w_buf, c_main, c_col, c_row, ring_row, ring_col):
        self.steps, self.rows, self.cols, self.n_rows, self.n_cols, self.c_in = sizes
        self.x_buf, self.p_buf, self.w_buf = x_buf, p_buf, w_buf
        self.c_main, self.c_col, self.c_row = c_main, c_col, c_row
        self.ring_row, self.ring_col = ring_row, ring_col
        self.hid = x_buf.shape[-1]
        self.width = self.cols - 2 * SIDE
        self.long = self.rows + 8
        self.side_cols = tuple(range(SIDE)) + tuple(range(self.cols - SIDE, self.cols))
        self.edge_rows = (0, 1, self.rows - 2, self.rows - 1)
        self.last = len(self.side_cols) - 1

    def run_index(self, start, length, vertical):
        return pl.ds(start, length, stride=PITCH) if vertical else pl.ds(start, length)

    def gates_of(self, slot, p_slot, groups):
        parts = []
        for dy in range(3):
            for dx in range(3):
                pieces = [self.x_buf[slot, self.run_index(cell(r + dy - 1, c + dx - 1), length, vertical), :]
                          for r, c, length, vertical in groups]
                parts.append(jnp.concatenate(pieces, axis=0) if len(pieces) > 1 else pieces[0])
        for dy in range(3):
            pieces = [self.p_buf[p_slot, self.run_index(pcell(r + dy - 1, c), length, vertical), :]
                      for r, c, length, vertical in groups]
            parts.append(jnp.concatenate(pieces, axis=0) if len(pieces) > 1 else pieces[0])
        lhs = jnp.concatenate(parts, axis=1).astype(BF16)
        return jnp.dot(lhs, self.w_buf[...], preferred_element_type=F32)

    def finish(self, slot, groups, gates, c_ref, c_at, mask=None):
        index = pl.ds(c_at, gates.shape[0])
        c_prev = c_ref[index, :]
        gi, gf, go, gg = (jnp.tanh(gates[:, self.hid * k:self.hid * (k + 1)]) for k in range(4))
        c_next = 0.5 * ((gf * c_prev + c_prev) + (gi * gg + gg))
        h = (0.5 * go + 0.5) * jnp.tanh(c_next)
        if mask is None:
            c_ref[index, :] = c_next
        else:
            h = h * mask
        at = 0
        for r, c, length, vertical in groups:
            self.x_buf[1 - slot, self.run_index(cell(r, c), length, vertical), :] = h[at:at + length]
            at += length

    def update(self, slot, p_slot, groups, c_ref, c_at):
        self.finish(slot, groups, self.gates_of(slot, p_slot, groups), c_ref, c_at)

    def main_run(self, first, stop):
        return [(r, SIDE, self.width, False) for r in range(first, stop)]

    def side_run(self, *ids):
        return [(0, self.side_cols[i], self.rows, True) for i in ids]

    def main_rows(self, slot, p_slot, first, stop):
        self.update(slot, p_slot, self.main_run(first, stop), self.c_main, (first - 2) * self.width)

    def write_out(self, slot, ref):
        for r in range(self.rows):
            ref[r] = self.x_buf[slot, pl.ds(cell(r, 0), self.cols), :].astype(BF16)

    def before_wait(self, pa, write):
        rows, last = self.rows, self.last
        for at in range(2, rows - 2, BLOCK):
            self.main_rows(0, pa, at, at + BLOCK)
        self.update(0, pa, self.side_run(1, 2, 3), self.c_col, rows)
        self.update(0, pa, self.side_run(last - 3, last - 2, last - 1), self.c_col, (last - 3) * rows)
        write()
        for first, stop in ((3, FIRST), (STOP, rows - 11), (rows - 11, rows - 3)):
            self.main_rows(1, pa + 1, first, stop)

    def after_wait(self, pa, send=lambda: None):
        rows, cols, last = self.rows, self.cols, self.last
        there = [exists(d, self.n_rows, self.n_cols).astype(jnp.int32).astype(F32) for d in range(4)]
        place = lax.broadcasted_iota(jnp.int32, (self.long, self.hid), 0)
        ends = jnp.where(place == 0, there[0], jnp.where(place == rows + 1, there[1], 1.0))
        ring_col_run = [(-1, -1, self.long, True), (-1, cols, self.long, True)]
        ring_row_run = [(-1, 0, cols, False), (rows, 0, cols, False)]
        row_run = [(r, 0, cols, False) for r in self.edge_rows]
        n_long = 2 * self.long
        middle = (FIRST + STOP) // 2
        c_col, c_row, c_main, finish = self.c_col, self.c_row, self.c_main, self.finish

        own = self.side_run(0) + self.side_run(last) + row_run
        own_gates = self.gates_of(0, pa, own)
        ring_gates = self.gates_of(0, pa, ring_col_run + ring_row_run)
        run = self.main_run(FIRST, middle)
        beside = self.gates_of(1, pa + 1, run)
        finish(0, self.side_run(0), own_gates[:rows], c_col, 0)
        finish(0, self.side_run(last), own_gates[rows:2 * rows], c_col, last * rows)
        finish(0, row_run, own_gates[2 * rows:], c_row, 0)
        mask = jnp.concatenate([ends * there[2], ends * there[3]], axis=0)
        finish(0, ring_col_run, ring_gates[:n_long], self.ring_col, 0, mask)
        mask = jnp.concatenate([jnp.full((cols, self.hid), 1.0, F32) * there[k] for k in range(2)], axis=0)
        finish(0, ring_row_run, ring_gates[n_long:], self.ring_row, 0, mask)
        for i, r in ((0, 0), (3, rows - 1)):
            for first in (1, last - 3):
                c_col[pl.ds(first * rows + r, 3, stride=rows), :] = c_row[pl.ds(i * cols + self.side_cols[first], 3), :]
        finish(1, run, beside, c_main, (FIRST - 2) * self.width)
        edge_gates = self.gates_of(1, pa + 1, self.side_run(0, 1, last - 1, last) + row_run)
        run = self.main_run(middle, STOP)
        beside = self.gates_of(1, pa + 1, run)
        finish(1, self.side_run(0, 1), edge_gates[:2 * rows], c_col, 0)
        finish(1, self.side_run(last - 1, last), edge_gates[2 * rows:4 * rows], c_col, (last - 1) * rows)
        finish(1, row_run, edge_gates[4 * rows:], c_row, 0)
        send()

        finish(1, run, beside, c_main, (middle - 2) * self.width)
        runs = [(self.side_run(2, 3), c_col, 2 * rows), (self.side_run(last - 3, last - 2), c_col, (last - 3) * rows),
                (self.main_run(2, 3), c_main, 0), (self.main_run(rows - 3, rows - 2), c_main, (rows - 5) * self.width)]
        gates = self.gates_of(1, pa + 1, sum((run for run, _, _ in runs), []))
        at = 0
        for run, c_ref, c_at in runs:
            size = sum(length for _, _, length, _ in run)
            finish(1, run, gates[at:at + size], c_ref, c_at)
            at += size


def kernel(sizes, frames_ref, w_rec_ref, w_in_ref, bias_ref, h0_ref, c0_ref,
           seq_ref, x_buf, p_buf, w_buf, c_main, c_col, c_row, ring_row, ring_col,
           bias_buf, f_buf, f_side, c_buf, row_send, col_send, corner_send, crow_send, ccol_send,
           row_recv, col_recv, corner_recv, crow_recv, ccol_recv,
           send_sem, recv_sem, f_sem, f_send_sem, f_recv_sem, arg_sem):
    tile = Tile(sizes, x_buf, p_buf, w_buf, c_main, c_col, c_row, ring_row, ring_col)
    steps, rows, cols, n_rows, n_cols, c_in = sizes
    hid, width, long, last = tile.hid, tile.width, tile.long, tile.last
    side_cols, edge_rows = tile.side_cols, tile.edge_rows
    gates_n = 4 * hid
    packed = 3 * c_in
    my_row = lax.axis_index("rows")
    my_col = lax.axis_index("cols")

    def device(d):
        dr, dc = DIRECTIONS[d]
        return {"rows": my_row + dr, "cols": my_col + dc}

    def opposite(d):
        return DIRECTIONS.index((-DIRECTIONS[d][0], -DIRECTIONS[d][1]))

    def source(slot, d, kind):
        dr, dc = DIRECTIONS[d]
        if dr and dc:
            return corner_send.at[slot, d - 4]
        if dr:
            return (crow_send if kind else row_send).at[slot, d]
        return (ccol_send if kind else col_send).at[slot, d - 2]

    def landing(slot, d, kind):
        dr, dc = DIRECTIONS[d]
        if dr and dc:
            return corner_recv.at[slot, d - 4]
        if dr:
            return (crow_recv if kind else row_recv).at[slot, d]
        return (ccol_recv if kind else col_recv).at[slot, d - 2]

    def departure(slot, d, kind):
        return pltpu.make_async_remote_copy(
            src_ref=source(slot, d, kind), dst_ref=landing(slot, opposite(d), kind), send_sem=send_sem.at[slot, kind, d],
            recv_sem=recv_sem.at[slot, kind, opposite(d)], device_id=device(d), device_id_type=MESH)

    def arrival(slot, d, kind):
        return pltpu.make_async_remote_copy(
            src_ref=source(slot, d, kind), dst_ref=landing(slot, d, kind), send_sem=send_sem.at[slot, kind, d],
            recv_sem=recv_sem.at[slot, kind, d], device_id=device(d), device_id_type=MESH)

    def frame_part(part):
        first, stop = (0, *PARTS, steps)[part:part + 2]
        return pl.ds(first, stop - first)

    def frame_side(part, d, arriving=False):
        ts = frame_part(part)
        k = d - 2
        at = k if arriving else 1 - k
        return pltpu.make_async_remote_copy(
            src_ref=f_buf.at[ts, pl.ds(0 if k == 0 else cols - 2, 2)], dst_ref=f_side.at[at, ts],
            send_sem=f_send_sem.at[part, k], recv_sem=f_recv_sem.at[part, at], device_id=device(d), device_id_type=MESH)

    def frame_load(part):
        ts = frame_part(part)
        return pltpu.make_async_copy(frames_ref.at[ts], f_buf.at[ts], f_sem.at[part])

    parts = range(len(PARTS) + 1)
    loads = [(h0_ref, seq_ref.at[steps - 1]), (c0_ref, c_buf), (w_rec_ref, w_buf.at[pl.ds(0, 9 * hid)]), (bias_ref, bias_buf)]
    loads += [(w_in_ref.at[pl.ds(packed * dy, packed)], w_buf.at[pl.ds(9 * hid + LANES * dy, packed)]) for dy in range(3)]
    loads = [pltpu.make_async_copy(src, dst, arg_sem.at[k]) for k, (src, dst) in enumerate(loads)]
    frame_load(0).start()
    for load in loads:
        load.start()
    for part in parts[1:]:
        frame_load(part).start()
    for ref in (row_recv, col_recv, corner_recv, crow_recv, ccol_recv, f_side):
        ref[...] = jnp.zeros_like(ref)
    for slot in range(2):
        x_buf[slot, pl.ds(0, 2 * PITCH), :] = jnp.zeros((2 * PITCH, hid), F32)
        x_buf[slot, pl.ds((rows + 2) * PITCH, 10 * PITCH), :] = jnp.zeros((10 * PITCH, hid), F32)
    for slot in range(4):
        p_buf[slot, pl.ds(0, 2 * PITCH), :] = jnp.zeros((2 * PITCH, LANES), F32)
        p_buf[slot, pl.ds((rows + 2) * PITCH, 10 * PITCH), :] = jnp.zeros((10 * PITCH, LANES), F32)
    ring_col[...] = jnp.zeros_like(ring_col)

    barrier = pltpu.get_barrier_semaphore()
    count = jnp.int32(0)
    for d in range(8):
        @pl.when(exists(d, n_rows, n_cols))
        def _():
            pl.semaphore_signal(barrier, inc=1, device_id=device(d), device_id_type=MESH)
        count = count + exists(d, n_rows, n_cols).astype(jnp.int32)
    pl.semaphore_wait(barrier, count)

    def send_sides(part):
        frame_load(part).wait()
        for d in (2, 3):
            @pl.when(exists(d, n_rows, n_cols))
            def _():
                frame_side(part, d).start()

    def receive_sides(part):
        for d in (2, 3):
            @pl.when(exists(d, n_rows, n_cols))
            def _():
                frame_side(part, d, True).wait_recv()

    send_sides(0)
    loads[0].wait()
    for r in range(rows):
        x_buf[0, pl.ds(cell(r, 0), cols), :] = seq_ref[steps - 1, r].astype(F32)
    loads[1].wait()
    for r in range(2, rows - 2):
        c_main[pl.ds((r - 2) * width, width), :] = c_buf[pl.ds(r * cols + SIDE, width), :]
    for i, c in enumerate(side_cols):
        c_col[pl.ds(i * rows, rows), :] = c_buf[pl.ds(c, rows, stride=cols), :]
    for i, r in enumerate(edge_rows):
        c_row[pl.ds(i * cols, cols), :] = c_buf[pl.ds(r * cols, cols), :]

    lane = lax.broadcasted_iota(jnp.int32, (1, gates_n), 1)
    scale = jnp.where(lane < 3 * hid, 0.5, 1.0)
    for load in loads[2:]:
        load.wait()
    for at in range(0, 9 * hid, LANES):
        w_buf[pl.ds(at, LANES), :] = (w_buf[pl.ds(at, LANES), :].astype(F32) * scale).astype(BF16)
    bias = bias_buf[...] * scale
    b0 = bias.astype(BF16).astype(F32)
    b1 = (bias - b0).astype(BF16).astype(F32)
    b2 = bias - b0 - b1
    row = lax.broadcasted_iota(jnp.int32, (16, gates_n), 0)
    bias_rows = jnp.where(row == 0, b0, jnp.where(row == 1, b1, jnp.where(row == 2, b2, 0.0)))
    for dy in range(3):
        at = 9 * hid + LANES * dy
        w_buf[pl.ds(at, packed), :] = (w_buf[pl.ds(at, packed), :].astype(F32) * scale).astype(BF16)
        w_buf[pl.ds(at + packed, LANES - packed), :] = jnp.zeros((LANES - packed, gates_n), BF16)
        if dy == 1:
            w_buf[pl.ds(at + packed, 16), :] = bias_rows.astype(BF16)

    row = lax.broadcasted_iota(jnp.int32, (LANES - packed, rows), 0)
    ones = (row < 3).astype(F32).astype(BF16)

    def pack_frame(t, slot):
        for c in range(-1, cols + 1):
            pieces = []
            for k in range(c - 1, c + 2):
                if k < 0:
                    pieces.append(f_side[0, t, k + 2])
                elif k < cols:
                    pieces.append(f_buf[t, k])
                else:
                    pieces.append(f_side[1, t, k - cols])
            window = jnp.concatenate(pieces + [ones], axis=0)
            p_buf[slot, pl.ds(pcell(0, c), rows, stride=PITCH), :] = window.T.astype(F32)

    def stage(slot, p_first):
        state = x_buf.at[0]
        for k, r in enumerate((0, rows - 2)):
            for n in range(2):
                row_send[slot, k, n * cols:(n + 1) * cols] = state[pl.ds(cell(r + n, 0), cols), :].astype(BF16)
            at = 2 * cols
            row_send[slot, k, at:at + 2 * PITCH] = p_buf[p_first, pl.ds(pcell(r, -1), 2 * PITCH), :].astype(BF16)
            at += 2 * PITCH
            r_one = 0 if k == 0 else rows - 1
            row_send[slot, k, at:at + PITCH] = p_buf[p_first + 1, pl.ds(pcell(r_one, -1), PITCH), :].astype(BF16)
            crow_send[slot, k] = c_row[pl.ds((0 if k == 0 else 3) * cols, cols), :]
        for k, c in enumerate((0, cols - 2)):
            for n in range(2):
                col_send[slot, k, n] = state[pl.ds(cell(0, c + n), rows, stride=PITCH), :].astype(BF16)
            ccol_send[slot, k] = c_col[pl.ds((0 if k == 0 else last) * rows, rows), :]
        for k, (dr, dc) in enumerate(DIRECTIONS[4:]):
            r, c = (0 if dr < 0 else rows - 2), (0 if dc < 0 else cols - 2)
            for n in range(2):
                corner = state[pl.ds(cell(r + n, c), 2), :].astype(BF16).astype(F32)
                corner_send[slot, k, 2 * n:2 * n + 2] = corner
            c_at = (0 if dr < 0 else 3 * cols) + (0 if dc < 0 else cols - 1)
            corner_send[slot, k, 4:5] = c_row[pl.ds(c_at, 1), :]

    def each_copy(act, slot, wanted=None):
        for kind in range(2):
            for d in range(8 if kind == 0 else 4):
                @pl.when(exists(d, n_rows, n_cols) if wanted is None else jnp.logical_and(exists(d, n_rows, n_cols), wanted))
                def _():
                    act(slot, d, kind)

    def send_halo(slot, wanted=None):
        each_copy(lambda *which: departure(*which).start(), slot, wanted)

    def receive_halo(slot):
        each_copy(lambda *which: arrival(*which).wait_recv(), slot)

    def wait_sent(slot):
        each_copy(lambda *which: departure(*which).wait_send(), slot)

    def unpack_halo(slot, p_first):
        state = x_buf.at[0]
        for k, r in enumerate((-2, rows)):
            for n in range(2):
                state[pl.ds(cell(r + n, 0), cols), :] = row_recv[slot, k, n * cols:(n + 1) * cols].astype(F32)
            at = 2 * cols
            p_buf[p_first, pl.ds(pcell(r, -1), 2 * PITCH), :] = row_recv[slot, k, at:at + 2 * PITCH].astype(F32)
            at += 2 * PITCH
            r_one = -1 if k == 0 else rows
            p_buf[p_first + 1, pl.ds(pcell(r_one, -1), PITCH), :] = row_recv[slot, k, at:at + PITCH].astype(F32)
            ring_row[pl.ds(k * cols, cols), :] = crow_recv[slot, k]
        for k, c in enumerate((-2, cols)):
            for n in range(2):
                state[pl.ds(cell(0, c + n), rows, stride=PITCH), :] = col_recv[slot, k, n].astype(F32)
            ring_col[pl.ds(k * long + 1, rows), :] = ccol_recv[slot, k]
        for k, (dr, dc) in enumerate(DIRECTIONS[4:]):
            r, c = (-2 if dr < 0 else rows), (-2 if dc < 0 else cols)
            for n in range(2):
                state[pl.ds(cell(r + n, c), 2), :] = corner_recv[slot, k, 2 * n:2 * n + 2]
            at = (0 if dc < 0 else long) + (0 if dr < 0 else rows + 1)
            ring_col[pl.ds(at, 1), :] = corner_recv[slot, k, 4:5]

    receive_sides(0)
    pack_frame(0, 0)
    pack_frame(1, 1)
    stage(0, 0)
    send_halo(0)
    send_sides(1)

    def before(m, now):
        t = 2 * m
        other = 2 * (1 - now)
        pack_frame(jnp.minimum(t + 2, steps - 2), other)
        pack_frame(jnp.minimum(t + 3, steps - 1), other + 1)
        tile.before_wait(2 * now, lambda: tile.write_out(0, seq_ref.at[jnp.maximum(t - 1, 0)]))

        @pl.when(m >= 1)
        def _():
            wait_sent(1 - now)
        receive_halo(now)
        unpack_halo(now, 2 * now)

    def pair(m, now):
        def send():
            stage(1 - now, 2 * (1 - now))
            send_halo(1 - now)
            if now == 0:
                @pl.when(m == 0)
                def _():
                    receive_sides(1)
                    send_sides(2)

                @pl.when(m == 2)
                def _():
                    receive_sides(2)

        before(m, now)
        tile.after_wait(2 * now, send)
        tile.write_out(1, seq_ref.at[2 * m])

    def trip(i, carry):
        pair(2 * i, 0)
        pair(2 * i + 1, 1)
        return carry

    n_pairs = steps // 2
    lax.fori_loop(0, (n_pairs - 1) // 2, trip, 0)
    for m in range(n_pairs - 2 + n_pairs % 2, n_pairs - 1):
        pair(m, m % 2)
    before(n_pairs - 1, (n_pairs - 1) % 2)
    wait_sent((n_pairs - 1) % 2)
    for part in parts:
        for d in (2, 3):
            @pl.when(exists(d, n_rows, n_cols))
            def _():
                frame_side(part, d).wait_send()


def finish_kernel(sizes, seq_in, x_in, p_buf, w_buf, c_main_in, c_col_in, c_row_in, ring_row, ring_col,
                  seq_out, c_out, x_buf, c_main, c_col, c_row, out_buf, c_buf, sem):
    tile = Tile(sizes, x_buf, p_buf, w_buf, c_main, c_col, c_row, ring_row, ring_col)
    steps, rows, cols = sizes[:3]
    copies = [pltpu.make_async_copy(seq_in.at[pl.ds(t, CHUNK)], seq_out.at[pl.ds(t, CHUNK)], sem.at[t // CHUNK])
              for t in range(0, steps - 2, CHUNK)]
    for copy in copies:
        copy.start()
    tile.after_wait(2 * ((steps // 2 - 1) % 2))
    for slot in range(2):
        tile.write_out(1 - slot, out_buf.at[slot])
    for r in range(2, rows - 2):
        c_buf[pl.ds(r * cols + SIDE, tile.width), :] = c_main[pl.ds((r - 2) * tile.width, tile.width), :]
    for i, c in enumerate(tile.side_cols):
        c_buf[pl.ds(c, rows, stride=cols), :] = c_col[pl.ds(i * rows, rows), :]
    for i, r in enumerate(tile.edge_rows):
        c_buf[pl.ds(r * cols, cols), :] = c_row[pl.ds(i * cols, cols), :]
    tail = [pltpu.make_async_copy(out_buf, seq_out.at[pl.ds(steps - 2, 2)], sem.at[steps // CHUNK]),
            pltpu.make_async_copy(c_buf, c_out, sem.at[steps // CHUNK + 1])]
    for copy in tail:
        copy.start()
    for copy in copies + tail:
        copy.wait()


def solution(mesh):
    n_rows = mesh.shape["rows"]
    n_cols = mesh.shape["cols"]
    seq_spec = P(None, "dp", "rows", "cols", None)
    state_spec = P("dp", "rows", "cols", None)

    def local_run(frames, w_in, w_rec, gate_bias, h_init, c_init):
        steps, _, rows, cols, c_in = frames.shape
        hid = h_init.shape[-1]
        row_words = 2 * cols + 3 * PITCH + 4
        both = (2, 2)
        vmem = pl.BlockSpec(memory_space=pltpu.VMEM)
        args = (jnp.transpose(frames[:, 0], (0, 2, 3, 1)), w_rec.reshape(9 * hid, 4 * hid),
                w_in.reshape(9 * c_in, 4 * hid), gate_bias.reshape(1, 4 * hid), h_init[0],
                c_init[0].reshape(rows * cols, hid))
        hbm = pl.BlockSpec(memory_space=pltpu.HBM)
        sizes = (steps, rows, cols, n_rows, n_cols, c_in)

        def wide(*shape):
            return jax.ShapeDtypeStruct((*shape, hid), F32)

        state = (wide(2, (rows + 12) * PITCH), wide(4, (rows + 12) * PITCH),
                 jax.ShapeDtypeStruct((9 * hid + 3 * hid, 4 * hid), BF16), wide((rows - 4) * (cols - 2 * SIDE)),
                 wide(rows * 2 * SIDE), wide(cols * 4), wide(cols * 2), wide((rows + 8) * 2))
        seq_shape = jax.ShapeDtypeStruct((steps, rows, cols, hid), BF16)
        seq, *held = pl.pallas_call(
            functools.partial(kernel, sizes),
            out_shape=(seq_shape, *state),
            in_specs=[hbm] * 6,
            out_specs=(vmem,) * 9,
            scratch_shapes=[
                pltpu.VMEM((1, 4 * hid), F32),
                pltpu.VMEM((steps, cols, c_in, rows), BF16),
                pltpu.VMEM((2, steps, 2, c_in, rows), BF16),
                pltpu.VMEM((rows * cols, hid), F32),
                *[shape for _ in both for shape in (
                    pltpu.VMEM((*both, row_words, hid), BF16),
                    pltpu.VMEM((*both, 2, rows, hid), BF16),
                    pltpu.VMEM((2, 4, 8, hid), F32),
                    pltpu.VMEM((*both, cols, hid), F32),
                    pltpu.VMEM((*both, rows, hid), F32))],
                pltpu.SemaphoreType.DMA((*both, 8)),
                pltpu.SemaphoreType.DMA((*both, 8)),
                pltpu.SemaphoreType.DMA((len(PARTS) + 1,)),
                pltpu.SemaphoreType.DMA((len(PARTS) + 1, 2)),
                pltpu.SemaphoreType.DMA((len(PARTS) + 1, 2)),
                pltpu.SemaphoreType.DMA((7,)),
            ],
            compiler_params=pltpu.CompilerParams(
                collective_id=0, has_side_effects=True, vmem_limit_bytes=14 * 2**20),
            name="convlstm",
        )(*(pltpu.with_memory_space_constraint(x, pltpu.HBM) for x in args))
        changed = (0, 3, 4, 5)
        seq, c_last, *_ = pl.pallas_call(
            functools.partial(finish_kernel, sizes),
            out_shape=(seq_shape, wide(rows * cols), *(state[k] for k in changed)),
            in_specs=[vmem] * 9,
            out_specs=(hbm, hbm, *[vmem] * len(changed)),
            input_output_aliases={1 + k: 2 + n for n, k in enumerate(changed)},
            scratch_shapes=[
                pltpu.VMEM((2, rows, cols, hid), BF16),
                pltpu.VMEM((rows * cols, hid), F32),
                pltpu.SemaphoreType.DMA((steps // CHUNK + 2,)),
            ],
            compiler_params=pltpu.CompilerParams(vmem_limit_bytes=6 * 2**20),
            name="finish",
        )(seq, *held)
        return seq[:, None], c_last.reshape(c_init.shape)

    return jax.shard_map(local_run, mesh=mesh, in_specs=(seq_spec, P(), P(), P(), state_spec, state_spec),
                         out_specs=(seq_spec, state_spec), check_vma=False)
```
